128 devices in a mesh: row: 8 (over y, core), col: 16 (over z, x).
Axes of the slice: x: 4, y: 4, z: 4, core: 2. Of those that a mesh axis runs over, the one named last changes fastest.
Arguments:
- nodes: bfloat16 [512, 512, 128], P('row', 'col'), may hold values from -6 to 6
- edges: bfloat16 [8, 16, 16, 1024, 128], P('row', 'col'), may hold values from -2000 to 2000
- senders: int32 [8, 16, 16, 1024], P('row', 'col'), may hold values from 0 to 203, as said below
- receivers: int32 [8, 16, 16, 1024], P('row', 'col'), may hold values from 0 to 127, as said below
- counts: int32 [8, 16, 16], P('row', 'col'), may hold values from 512 to 1024, as said below
- w_edge_in: bfloat16 [384, 128], replicated, may hold values from -0.3125 to 0.3125
- w_edge_hid: bfloat16 [128, 128], replicated, may hold values from -0.5 to 0.5
- w_edge_out: bfloat16 [128, 128], replicated, may hold values from -0.5 to 0.5
- edge_bias: float32 [3, 128], replicated, may hold values from -3 to 3
- edge_gain: float32 [128], replicated, may hold values from 0.25 to 1.75
- edge_shift: float32 [128], replicated, may hold values from -3 to 3
- w_node_in: bfloat16 [256, 128], replicated, may hold values from -0.375 to 0.375
- w_node_hid: bfloat16 [128, 128], replicated, may hold values from -0.5 to 0.5
- w_node_out: bfloat16 [128, 128], replicated, may hold values from -0.5 to 0.5
- node_bias: float32 [3, 128], replicated, may hold values from -3 to 3
- node_gain: float32 [128], replicated, may hold values from 0.25 to 1.75
- node_shift: float32 [128], replicated, may hold values from -3 to 3
Outputs:
- new_nodes: bfloat16 [512, 512, 128], P('row', 'col')
- new_edges: bfloat16 [8, 16, 16, 1024, 128], P('row', 'col')
The draws below stay inside these ranges and needn't reach their ends.
Inputs may be any that keep to these rules, and one draw needn't show every extreme that they name: `senders`: the sender of slot k of band b is numbered in the window of node rows b * 4 - 1 to b * 4 + 4 and node columns -1 to 32 of its tile, row by row over 32 + 2 columns; it is one of the eight nodes around the receiver and lies inside the mesh. `receivers`: receivers are numbered row by row over the 4 x 32 nodes of the slot's band. Slots 0 to counts - 1 of a band hold edges, the others are empty; some band of every draw is full.
All inputs are finite; a program needn't handle non-finite values.
Results may differ from the reference program's by a relative error of at most 0.009.
Values may be sent and summed in bfloat16 or wider, within the bound.
A program may use at most 64 MiB of HBM per device.

```python
import jax
import jax.numpy as jnp
from jax import lax

L = 128
BR = 4
BANDS = 16
TC = 32
TR = 64
EDGE_SLOTS = 1024
TILES_R = 8
TILES_C = 16
NR = 512
NC = 512


def edge_geometry(key):
    local_key = jax.random.fold_in(key, 11)
    first_key, second_key = jax.random.split(local_key)
    shape = (TILES_R, TILES_C, BANDS, EDGE_SLOTS)
    recv_index = jax.random.randint(first_key, shape, 0, BR * TC, dtype=jnp.int32)
    direction = jax.random.randint(second_key, shape, 0, 8, dtype=jnp.int32)
    position = direction + (direction >= 4).astype(jnp.int32)
    step_row = position // 3 - 1
    step_col = position % 3 - 1
    tile_row = lax.broadcasted_iota(jnp.int32, shape, 0)
    tile_col = lax.broadcasted_iota(jnp.int32, shape, 1)
    band_index = lax.broadcasted_iota(jnp.int32, shape, 2)
    local_row = recv_index // TC
    local_col = recv_index % TC
    global_row = tile_row * (BANDS * BR) + band_index * BR + local_row
    global_col = tile_col * TC + local_col
    outside_row = (global_row + step_row < 0) | (global_row + step_row >= TILES_R * BANDS * BR)
    outside_col = (global_col + step_col < 0) | (global_col + step_col >= TILES_C * TC)
    step_row = jnp.where(outside_row, -step_row, step_row)
    step_col = jnp.where(outside_col, -step_col, step_col)
    send_index = (local_row + 1 + step_row) * (TC + 2) + local_col + 1 + step_col
    return (send_index.astype(jnp.int32), recv_index.astype(jnp.int32))


def draw_senders(key, part):
    return edge_geometry(key)[0]


def draw_receivers(key, part):
    return edge_geometry(key)[1]


def draw_counts(key, part):
    local_key = jax.random.fold_in(key, 23)
    first_key, second_key, third_key = jax.random.split(local_key, 3)
    shape = (TILES_R, TILES_C, BANDS)
    values = jax.random.randint(first_key, shape, EDGE_SLOTS // 2, EDGE_SLOTS + 1, dtype=jnp.int32)
    number = TILES_R * TILES_C * BANDS
    full_pick = jax.random.randint(second_key, (), 0, number, dtype=jnp.int32)
    least_pick = jax.random.randint(third_key, (), 0, number, dtype=jnp.int32)
    position = jnp.arange(number, dtype=jnp.int32).reshape(shape)
    values = jnp.where(position == least_pick, EDGE_SLOTS // 2, values)
    values = jnp.where(position == full_pick, EDGE_SLOTS, values)
    return values.astype(jnp.int32)


def draw_edges(key, part):
    local_key = jax.random.fold_in(key, 31)
    keys = jax.random.split(local_key, 5)
    shape = (TILES_R, TILES_C, BANDS, EDGE_SLOTS, L)
    row_part = jnp.arange(TILES_R, dtype=jnp.float32).reshape(TILES_R, 1, 1, 1, 1) / max(TILES_R - 1, 1)
    col_part = jnp.arange(TILES_C, dtype=jnp.float32).reshape(1, TILES_C, 1, 1, 1) / max(TILES_C - 1, 1)
    tile_scale = 1.0 + row_part + col_part
    row_scale = jnp.exp(jax.random.uniform(keys[0], (TILES_R, TILES_C, BANDS, EDGE_SLOTS, 1), jnp.float32, 0.0, jnp.log(10.0)))
    col_scale = jnp.exp(jax.random.uniform(keys[1], (L,), jnp.float32, 0.0, jnp.log(10.0)))
    noise = jnp.clip(jax.random.normal(keys[2], shape, jnp.float32), -4.0, 4.0)
    col_mean = 2.0 * jnp.clip(jax.random.normal(keys[4], (L,), jnp.float32), -3.0, 3.0) * col_scale
    row_offset = 6.0 * row_part * col_scale
    values = col_mean + row_offset + tile_scale * row_scale * col_scale * noise
    return values.astype(jnp.bfloat16)


def block_levels(own_key, extent, pieces, least, top_value):
    loudness, own = 1.0, jax.random.fold_in(own_key, 6)
    for dim, blocks in pieces:
        steps = jnp.exp(jax.random.uniform(jax.random.fold_in(own, dim), (blocks,), jnp.float32, least / len(pieces), top_value / len(pieces)))
        loudness = loudness * jnp.repeat(steps, extent[dim] // blocks).reshape([-1 if axis == dim else 1 for axis in range(len(extent))])
    return loudness


def normal_values(key, shape, scale, most, pieces=(), kind=jnp.bfloat16):
    values = jax.random.normal(key, shape, jnp.float32) * scale
    if len(pieces) > 0:
        values = block_levels(key, shape, pieces, -0.22, 0.18) * values
    return jnp.clip(values, min=-most, max=most).astype(kind)


def setup_inputs(seed: int = 0) -> dict:
    key_of = jax.random.split(jax.random.key(seed), 18)
    nodes = normal_values(key_of[0], (NR, NC, L), 1.0, 6.0, ((0, 8), (1, 16)))
    edges = draw_edges(jax.random.fold_in(key_of[17], 71), 0)
    senders = draw_senders(jax.random.fold_in(key_of[17], 71), 0)
    receivers = draw_receivers(jax.random.fold_in(key_of[17], 71), 0)
    counts = draw_counts(jax.random.fold_in(key_of[17], 71), 0)
    w_edge_in = normal_values(key_of[5], (3 * L, L), (3 * L) ** -0.5, 0.3125)
    w_edge_hid = normal_values(key_of[6], (L, L), L ** -0.5, 0.5)
    w_edge_out = normal_values(key_of[7], (L, L), L ** -0.5, 0.5)
    edge_bias = normal_values(key_of[8], (3, L), 0.5, 3.0, (), jnp.float32)
    edge_gain = jnp.clip(1.0 + 0.15 * jax.random.normal(key_of[9], (L,), jnp.float32), 0.25, 1.75)
    edge_shift = normal_values(key_of[10], (L,), 0.5, 3.0, (), jnp.float32)
    w_node_in = normal_values(key_of[11], (2 * L, L), (2 * L) ** -0.5, 0.375)
    w_node_hid = normal_values(key_of[12], (L, L), L ** -0.5, 0.5)
    w_node_out = normal_values(key_of[13], (L, L), L ** -0.5, 0.5)
    node_bias = normal_values(key_of[14], (3, L), 0.5, 3.0, (), jnp.float32)
    node_gain = jnp.clip(1.0 + 0.15 * jax.random.normal(key_of[15], (L,), jnp.float32), 0.25, 1.75)
    node_shift = normal_values(key_of[16], (L,), 0.5, 3.0, (), jnp.float32)
    return dict(nodes=nodes, edges=edges, senders=senders, receivers=receivers, counts=counts, w_edge_in=w_edge_in, w_edge_hid=w_edge_hid, w_edge_out=w_edge_out, edge_bias=edge_bias, edge_gain=edge_gain, edge_shift=edge_shift, w_node_in=w_node_in, w_node_hid=w_node_hid, w_node_out=w_node_out, node_bias=node_bias, node_gain=node_gain, node_shift=node_shift)


def layer_norm(values):
    centred = values - lax.optimization_barrier(jnp.mean(values, axis=-1, keepdims=True))
    spread = lax.optimization_barrier(jnp.mean(centred * centred, axis=-1, keepdims=True))
    return centred * lax.rsqrt(spread + 1e-05)

def reference(nodes, edges, senders, receivers, counts, w_edge_in, w_edge_hid, w_edge_out, edge_bias, edge_gain, edge_shift, w_node_in, w_node_hid, w_node_out, node_bias, node_gain, node_shift):
    tile_count = TILES_R * TILES_C
    latent = L
    flat_edges = edges.reshape(tile_count, BANDS, EDGE_SLOTS, latent)
    flat_send = senders.reshape(tile_count, BANDS, EDGE_SLOTS)
    flat_recv = receivers.reshape(tile_count, BANDS, EDGE_SLOTS)
    flat_count = counts.reshape(tile_count, BANDS)
    slot_index = jnp.arange(EDGE_SLOTS, dtype=jnp.int32)

    def live_of(count_row):
        return (slot_index[None, :] < count_row[:, None]).astype(jnp.float32)

    def first_pass(inputs):
        edge_block, count_row = inputs
        return lax.optimization_barrier(jnp.sum(edge_block.astype(jnp.float32) * live_of(count_row)[..., None], axis=(0, 1)))
    edge_total = jnp.sum(counts).astype(jnp.float32)
    edge_mean = lax.optimization_barrier(jnp.sum(lax.map(first_pass, (flat_edges, flat_count)), axis=0)) / edge_total

    def second_pass(inputs):
        edge_block, count_row = inputs
        centred = edge_block.astype(jnp.float32) - edge_mean
        return lax.optimization_barrier(jnp.sum(centred * centred * live_of(count_row)[..., None], axis=(0, 1)))
    edge_var = lax.optimization_barrier(jnp.sum(lax.map(second_pass, (flat_edges, flat_count)), axis=0)) / edge_total
    inv_spread = lax.rsqrt(edge_var + 1e-05)
    padded = jnp.pad(nodes, ((1, 1), (1, 1), (0, 0)))
    send_base = (jnp.arange(BANDS, dtype=jnp.int32) * (BR * (TC + 2)))[:, None]
    recv_base = (jnp.arange(BANDS, dtype=jnp.int32) * (BR * TC))[:, None]
    zero_index = jnp.zeros((), jnp.int32)

    def tile_step(inputs):
        tile_id, edge_block, send_index, recv_index, count_row = inputs
        tile_row = (tile_id // TILES_C).astype(jnp.int32)
        tile_col = (tile_id % TILES_C).astype(jnp.int32)
        window = lax.dynamic_slice(padded, (tile_row * TR, tile_col * TC, zero_index), (TR + 2, TC + 2, latent)).reshape(-1, latent)
        own_nodes = lax.dynamic_slice(nodes, (tile_row * TR, tile_col * TC, zero_index), (TR, TC, latent)).reshape(-1, latent)
        sender_lat = window[(send_index + send_base).reshape(-1)]
        receiver_index = (recv_index + recv_base).reshape(-1).astype(jnp.int32)
        receiver_lat = own_nodes[receiver_index]
        normed = ((edge_block.reshape(-1, latent).astype(jnp.float32) - edge_mean) * inv_spread).astype(jnp.bfloat16)
        joined = jnp.concatenate([normed, sender_lat, receiver_lat], axis=1)
        hidden_one = jax.nn.relu(jnp.dot(joined, w_edge_in, preferred_element_type=jnp.float32) + edge_bias[0]).astype(jnp.bfloat16)
        hidden_two = jax.nn.relu(jnp.dot(hidden_one, w_edge_hid, preferred_element_type=jnp.float32) + edge_bias[1]).astype(jnp.bfloat16)
        message = jnp.dot(hidden_two, w_edge_out, preferred_element_type=jnp.float32) + edge_bias[2]
        live_mask = live_of(count_row).reshape(-1, 1)
        fresh = (live_mask * (normed.astype(jnp.float32) + layer_norm(message) * edge_gain + edge_shift)).astype(jnp.bfloat16)
        gathered = jax.ops.segment_sum(fresh.astype(jnp.float32), receiver_index, num_segments=TR * TC).astype(jnp.bfloat16)
        node_input = jnp.concatenate([own_nodes, gathered], axis=1)
        node_one = jax.nn.relu(jnp.dot(node_input, w_node_in, preferred_element_type=jnp.float32) + node_bias[0]).astype(jnp.bfloat16)
        node_two = jax.nn.relu(jnp.dot(node_one, w_node_hid, preferred_element_type=jnp.float32) + node_bias[1]).astype(jnp.bfloat16)
        node_message = jnp.dot(node_two, w_node_out, preferred_element_type=jnp.float32) + node_bias[2]
        updated = (own_nodes.astype(jnp.float32) + layer_norm(node_message) * node_gain + node_shift).astype(jnp.bfloat16)
        return (fresh.reshape(BANDS, EDGE_SLOTS, latent), updated.reshape(TR, TC, latent))
    tile_ids = jnp.arange(tile_count, dtype=jnp.int32)
    fresh_edges, fresh_tiles = lax.map(tile_step, (tile_ids, flat_edges, flat_send, flat_recv, flat_count))
    new_edges = fresh_edges.reshape(TILES_R, TILES_C, BANDS, EDGE_SLOTS, latent)
    new_nodes = fresh_tiles.reshape(TILES_R, TILES_C, TR, TC, latent).transpose(0, 2, 1, 3, 4).reshape(NR, NC, latent)
    return (new_nodes, new_edges)
```

```python
import functools

import jax
import jax.numpy as jnp
from jax import lax
from jax.experimental import pallas as pl
from jax.experimental.pallas import tpu as pltpu
from jax.sharding import PartitionSpec as P

F32 = jnp.float32
BF16 = jnp.bfloat16
LAT = 128
ROWS = 64
COLS = 32
BANDS = 16
SLOTS = 1024
BAND_NODES = 128
BLK = 256
HALF = BLK // 2
NBLK = SLOTS // BLK
NB = 2
RING = 8
STAGES = 5
TRASH = BANDS * NBLK
WORK = TRASH + NB * (STAGES + 2)
EPS = 1e-5
MESH = pl.DeviceIdType.MESH


def combine(parts):
    n = functools.reduce(jnp.add, [p[0:1] for p in parts])
    weighted = functools.reduce(jnp.add, [p[0:1] * p[1:2] for p in parts])
    mean = weighted / n
    m2 = None
    for p in parts:
        d = p[1:2] - mean
        t = p[2:3] + p[0:1] * d * d
        m2 = t if m2 is None else m2 + t
    return n, mean, m2


def comm_kernel(
    nodes_hbm, edges_hbm, counts, stats_out, halo_out,
    nodes_v, edges_v, cols_v, halo_v, mine1, mine2, got1, got2,
    edge_sem, node_sem, hs_sem, hr_sem, s1_sem, r1_sem, s2_sem, r2_sem,
):
    n_row, n_col = lax.axis_size("row"), lax.axis_size("col")
    row, col = lax.axis_index("row"), lax.axis_index("col")
    up, down = lax.rem(row + n_row - 1, n_row), lax.rem(row + 1, n_row)
    left, right = lax.rem(col + n_col - 1, n_col), lax.rem(col + 1, n_col)

    node_copy = pltpu.make_async_copy(nodes_hbm, nodes_v, node_sem)
    node_copy.start()
    edge_copies = []
    for b in range(BANDS):
        c = pltpu.make_async_copy(
            edges_hbm.at[pl.ds(b * SLOTS, SLOTS)], edges_v.at[pl.ds(b * SLOTS, SLOTS)], edge_sem.at[b]
        )
        c.start()
        edge_copies.append(c)

    barrier = pltpu.get_barrier_semaphore()
    peers = [(row, lax.rem(col + k, n_col)) for k in range(1, n_col)]
    peers += [(lax.rem(row + k, n_row), col) for k in range(1, n_row)]
    peers += [(up, left), (up, right), (down, left), (down, right)]
    for p in peers:
        pl.semaphore_signal(barrier, inc=1, device_id=p, device_id_type=MESH)

    node_copy.wait()
    cols_v[0] = nodes_v[:, 0, :]
    cols_v[1] = nodes_v[:, COLS - 1, :]
    pl.semaphore_wait(barrier, len(peers))

    sends = [
        (nodes_v.at[ROWS - 1], (0, 32), (down, col)),
        (nodes_v.at[0], (32, 32), (up, col)),
        (cols_v.at[1], (64, 64), (row, right)),
        (cols_v.at[0], (128, 64), (row, left)),
        (cols_v.at[1, pl.ds(48, 16)], (192, 16), (down, right)),
        (cols_v.at[0, pl.ds(48, 16)], (208, 16), (down, left)),
        (cols_v.at[1, pl.ds(0, 16)], (224, 16), (up, right)),
        (cols_v.at[0, pl.ds(0, 16)], (240, 16), (up, left)),
    ]
    halo_copies = []
    for k, (src, (start, size), dev) in enumerate(sends):
        c = pltpu.make_async_remote_copy(
            src_ref=src, dst_ref=halo_v.at[pl.ds(start, size)],
            send_sem=hs_sem.at[k], recv_sem=hr_sem.at[k], device_id=dev, device_id_type=MESH,
        )
        c.start()
        halo_copies.append(c)

    edge_copies[0].wait()
    pivot = edges_v[0:16, :].astype(F32)[0:1]
    slot_id = lax.broadcasted_iota(jnp.int32, (64, LAT), 0)

    def band_stats(b, carry):
        s, q = carry
        pltpu.make_async_copy(
            edges_hbm.at[pl.ds(b * SLOTS, SLOTS)], edges_v.at[pl.ds(b * SLOTS, SLOTS)], edge_sem.at[b]
        ).wait()
        return band_sums(b, s, q)

    def band_sums(b, s, q):
        count = counts[0, b]
        for j in range(SLOTS // 64):
            d = edges_v[pl.ds(pl.multiple_of(b * SLOTS + j * 64, 64), 64), :].astype(F32) - pivot
            if j >= SLOTS // 128:
                d = jnp.where(slot_id < count - j * 64, d, 0.0)
            e = d * d
            s = s + ((d[0:8] + d[8:16]) + (d[16:24] + d[24:32])) + ((d[32:40] + d[40:48]) + (d[48:56] + d[56:64]))
            q = q + ((e[0:8] + e[8:16]) + (e[16:24] + e[24:32])) + ((e[32:40] + e[40:48]) + (e[48:56] + e[56:64]))
        return s, q

    zero = jnp.zeros((8, LAT), F32)
    s, q = band_sums(0, zero, zero)
    s, q = lax.fori_loop(1, BANDS, band_stats, (s, q))
    total = counts[0, 0]
    for b in range(1, BANDS):
        total = total + counts[0, b]
    n = jnp.full((1, LAT), total.astype(F32))
    s = jnp.sum(s, axis=0, keepdims=True)
    q = jnp.sum(q, axis=0, keepdims=True)
    local_mean = s / n
    filler = jnp.zeros((5, LAT), F32)
    mine1[...] = jnp.concatenate([n, pivot + local_mean, q - s * local_mean, filler], axis=0)

    copies = []
    for k in range(1, n_col):
        c = pltpu.make_async_remote_copy(
            src_ref=mine1, dst_ref=got1.at[k], send_sem=s1_sem.at[k], recv_sem=r1_sem.at[k],
            device_id=(row, lax.rem(col + k, n_col)), device_id_type=MESH,
        )
        c.start()
        copies.append(c)
    for c in copies:
        c.wait_recv()
    n, mean, m2 = combine([mine1[...]] + [got1[k] for k in range(1, n_col)])
    mine2[...] = jnp.concatenate([n, mean, m2, filler], axis=0)
    copies2 = []
    for k in range(1, n_row):
        c = pltpu.make_async_remote_copy(
            src_ref=mine2, dst_ref=got2.at[k], send_sem=s2_sem.at[k], recv_sem=r2_sem.at[k],
            device_id=(lax.rem(row + k, n_row), col), device_id_type=MESH,
        )
        c.start()
        copies2.append(c)
    for c in halo_copies:
        c.wait_recv()
    halo_out[...] = halo_v[...]
    for c in copies2:
        c.wait_recv()
    n, mean, m2 = combine([mine2[...]] + [got2[k] for k in range(1, n_row)])
    inv = lax.rsqrt(m2 / n + EPS)
    stats_out[...] = jnp.concatenate([mean, inv, jnp.zeros((6, LAT), F32)], axis=0)
    for c in halo_copies + copies + copies2:
        c.wait_send()


def communicate(nodes, edges, counts):
    n_row, n_col = lax.axis_size("row"), lax.axis_size("col")
    any_spec = pl.BlockSpec(memory_space=pl.ANY)
    return pl.pallas_call(
        comm_kernel,
        out_shape=(jax.ShapeDtypeStruct((8, LAT), F32), jax.ShapeDtypeStruct((256, LAT), BF16)),
        in_specs=[any_spec, any_spec, pl.BlockSpec(memory_space=pltpu.SMEM)],
        out_specs=(pl.BlockSpec(memory_space=pltpu.VMEM), pl.BlockSpec(memory_space=pltpu.VMEM)),
        scratch_shapes=[
            pltpu.VMEM((ROWS, COLS, LAT), BF16),
            pltpu.VMEM((BANDS * SLOTS, LAT), BF16),
            pltpu.VMEM((2, ROWS, LAT), BF16),
            pltpu.VMEM((256, LAT), BF16),
            pltpu.VMEM((8, LAT), F32),
            pltpu.VMEM((8, LAT), F32),
            pltpu.VMEM((n_col, 8, LAT), F32),
            pltpu.VMEM((n_row, 8, LAT), F32),
            pltpu.SemaphoreType.DMA((BANDS,)),
            pltpu.SemaphoreType.DMA,
            pltpu.SemaphoreType.DMA((8,)),
            pltpu.SemaphoreType.DMA((8,)),
            pltpu.SemaphoreType.DMA((n_col,)),
            pltpu.SemaphoreType.DMA((n_col,)),
            pltpu.SemaphoreType.DMA((n_row,)),
            pltpu.SemaphoreType.DMA((n_row,)),
        ],
        compiler_params=pltpu.CompilerParams(collective_id=0, has_side_effects=True),
        name="exchange",
    )(nodes, edges, counts)


def dot(a, b):
    return jnp.dot(a, b, preferred_element_type=F32)


def block_diagonal(w):
    z = jnp.zeros_like(w)
    return jnp.concatenate(
        [jnp.concatenate([w, z], axis=1), jnp.concatenate([z, w], axis=1)], axis=0
    )


def twice(v):
    return jnp.concatenate([v, v], axis=1)


def norm_weights(w_out, bias, gain):
    w = w_out.astype(F32)
    w = (w - jnp.mean(w, axis=1, keepdims=True)) * gain
    b = (bias - jnp.mean(bias, axis=1, keepdims=True)) * gain
    weights = jnp.transpose(jnp.broadcast_to(1.0 / (LAT * gain * gain), (LAT, LAT)))
    return w.astype(BF16), b, weights.astype(BF16)


def main_kernel(
    counts, nodes, edges_hbm, senders, receivers, stats, halo,
    w_in, w_hid, w_out, e_bias, e_gain, e_shift,
    wn_in, wn_hid, wn_out, n_bias, n_gain, n_shift,
    new_nodes, edges_out,
    edges_v, out_v, zeros_v, ps_t, pr_t, col_t, lr, sidx, ridx,
    w_hid2, w_out2, w_avg2, vecs, acc, work,
    x_ring, or_ring, oh_s, h1_s, h2_s, cg_s, sq_s,
    in_sem, out_sem,
):
    load = pltpu.make_async_copy(edges_hbm, edges_v.at[pl.ds(0, BANDS * SLOTS)], in_sem)
    load.start()
    zeros_v[...] = jnp.zeros_like(zeros_v)

    place = jnp.int32(0)
    for b in range(BANDS):
        count = counts[0, b]
        for j in range(NBLK):
            work[place + NB * STAGES] = jnp.int32(b * NBLK + j)
            place = place + (count > j * BLK).astype(jnp.int32)
    for k in range(NB * STAGES):
        work[k] = jnp.int32(TRASH)
    for k in range(NB * (STAGES + 2) - NB * STAGES + NB * STAGES):
        work[place + NB * STAGES + k] = jnp.int32(TRASH)

    w_snd, w_rcv = w_in[LAT : 2 * LAT], w_in[2 * LAT :]
    w_both = jnp.concatenate([w_snd, w_rcv], axis=1)
    bias1 = e_bias[0:1]
    for k in range(ROWS * COLS // BLK):
        p = dot(nodes[k * BLK : (k + 1) * BLK], w_both)
        ps_t[COLS + k * BLK : COLS + (k + 1) * BLK] = p[:, :LAT].astype(BF16)
        pr_t[k * BLK : (k + 1) * BLK] = (p[:, LAT:] + bias1).astype(BF16)
    p = dot(halo[...], w_snd)
    ps_t[0:COLS] = p[0:32].astype(BF16)
    ps_t[COLS + ROWS * COLS : 2 * COLS + ROWS * COLS] = p[32:64].astype(BF16)
    lr[0, 64:72] = jnp.zeros((8, LAT), F32)
    lr[1, 64:72] = jnp.zeros((8, LAT), F32)
    lr[0, 1:65] = p[64:128]
    lr[1, 1:65] = p[128:192]
    lr[0, 0:1] = p[207:208]
    lr[1, 0:1] = p[223:224]
    lr[0, 65:66] = p[224:225]
    lr[1, 65:66] = p[240:241]
    for b in range(BANDS):
        pair = jnp.concatenate([lr[0, 4 * b : 4 * b + 8], lr[1, 4 * b : 4 * b + 8]], axis=0)
        col_t[16 * b : 16 * b + 16] = pair.astype(BF16)
    pr_t[ROWS * COLS :] = jnp.zeros((BAND_NODES, LAT), BF16)
    ps_t[2 * COLS + ROWS * COLS :] = jnp.zeros((128, LAT), BF16)
    col_t[16 * BANDS :] = jnp.zeros((16, LAT), BF16)

    s = senders[...]
    r = lax.shift_right_logical(s * 241, 13)
    c = s - r * 34
    place_s = jnp.where(c == 0, 192 + r, jnp.where(c == 33, 200 + r, r * 32 + c - 1)).astype(F32)
    place_r = receivers[...].astype(F32)
    for j in range(NBLK):
        sidx[j, 0:BANDS] = place_s[:, j * BLK : (j + 1) * BLK]
        ridx[j, 0:BANDS] = place_r[:, j * BLK : (j + 1) * BLK]

    w_hid2[...] = block_diagonal(w_hid[...])
    w, b3, avg = norm_weights(w_out[...], e_bias[2:3], e_gain[...])
    w_out2[...] = block_diagonal(w)
    w_avg2[...] = block_diagonal(avg)
    vecs[0:1] = twice(e_bias[1:2])
    vecs[1:2] = twice(b3)
    vecs[2:3] = twice(e_shift[...])
    acc[...] = jnp.zeros_like(acc)

    for b in range(BANDS):
        for j in range(2, NBLK):

            @pl.when(counts[0, b] <= j * BLK)
            def _():
                pltpu.make_async_copy(
                    zeros_v, edges_out.at[pl.ds(b * SLOTS + j * BLK, BLK)], out_sem
                ).start()

    load.wait()

    mean, inv = stats[0:1], stats[1:2]
    node_id = lax.broadcasted_iota(jnp.int32, (256, BLK), 0).astype(F32).astype(BF16)
    one, nought = jnp.ones((), BF16), jnp.zeros((), BF16)

    def item(i, stage, u):
        return work[(i + STAGES - stage) * NB + u]

    def step(i, _):
        for u in range(NB):
            k = item(i, 5, u)
            band = lax.shift_right_logical(k, 2)
            slot = lax.rem(i + RING - 5, RING)
            fresh = out_v[pl.ds(pl.multiple_of(k * BLK, BLK), BLK), :]
            acc[band] += dot(or_ring[slot, u], fresh)
        for u in range(NB):
            k = item(i, 4, u)
            band, j = lax.shift_right_logical(k, 2), lax.rem(k, NBLK)
            slot = lax.rem(i + RING - 4, RING)
            var = dot(sq_s[u], w_avg2[...])
            normed = x_ring[slot, u]
            scaled = cg_s[u] * lax.rsqrt(var + EPS) + vecs[2:3]
            left_count = counts[0, jnp.minimum(band, BANDS - 1)] - j * BLK
            slot_id = lax.broadcasted_iota(jnp.int32, (HALF, LAT), 0)
            for h in range(2):
                v = scaled[:, h * LAT : (h + 1) * LAT] + normed[h * HALF : (h + 1) * HALF].astype(F32)
                v = jnp.where(slot_id < left_count - h * HALF, v, 0.0)
                out_v[pl.ds(pl.multiple_of(k * BLK + h * HALF, HALF), HALF), :] = v.astype(BF16)
        for u in range(NB):
            cg = dot(h2_s[u], w_out2[...]) + vecs[1:2]
            cg_s[u] = cg
            sq_s[u] = (cg * cg).astype(BF16)
        for u in range(NB):
            h2_s[u] = jnp.maximum(dot(h1_s[u], w_hid2[...]) + vecs[0:1], 0.0).astype(BF16)
        for u in range(NB):
            k = item(i, 1, u)
            band = lax.shift_right_logical(k, 2)
            slot = lax.rem(i + RING - 1, RING)
            lhs = jnp.concatenate([x_ring[slot, u], oh_s[u]], axis=1)
            start = pl.multiple_of(band * BAND_NODES, BAND_NODES)
            table = jnp.concatenate(
                [
                    w_in[0:LAT],
                    pr_t[pl.ds(start, BAND_NODES), :],
                    ps_t[pl.ds(start, 192), :],
                    col_t[pl.ds(pl.multiple_of(band * 16, 16), 16), :],
                    jnp.zeros((48, LAT), BF16),
                ],
                axis=0,
            )
            h = jnp.maximum(dot(lhs, table), 0.0).astype(BF16)
            h1_s[u] = jnp.concatenate([h[:HALF], h[HALF:]], axis=1)
        for u in range(NB):
            k = item(i, 0, u)
            band, j = lax.shift_right_logical(k, 2), lax.rem(k, NBLK)
            slot = lax.rem(i, RING)
            x = edges_v[pl.ds(pl.multiple_of(k * BLK, BLK), BLK), :].astype(F32)
            x_ring[slot, u] = ((x - mean) * inv).astype(BF16)
            si = sidx[j, pl.ds(band, 1), :].astype(BF16)
            ri = ridx[j, pl.ds(band, 1), :].astype(BF16)
            pick_s = jnp.where(node_id == si, one, nought)
            pick_r = jnp.where(node_id[:BAND_NODES] == ri, one, nought)
            or_ring[slot, u] = pick_r
            oh_s[u, :, 0:LAT] = pick_r.T
            oh_s[u, :, LAT:] = pick_s.T

        @pl.when(i >= 4)
        def _():
            for u in range(NB):
                k = item(i, 4, u)

                @pl.when(k < TRASH)
                def _():
                    pltpu.make_async_copy(
                        out_v.at[pl.ds(pl.multiple_of(k * BLK, BLK), BLK)],
                        edges_out.at[pl.ds(pl.multiple_of(k * BLK, BLK), BLK)],
                        out_sem,
                    ).start()

        return 0

    lax.fori_loop(0, lax.div(place + (NB - 1), NB) + STAGES, step, 0)

    w, b3, avg = norm_weights(wn_out[...], n_bias[2:3], n_gain[...])
    wh2, wo2, wa2 = block_diagonal(wn_hid[...]), block_diagonal(w), block_diagonal(avg)
    bias2, bias3, shift = twice(n_bias[1:2]), twice(b3), twice(n_shift[...])
    size = 2 * BLK
    for k in range(ROWS * COLS // size):
        own = nodes[k * size : (k + 1) * size]
        gathered = jnp.concatenate([acc[k * 4 + t] for t in range(4)], axis=0).astype(BF16)
        h = dot(jnp.concatenate([own, gathered], axis=1), wn_in[...]) + n_bias[0:1]
        h = jnp.maximum(h, 0.0).astype(BF16)
        h = jnp.concatenate([h[:BLK], h[BLK:]], axis=1)
        h = jnp.maximum(dot(h, wh2) + bias2, 0.0).astype(BF16)
        cg = dot(h, wo2) + bias3
        var = dot((cg * cg).astype(BF16), wa2)
        v = cg * lax.rsqrt(var + EPS) + shift
        new_nodes[k * size : k * size + BLK] = (v[:, :LAT] + own[:BLK].astype(F32)).astype(BF16)
        new_nodes[k * size + BLK : (k + 1) * size] = (v[:, LAT:] + own[BLK:].astype(F32)).astype(BF16)
    pltpu.make_async_copy(out_v.at[pl.ds(0, BANDS * SLOTS)], edges_out, out_sem).wait()


def process(counts, nodes, edges, senders, receivers, stats, halo, *params):
    vmem, smem = pl.BlockSpec(memory_space=pltpu.VMEM), pl.BlockSpec(memory_space=pltpu.SMEM)
    any_spec = pl.BlockSpec(memory_space=pl.ANY)
    return pl.pallas_call(
        main_kernel,
        out_shape=(
            jax.ShapeDtypeStruct((ROWS * COLS, LAT), BF16),
            jax.ShapeDtypeStruct((BANDS * SLOTS, LAT), BF16),
        ),
        in_specs=[smem, vmem, any_spec] + [vmem] * (4 + len(params)),
        out_specs=(vmem, any_spec),
        scratch_shapes=[
            pltpu.VMEM(((TRASH + 1) * BLK, LAT), BF16),
            pltpu.VMEM(((TRASH + 1) * BLK, LAT), BF16),
            pltpu.VMEM((BLK, LAT), BF16),
            pltpu.VMEM((ROWS * COLS + 2 * COLS + 128, LAT), BF16),
            pltpu.VMEM((ROWS * COLS + BAND_NODES, LAT), BF16),
            pltpu.VMEM((16 * (BANDS + 1), LAT), BF16),
            pltpu.VMEM((2, 72, LAT), F32),
            pltpu.VMEM((NBLK, 24, BLK), F32),
            pltpu.VMEM((NBLK, 24, BLK), F32),
            pltpu.VMEM((256, 256), BF16),
            pltpu.VMEM((256, 256), BF16),
            pltpu.VMEM((256, 256), BF16),
            pltpu.VMEM((8, 256), F32),
            pltpu.VMEM((BANDS + 1, BAND_NODES, LAT), F32),
            pltpu.SMEM((WORK + NB * STAGES + 8,), jnp.int32),
            pltpu.VMEM((RING, NB, BLK, LAT), BF16),
            pltpu.VMEM((RING, NB, BAND_NODES, BLK), BF16),
            pltpu.VMEM((NB, BLK, 384), BF16),
            pltpu.VMEM((NB, HALF, 256), BF16),
            pltpu.VMEM((NB, HALF, 256), BF16),
            pltpu.VMEM((NB, HALF, 256), F32),
            pltpu.VMEM((NB, HALF, 256), BF16),
            pltpu.SemaphoreType.DMA,
            pltpu.SemaphoreType.DMA,
        ],
        compiler_params=pltpu.CompilerParams(vmem_limit_bytes=50 * 1024 * 1024),
        name="process",
    )(counts, nodes, edges, senders, receivers, stats, halo, *params)


def per_device(
    nodes, edges, senders, receivers, counts,
    w_edge_in, w_edge_hid, w_edge_out, edge_bias, edge_gain, edge_shift,
    w_node_in, w_node_hid, w_node_out, node_bias, node_gain, node_shift,
):
    flat_edges = edges.reshape(BANDS * SLOTS, LAT)
    count_row = counts.reshape(1, BANDS)
    stats, halo = communicate(nodes, flat_edges, count_row)
    new_nodes, new_edges = process(
        count_row, nodes.reshape(ROWS * COLS, LAT), flat_edges,
        senders.reshape(BANDS, SLOTS), receivers.reshape(BANDS, SLOTS), stats, halo,
        w_edge_in, w_edge_hid, w_edge_out, edge_bias, edge_gain.reshape(1, LAT), edge_shift.reshape(1, LAT),
        w_node_in, w_node_hid, w_node_out, node_bias, node_gain.reshape(1, LAT), node_shift.reshape(1, LAT),
    )
    return new_nodes.reshape(nodes.shape), new_edges.reshape(edges.shape)


def solution(mesh):
    in_specs = (
        P("row", "col", None),
        P("row", "col", None, None, None),
        P("row", "col", None, None),
        P("row", "col", None, None),
        P("row", "col", None),
    ) + (P(),) * 12
    out_specs = (P("row", "col", None), P("row", "col", None, None, None))
    return jax.shard_map(
        per_device, mesh=mesh, in_specs=in_specs, out_specs=out_specs, check_vma=False
    )
```

```python
import functools

import jax
import jax.numpy as jnp
from jax import lax
from jax.experimental import pallas as pl
from jax.experimental.pallas import tpu as pltpu
from jax.sharding import PartitionSpec as P

F32 = jnp.float32
BF16 = jnp.bfloat16
LAT = 128
ROWS = 64
COLS = 32
BANDS = 16
SLOTS = 1024
BAND_NODES = 128
BLK = 256
HALF = BLK // 2
NBLK = SLOTS // BLK
NA = 2
SPLIT = 12
NB = 2
RING = 4
STAGES = 4
TRASH = BANDS * NBLK
EPS = 1e-5
MESH = pl.DeviceIdType.MESH


def combine(parts):
    n = functools.reduce(jnp.add, [p[0:1] for p in parts])
    weighted = functools.reduce(jnp.add, [p[0:1] * p[1:2] for p in parts])
    mean = weighted / n
    m2 = None
    for p in parts:
        d = p[1:2] - mean
        t = p[2:3] + p[0:1] * d * d
        m2 = t if m2 is None else m2 + t
    return n, mean, m2


def dot(a, b):
    return jnp.dot(a, b, preferred_element_type=F32)


def block_diagonal(w):
    z = jnp.zeros_like(w)
    return jnp.concatenate(
        [jnp.concatenate([w, z], axis=1), jnp.concatenate([z, w], axis=1)], axis=0
    )


def twice(v):
    return jnp.concatenate([v, v], axis=1)


def norm_weights(w_out, bias, gain):
    w = w_out.astype(F32)
    w = (w - jnp.mean(w, axis=1, keepdims=True)) * gain
    b = (bias - jnp.mean(bias, axis=1, keepdims=True)) * gain
    weights = jnp.transpose(jnp.broadcast_to(1.0 / (LAT * gain * gain), (LAT, LAT)))
    return w.astype(BF16), b, weights.astype(BF16)


def prepare(hid, out, bias, gain, shift, hid2, out2, avg2, vecs):
    hid2[...] = block_diagonal(hid[...])
    w, b3, avg = norm_weights(out[...], bias[2:3], gain[...])
    out2[...] = block_diagonal(w)
    avg2[...] = block_diagonal(avg)
    vecs[0:1] = twice(bias[1:2])
    vecs[1:2] = twice(b3)
    vecs[2:3] = twice(shift[...])
    vecs[3:4] = twice(bias[0:1])


N_SMALL = 14


def exchange_kernel(*refs):
    nodes_hbm, edges_hbm, counts = refs[:3]
    small_hbm = refs[3 : 3 + N_SMALL]
    (
        stats_out, edges_v, part_v, nodes_v, ridx, w_x2, w_hid2, w_out2, w_avg2, vecs,
        wn_first, wn_hid2, wn_out2, wn_avg2, n_vecs,
    ) = refs[3 + N_SMALL : 18 + N_SMALL]
    small = refs[18 + N_SMALL : 18 + 2 * N_SMALL]
    (
        cols_v, halo_v, mine1, mine2, got1, got2, ps_t, pr_t, col_t, lr, sidx, oh_s,
        edge_sem, node_sem, small_sem, hs_sem, hr_sem, s1_sem, r1_sem, s2_sem, r2_sem,
    ) = refs[18 + 2 * N_SMALL :]
    (
        senders, receivers, w_in, w_hid, w_out, e_bias, e_gain, e_shift,
        wn_in, wn_hid, wn_out, n_bias, n_gain, n_shift,
    ) = small
    n_row, n_col = lax.axis_size("row"), lax.axis_size("col")
    row, col = lax.axis_index("row"), lax.axis_index("col")
    up, down = lax.rem(row + n_row - 1, n_row), lax.rem(row + 1, n_row)
    left, right = lax.rem(col + n_col - 1, n_col), lax.rem(col + 1, n_col)

    barrier = pltpu.get_barrier_semaphore()
    peers = [(row, lax.rem(col + k, n_col)) for k in range(1, n_col)]
    peers += [(lax.rem(row + k, n_row), col) for k in range(1, n_row)]
    peers += [(up, left), (up, right), (down, left), (down, right)]
    for p in peers:
        pl.semaphore_signal(barrier, inc=1, device_id=p, device_id_type=MESH)

    def edge_copy(b):
        return pltpu.make_async_copy(
            edges_hbm.at[pl.ds(b * SLOTS, SLOTS)], edges_v.at[pl.ds(b * SLOTS, SLOTS)], edge_sem.at[b]
        )

    node_copy = pltpu.make_async_copy(nodes_hbm, nodes_v, node_sem)
    for b in range(4):
        edge_copy(b).start()
    node_copy.start()
    for b in range(4, BANDS):
        edge_copy(b).start()
    small_copies = [
        pltpu.make_async_copy(src, dst, small_sem.at[k])
        for k, (src, dst) in enumerate(zip(small_hbm, small))
    ]
    for c in small_copies:
        c.start()

    edge_copy(0).wait()
    pivot = edges_v[0:16, :].astype(F32)[0:1]
    slot_id = lax.broadcasted_iota(jnp.int32, (64, LAT), 0)

    def band_sums(b, s, q):
        count = counts[0, b]
        for j in range(SLOTS // 64):
            d = edges_v[pl.ds(pl.multiple_of(b * SLOTS + j * 64, 64), 64), :].astype(F32) - pivot
            if j >= SLOTS // 128:
                d = jnp.where(slot_id < count - j * 64, d, 0.0)
            e = d * d
            s = s + ((d[0:8] + d[8:16]) + (d[16:24] + d[24:32])) + ((d[32:40] + d[40:48]) + (d[48:56] + d[56:64]))
            q = q + ((e[0:8] + e[8:16]) + (e[16:24] + e[24:32])) + ((e[32:40] + e[40:48]) + (e[48:56] + e[56:64]))
        return s, q

    def band_stats(b, carry):
        edge_copy(b).wait()
        return band_sums(b, *carry)

    zero = jnp.zeros((8, LAT), F32)
    carry = band_sums(0, zero, zero)
    carry = lax.fori_loop(1, 8, band_stats, carry)

    node_copy.wait()
    cols_v[0] = nodes_v[:, 0, :]
    cols_v[1] = nodes_v[:, COLS - 1, :]
    pl.semaphore_wait(barrier, len(peers))

    sends = [
        (nodes_v.at[ROWS - 1], (0, 32), (down, col)),
        (nodes_v.at[0], (32, 32), (up, col)),
        (cols_v.at[1], (64, 64), (row, right)),
        (cols_v.at[0], (128, 64), (row, left)),
        (cols_v.at[1, pl.ds(48, 16)], (192, 16), (down, right)),
        (cols_v.at[0, pl.ds(48, 16)], (208, 16), (down, left)),
        (cols_v.at[1, pl.ds(0, 16)], (224, 16), (up, right)),
        (cols_v.at[0, pl.ds(0, 16)], (240, 16), (up, left)),
    ]
    halo_copies = []
    for k, (src, (start, size), dev) in enumerate(sends):
        c = pltpu.make_async_remote_copy(
            src_ref=src, dst_ref=halo_v.at[pl.ds(start, size)],
            send_sem=hs_sem.at[k], recv_sem=hr_sem.at[k], device_id=dev, device_id_type=MESH,
        )
        c.start()
        halo_copies.append(c)

    s, q = lax.fori_loop(8, BANDS, band_stats, carry)
    total = counts[0, 0]
    for b in range(1, BANDS):
        total = total + counts[0, b]
    n = jnp.full((1, LAT), total.astype(F32))
    s = jnp.sum(s, axis=0, keepdims=True)
    q = jnp.sum(q, axis=0, keepdims=True)
    local_mean = s / n
    filler = jnp.zeros((5, LAT), F32)
    mine1[...] = jnp.concatenate([n, pivot + local_mean, q - s * local_mean, filler], axis=0)

    copies = []
    for k in range(1, n_col):
        c = pltpu.make_async_remote_copy(
            src_ref=mine1, dst_ref=got1.at[k], send_sem=s1_sem.at[k], recv_sem=r1_sem.at[k],
            device_id=(row, lax.rem(col + k, n_col)), device_id_type=MESH,
        )
        c.start()
        copies.append(c)

    for c in small_copies:
        c.wait()
    w_snd, w_rcv = w_in[LAT : 2 * LAT], w_in[2 * LAT :]
    w_both = jnp.concatenate([w_snd, w_rcv], axis=1)
    bias1 = e_bias[0:1]
    for k in range(ROWS * COLS // BLK):
        own = nodes_v[k * 8 : (k + 1) * 8].reshape(BLK, LAT)
        p = dot(own, w_both)
        ps_t[COLS + k * BLK : COLS + (k + 1) * BLK] = p[:, :LAT].astype(BF16)
        pr_t[k * BLK : (k + 1) * BLK] = (p[:, LAT:] + bias1).astype(BF16)

    s = senders[...]
    r = lax.shift_right_logical(s * 241, 13)
    c = s - r * 34
    place_s = jnp.where(c == 0, 192 + r, jnp.where(c == 33, 200 + r, r * 32 + c - 1)).astype(F32)
    place_r = receivers[...].astype(F32)
    for j in range(NBLK):
        sidx[j, 0:BANDS] = place_s[:, j * BLK : (j + 1) * BLK]
        ridx[j, 0:BANDS] = place_r[:, j * BLK : (j + 1) * BLK]

    w_x2[...] = block_diagonal(w_in[0:LAT])
    prepare(w_hid, w_out, e_bias, e_gain, e_shift, w_hid2, w_out2, w_avg2, vecs)

    node_id = lax.broadcasted_iota(jnp.int32, (256, BLK), 0).astype(F32).astype(BF16)
    one, nought = jnp.ones((), BF16), jnp.zeros((), BF16)

    def one_hot(i):
        for u in range(NA):
            k = i * NA + u
            band, j = lax.div(k, NBLK), lax.rem(k, NBLK)
            si = sidx[j, pl.ds(band, 1), :].astype(BF16)
            ri = ridx[j, pl.ds(band, 1), :].astype(BF16)
            pick_s = jnp.where(node_id == si, one, nought)
            pick_r = jnp.where(node_id[:BAND_NODES] == ri, one, nought)
            oh_s[u, :, 0:LAT] = pick_r.T
            oh_s[u, :, LAT:] = pick_s.T

    def gather(i):
        for u in range(NA):
            k = i * NA + u
            band = lax.div(k, NBLK)
            start = pl.multiple_of(band * BAND_NODES, BAND_NODES)
            table = jnp.concatenate(
                [
                    pr_t[pl.ds(start, BAND_NODES), :],
                    ps_t[pl.ds(start, 192), :],
                    col_t[pl.ds(pl.multiple_of(band * 16, 16), 16), :],
                    jnp.zeros((48, LAT), BF16),
                ],
                axis=0,
            )
            part_v[pl.ds(pl.multiple_of(k * BLK, BLK), BLK), :] = dot(oh_s[u], table)

    one_hot(0)
    for c in halo_copies:
        c.wait_recv()
    p = dot(halo_v[...], w_snd)
    ps_t[0:COLS] = p[0:32].astype(BF16)
    ps_t[COLS + ROWS * COLS :] = p[32:64].astype(BF16)
    lr[0, 64:72] = jnp.zeros((8, LAT), F32)
    lr[1, 64:72] = jnp.zeros((8, LAT), F32)
    lr[0, 1:65] = p[64:128]
    lr[1, 1:65] = p[128:192]
    lr[0, 0:1] = p[207:208]
    lr[1, 0:1] = p[223:224]
    lr[0, 65:66] = p[224:225]
    lr[1, 65:66] = p[240:241]
    for b in range(BANDS):
        pair = jnp.concatenate([lr[0, 4 * b : 4 * b + 8], lr[1, 4 * b : 4 * b + 8]], axis=0)
        col_t[16 * b : 16 * b + 16] = pair.astype(BF16)

    last = TRASH // NA - 1

    def step(i, _):
        gather(i)
        one_hot(jnp.minimum(i + 1, last))
        return 0

    lax.fori_loop(0, SPLIT, step, 0)
    for c in copies:
        c.wait_recv()
    n, mean, m2 = combine([mine1[...]] + [got1[k] for k in range(1, n_col)])
    mine2[...] = jnp.concatenate([n, mean, m2, filler], axis=0)
    copies2 = []
    for k in range(1, n_row):
        c = pltpu.make_async_remote_copy(
            src_ref=mine2, dst_ref=got2.at[k], send_sem=s2_sem.at[k], recv_sem=r2_sem.at[k],
            device_id=(lax.rem(row + k, n_row), col), device_id_type=MESH,
        )
        c.start()
        copies2.append(c)
    wn_first[...] = wn_in[...]
    prepare(wn_hid, wn_out, n_bias, n_gain, n_shift, wn_hid2, wn_out2, wn_avg2, n_vecs)
    lax.fori_loop(SPLIT, last + 1, step, 0)
    for c in copies2:
        c.wait_recv()
    n, mean, m2 = combine([mine2[...]] + [got2[k] for k in range(1, n_row)])
    inv = lax.rsqrt(m2 / n + EPS)
    stats_out[...] = jnp.concatenate([mean, inv, jnp.zeros((6, LAT), F32)], axis=0)
    for c in halo_copies + copies + copies2:
        c.wait_send()


def exchange(nodes, edges, counts, *small):
    n_row, n_col = lax.axis_size("row"), lax.axis_size("col")
    hbm, vmem = pl.BlockSpec(memory_space=pltpu.HBM), pl.BlockSpec(memory_space=pltpu.VMEM)
    pin = lambda a: pltpu.with_memory_space_constraint(a, pltpu.HBM)
    square = pltpu.VMEM((256, 256), BF16)
    outs = (
        pltpu.VMEM((8, LAT), F32),
        pltpu.VMEM(((TRASH + 1) * BLK, LAT), BF16),
        pltpu.VMEM(((TRASH + 1) * BLK, LAT), F32),
        pltpu.VMEM((ROWS, COLS, LAT), BF16),
        pltpu.VMEM((NBLK, 24, BLK), F32),
        square, square, square, square, pltpu.VMEM((8, 256), F32),
        pltpu.VMEM((2 * LAT, LAT), BF16), square, square, square, pltpu.VMEM((8, 256), F32),
    )
    return pl.pallas_call(
        exchange_kernel,
        out_shape=outs,
        in_specs=[hbm, hbm, pl.BlockSpec(memory_space=pltpu.SMEM)] + [hbm] * N_SMALL,
        out_specs=(vmem,) * len(outs),
        scratch_shapes=[pltpu.VMEM(a.shape, a.dtype) for a in small]
        + [
            pltpu.VMEM((2, ROWS, LAT), BF16),
            pltpu.VMEM((256, LAT), BF16),
            pltpu.VMEM((8, LAT), F32),
            pltpu.VMEM((8, LAT), F32),
            pltpu.VMEM((n_col, 8, LAT), F32),
            pltpu.VMEM((n_row, 8, LAT), F32),
            pltpu.VMEM((ROWS * COLS + 2 * COLS, LAT), BF16),
            pltpu.VMEM((ROWS * COLS, LAT), BF16),
            pltpu.VMEM((16 * BANDS, LAT), BF16),
            pltpu.VMEM((2, 72, LAT), F32),
            pltpu.VMEM((NBLK, 24, BLK), F32),
            pltpu.VMEM((NA, BLK, 384), BF16),
            pltpu.SemaphoreType.DMA((BANDS,)),
            pltpu.SemaphoreType.DMA,
            pltpu.SemaphoreType.DMA((N_SMALL,)),
            pltpu.SemaphoreType.DMA((8,)),
            pltpu.SemaphoreType.DMA((8,)),
            pltpu.SemaphoreType.DMA((n_col,)),
            pltpu.SemaphoreType.DMA((n_col,)),
            pltpu.SemaphoreType.DMA((n_row,)),
            pltpu.SemaphoreType.DMA((n_row,)),
        ],
        compiler_params=pltpu.CompilerParams(
            collective_id=0, has_side_effects=True, vmem_limit_bytes=32 * 1024 * 1024
        ),
        name="exchange",
    )(pin(nodes), pin(edges), counts, *[pin(a) for a in small])


def main_kernel(
    counts, stats, edges_v, part_v, nodes, ridx, w_x2, w_hid2, w_out2, w_avg2, vecs,
    wn_in, wn_hid2, wn_out2, wn_avg2, n_vecs,
    new_nodes, edges_out,
    out_v, zeros_v, acc, work, x_ring, h1_s, h2_s, cg_s, sq_s, out_sem,
):
    zeros_v[...] = jnp.zeros_like(zeros_v)

    place = jnp.int32(0)
    for b in range(BANDS):
        count = counts[0, b]
        for j in range(NBLK):
            work[place + NB * STAGES] = jnp.int32(b * NBLK + j)
            place = place + (count > j * BLK).astype(jnp.int32)
    for k in range(NB * STAGES):
        work[k] = jnp.int32(TRASH)
    for k in range(NB * (STAGES + 1)):
        work[place + NB * STAGES + k] = jnp.int32(TRASH)
    acc[...] = jnp.zeros_like(acc)
    for b in range(BANDS):
        for j in range(2, NBLK):

            @pl.when(counts[0, b] <= j * BLK)
            def _():
                pltpu.make_async_copy(
                    zeros_v, edges_out.at[pl.ds(b * SLOTS + j * BLK, BLK)], out_sem
                ).start()

    mean, inv = stats[0:1], stats[1:2]
    node_id = lax.broadcasted_iota(jnp.int32, (BAND_NODES, BLK), 0).astype(F32).astype(BF16)
    one, nought = jnp.ones((), BF16), jnp.zeros((), BF16)

    def item(i, stage, u):
        return work[(i + STAGES - stage) * NB + u]

    def step(i, _):
        for u in range(NB):
            k = item(i, 4, u)
            band, j = lax.shift_right_logical(k, 2), lax.rem(k, NBLK)
            fresh = out_v[pl.ds(pl.multiple_of(k * BLK, BLK), BLK), :]
            ri = ridx[j, pl.ds(band, 1), :].astype(BF16)
            acc[band] += dot(jnp.where(node_id == ri, one, nought), fresh)
        for u in range(NB):
            k = item(i, 3, u)
            band, j = lax.shift_right_logical(k, 2), lax.rem(k, NBLK)
            slot = lax.rem(i + RING - 3, RING)
            var = dot(sq_s[u], w_avg2[...])
            scaled = cg_s[u] * lax.rsqrt(var + EPS) + vecs[2:3] + x_ring[slot, u].astype(F32)
            left_count = counts[0, jnp.minimum(band, BANDS - 1)] - j * BLK
            slot_id = lax.broadcasted_iota(jnp.int32, (HALF, LAT), 0)
            for h in range(2):
                v = jnp.where(slot_id < left_count - h * HALF, scaled[:, h * LAT : (h + 1) * LAT], 0.0)
                out_v[pl.ds(pl.multiple_of(k * BLK + h * HALF, HALF), HALF), :] = v.astype(BF16)
        for u in range(NB):
            cg = dot(h2_s[u], w_out2[...]) + vecs[1:2]
            cg_s[u] = cg
            sq_s[u] = (cg * cg).astype(BF16)
        for u in range(NB):
            h2_s[u] = jnp.maximum(dot(h1_s[u], w_hid2[...]) + vecs[0:1], 0.0).astype(BF16)
        for u in range(NB):
            k = item(i, 0, u)
            halves, parts = [], []
            for h in range(2):
                here = pl.ds(pl.multiple_of(k * BLK + h * HALF, HALF), HALF)
                halves.append(((edges_v[here, :].astype(F32) - mean) * inv).astype(BF16))
                parts.append(part_v[here, :])
            x = jnp.concatenate(halves, axis=1)
            x_ring[lax.rem(i, RING), u] = x
            h1 = dot(x, w_x2[...]) + jnp.concatenate(parts, axis=1)
            h1_s[u] = jnp.maximum(h1, 0.0).astype(BF16)

        @pl.when(i >= 3)
        def _():
            for u in range(NB):
                k = item(i, 3, u)

                @pl.when(k < TRASH)
                def _():
                    pltpu.make_async_copy(
                        out_v.at[pl.ds(pl.multiple_of(k * BLK, BLK), BLK)],
                        edges_out.at[pl.ds(pl.multiple_of(k * BLK, BLK), BLK)],
                        out_sem,
                    ).start()

        return 0

    lax.fori_loop(0, lax.div(place + (NB - 1), NB) + STAGES, step, 0)

    size = 2 * BLK
    for k in range(ROWS * COLS // size):
        own = nodes[k * 16 : (k + 1) * 16].reshape(size, LAT)
        gathered = jnp.concatenate([acc[k * 4 + t] for t in range(4)], axis=0).astype(BF16)
        h = dot(jnp.concatenate([own, gathered], axis=1), wn_in[...]) + n_vecs[3:4, 0:LAT]
        h = jnp.maximum(h, 0.0).astype(BF16)
        h = jnp.concatenate([h[:BLK], h[BLK:]], axis=1)
        h = jnp.maximum(dot(h, wn_hid2[...]) + n_vecs[0:1], 0.0).astype(BF16)
        cg = dot(h, wn_out2[...]) + n_vecs[1:2]
        var = dot((cg * cg).astype(BF16), wn_avg2[...])
        v = cg * lax.rsqrt(var + EPS) + n_vecs[2:3]
        new_nodes[k * size : k * size + BLK] = (v[:, :LAT] + own[:BLK].astype(F32)).astype(BF16)
        new_nodes[k * size + BLK : (k + 1) * size] = (v[:, LAT:] + own[BLK:].astype(F32)).astype(BF16)
    pltpu.make_async_copy(out_v.at[pl.ds(0, BANDS * SLOTS)], edges_out, out_sem).wait()


def process(counts, *held):
    vmem, smem = pl.BlockSpec(memory_space=pltpu.VMEM), pl.BlockSpec(memory_space=pltpu.SMEM)
    pin = lambda a: pltpu.with_memory_space_constraint(a, pltpu.VMEM)
    return pl.pallas_call(
        main_kernel,
        out_shape=(
            jax.ShapeDtypeStruct((ROWS * COLS, LAT), BF16),
            jax.ShapeDtypeStruct((BANDS * SLOTS, LAT), BF16),
        ),
        in_specs=[smem] + [vmem] * len(held),
        out_specs=(vmem, pl.BlockSpec(memory_space=pl.ANY)),
        scratch_shapes=[
            pltpu.VMEM(((TRASH + 1) * BLK, LAT), BF16),
            pltpu.VMEM((BLK, LAT), BF16),
            pltpu.VMEM((BANDS + 1, BAND_NODES, LAT), F32),
            pltpu.SMEM((TRASH + NB * (2 * STAGES + 2),), jnp.int32),
            pltpu.VMEM((RING, NB, HALF, 256), BF16),
            pltpu.VMEM((NB, HALF, 256), BF16),
            pltpu.VMEM((NB, HALF, 256), BF16),
            pltpu.VMEM((NB, HALF, 256), F32),
            pltpu.VMEM((NB, HALF, 256), BF16),
            pltpu.SemaphoreType.DMA,
        ],
        compiler_params=pltpu.CompilerParams(vmem_limit_bytes=32 * 1024 * 1024),
        name="process",
    )(counts, *[pin(a) for a in held])


def per_device(
    nodes, edges, senders, receivers, counts,
    w_edge_in, w_edge_hid, w_edge_out, edge_bias, edge_gain, edge_shift,
    w_node_in, w_node_hid, w_node_out, node_bias, node_gain, node_shift,
):
    flat_edges = edges.reshape(BANDS * SLOTS, LAT)
    count_row = counts.reshape(1, BANDS)
    held = exchange(
        nodes, flat_edges, count_row, senders.reshape(BANDS, SLOTS), receivers.reshape(BANDS, SLOTS),
        w_edge_in, w_edge_hid, w_edge_out, edge_bias, edge_gain.reshape(1, LAT), edge_shift.reshape(1, LAT),
        w_node_in, w_node_hid, w_node_out, node_bias, node_gain.reshape(1, LAT), node_shift.reshape(1, LAT),
    )
    new_nodes, new_edges = process(count_row, *held)
    return new_nodes.reshape(nodes.shape), new_edges.reshape(edges.shape)


def solution(mesh):
    in_specs = (
        P("row", "col", None),
        P("row", "col", None, None, None),
        P("row", "col", None, None),
        P("row", "col", None, None),
        P("row", "col", None),
    ) + (P(),) * 12
    out_specs = (P("row", "col", None), P("row", "col", None, None, None))
    return jax.shard_map(
        per_device, mesh=mesh, in_specs=in_specs, out_specs=out_specs, check_vma=False
    )
```

```python
import functools

import jax
import jax.numpy as jnp
from jax import lax
from jax.experimental import pallas as pl
from jax.experimental.pallas import tpu as pltpu
from jax.sharding import PartitionSpec as P

F32 = jnp.float32
BF16 = jnp.bfloat16
LAT = 128
ROWS = 64
COLS = 32
BANDS = 16
SLOTS = 1024
BAND_NODES = 128
BLK = 256
HALF = BLK // 2
NBLK = SLOTS // BLK
NA = 4
SPLIT = 8
NB = 4
RING = 2
STAGES = 2
TRASH = BANDS * NBLK
EPS = 1e-5
MESH = pl.DeviceIdType.MESH


def combine(parts):
    n = functools.reduce(jnp.add, [p[0:1] for p in parts])
    weighted = functools.reduce(jnp.add, [p[0:1] * p[1:2] for p in parts])
    mean = weighted / n
    m2 = None
    for p in parts:
        d = p[1:2] - mean
        t = p[2:3] + p[0:1] * d * d
        m2 = t if m2 is None else m2 + t
    return n, mean, m2


def dot(a, b):
    return jnp.dot(a, b, preferred_element_type=F32)


def block_diagonal(w):
    z = jnp.zeros_like(w)
    return jnp.concatenate(
        [jnp.concatenate([w, z], axis=1), jnp.concatenate([z, w], axis=1)], axis=0
    )


def twice(v):
    return jnp.concatenate([v, v], axis=1)


def norm_weights(w_out, bias, gain):
    w = w_out.astype(F32)
    w = (w - jnp.mean(w, axis=1, keepdims=True)) * gain
    b = (bias - jnp.mean(bias, axis=1, keepdims=True)) * gain
    weights = jnp.transpose(jnp.broadcast_to(1.0 / (LAT * gain * gain), (LAT, LAT)))
    return w.astype(BF16), b, weights.astype(BF16)


def prepare(hid, out, bias, gain, shift, hid2, out2, avg2, vecs):
    hid2[...] = block_diagonal(hid[...])
    w, b3, avg = norm_weights(out[...], bias[2:3], gain[...])
    out2[...] = block_diagonal(w)
    avg2[...] = block_diagonal(avg)
    vecs[0:1] = twice(bias[1:2])
    vecs[1:2] = twice(b3)
    vecs[2:3] = twice(shift[...])
    vecs[3:4] = twice(bias[0:1])


N_SMALL = 14


def exchange_kernel(*refs):
    nodes_hbm, edges_hbm, counts_hbm = refs[:3]
    small_hbm = refs[3 : 3 + N_SMALL]
    (
        stats_out, edges_v, part_v, nodes_v, ridx, w_x2, w_hid2, w_out2, w_avg2, vecs,
        wn_first, wn_hid2, wn_out2, wn_avg2, n_vecs,
    ) = refs[3 + N_SMALL : 18 + N_SMALL]
    small = refs[18 + N_SMALL : 18 + 2 * N_SMALL]
    (
        cols_v, halo_v, mine1, mine2, got1, got2, ps_t, pr_t, col_t, lr, sidx, oh_s, counts,
        count_sem, edge_sem, node_sem, small_sem, hs_sem, hr_sem, s1_sem, r1_sem, s2_sem, r2_sem,
    ) = refs[18 + 2 * N_SMALL :]
    (
        senders, receivers, w_in, w_hid, w_out, e_bias, e_gain, e_shift,
        wn_in, wn_hid, wn_out, n_bias, n_gain, n_shift,
    ) = small
    n_row, n_col = lax.axis_size("row"), lax.axis_size("col")
    row, col = lax.axis_index("row"), lax.axis_index("col")
    up, down = lax.rem(row + n_row - 1, n_row), lax.rem(row + 1, n_row)
    left, right = lax.rem(col + n_col - 1, n_col), lax.rem(col + 1, n_col)

    barrier = pltpu.get_barrier_semaphore()
    peers = [(row, lax.rem(col + k, n_col)) for k in range(1, n_col)]
    peers += [(lax.rem(row + k, n_row), col) for k in range(1, n_row)]
    peers += [(up, left), (up, right), (down, left), (down, right)]
    for p in peers:
        pl.semaphore_signal(barrier, inc=1, device_id=p, device_id_type=MESH)

    def edge_copy(b):
        return pltpu.make_async_copy(
            edges_hbm.at[pl.ds(b * SLOTS, SLOTS)], edges_v.at[pl.ds(b * SLOTS, SLOTS)], edge_sem.at[b]
        )

    count_copy = pltpu.make_async_copy(counts_hbm, counts, count_sem)
    count_copy.start()
    node_copy = pltpu.make_async_copy(nodes_hbm, nodes_v, node_sem)
    for b in range(BANDS):
        edge_copy(b).start()
    node_copy.start()
    small_copies = [
        pltpu.make_async_copy(src, dst, small_sem.at[k])
        for k, (src, dst) in enumerate(zip(small_hbm, small))
    ]
    for c in small_copies:
        c.start()

    count_copy.wait()
    edge_copy(0).wait()
    pivot = edges_v[0:16, :].astype(F32)[0:1]
    slot_id = lax.broadcasted_iota(jnp.int32, (64, LAT), 0)

    def band_sums(b, s, q):
        count = counts[0, b]
        for j in range(SLOTS // 64):
            d = edges_v[pl.ds(pl.multiple_of(b * SLOTS + j * 64, 64), 64), :].astype(F32) - pivot
            if j >= SLOTS // 128:
                d = jnp.where(slot_id < count - j * 64, d, 0.0)
            e = d * d
            s = s + ((d[0:8] + d[8:16]) + (d[16:24] + d[24:32])) + ((d[32:40] + d[40:48]) + (d[48:56] + d[56:64]))
            q = q + ((e[0:8] + e[8:16]) + (e[16:24] + e[24:32])) + ((e[32:40] + e[40:48]) + (e[48:56] + e[56:64]))
        return s, q

    def band_stats(b, carry):
        edge_copy(b).wait()
        return band_sums(b, *carry)

    zero = jnp.zeros((8, LAT), F32)
    carry = band_sums(0, zero, zero)
    s, q = lax.fori_loop(1, BANDS, band_stats, carry)
    total = counts[0, 0]
    for b in range(1, BANDS):
        total = total + counts[0, b]
    n = jnp.full((1, LAT), total.astype(F32))
    s = jnp.sum(s, axis=0, keepdims=True)
    q = jnp.sum(q, axis=0, keepdims=True)
    local_mean = s / n
    filler = jnp.zeros((5, LAT), F32)
    mine1[...] = jnp.concatenate([n, pivot + local_mean, q - s * local_mean, filler], axis=0)

    node_copy.wait()
    cols_v[0] = nodes_v[:, 0, :]
    cols_v[1] = nodes_v[:, COLS - 1, :]
    pl.semaphore_wait(barrier, len(peers))
    copies = []
    for k in range(1, n_col):
        c = pltpu.make_async_remote_copy(
            src_ref=mine1, dst_ref=got1.at[k], send_sem=s1_sem.at[k], recv_sem=r1_sem.at[k],
            device_id=(row, lax.rem(col + k, n_col)), device_id_type=MESH,
        )
        c.start()
        copies.append(c)

    sends = [
        (nodes_v.at[ROWS - 1], (0, 32), (down, col)),
        (nodes_v.at[0], (32, 32), (up, col)),
        (cols_v.at[1], (64, 64), (row, right)),
        (cols_v.at[0], (128, 64), (row, left)),
        (cols_v.at[1, pl.ds(48, 16)], (192, 16), (down, right)),
        (cols_v.at[0, pl.ds(48, 16)], (208, 16), (down, left)),
        (cols_v.at[1, pl.ds(0, 16)], (224, 16), (up, right)),
        (cols_v.at[0, pl.ds(0, 16)], (240, 16), (up, left)),
    ]
    halo_copies = []
    for k, (src, (start, size), dev) in enumerate(sends):
        c = pltpu.make_async_remote_copy(
            src_ref=src, dst_ref=halo_v.at[pl.ds(start, size)],
            send_sem=hs_sem.at[k], recv_sem=hr_sem.at[k], device_id=dev, device_id_type=MESH,
        )
        c.start()
        halo_copies.append(c)

    for c in small_copies:
        c.wait()
    w_snd, w_rcv = w_in[LAT : 2 * LAT], w_in[2 * LAT :]
    w_both = jnp.concatenate([w_snd, w_rcv], axis=1)
    bias1 = e_bias[0:1]
    for k in range(ROWS * COLS // BLK):
        own = nodes_v[k * 8 : (k + 1) * 8].reshape(BLK, LAT)
        p = dot(own, w_both)
        ps_t[COLS + k * BLK : COLS + (k + 1) * BLK] = p[:, :LAT].astype(BF16)
        pr_t[k * BLK : (k + 1) * BLK] = (p[:, LAT:] + bias1).astype(BF16)

    s = senders[...]
    r = lax.shift_right_logical(s * 241, 13)
    c = s - r * 34
    place_s = jnp.where(c == 0, 192 + r, jnp.where(c == 33, 200 + r, r * 32 + c - 1)).astype(F32)
    place_r = receivers[...].astype(F32)
    for j in range(NBLK):
        sidx[j, 0:BANDS] = place_s[:, j * BLK : (j + 1) * BLK]
        ridx[j, 0:BANDS] = place_r[:, j * BLK : (j + 1) * BLK]

    w_x2[...] = block_diagonal(w_in[0:LAT])
    prepare(w_hid, w_out, e_bias, e_gain, e_shift, w_hid2, w_out2, w_avg2, vecs)

    node_id = lax.broadcasted_iota(jnp.int32, (256, BLK), 0).astype(F32).astype(BF16)
    one, nought = jnp.ones((), BF16), jnp.zeros((), BF16)

    def one_hot(i):
        for u in range(NA):
            k = i * NA + u
            band, j = lax.div(k, NBLK), lax.rem(k, NBLK)
            si = sidx[j, pl.ds(band, 1), :].astype(BF16)
            ri = ridx[j, pl.ds(band, 1), :].astype(BF16)
            pick_s = jnp.where(node_id == si, one, nought)
            pick_r = jnp.where(node_id[:BAND_NODES] == ri, one, nought)
            oh_s[k, :, 0:LAT] = pick_r.T
            oh_s[k, :, LAT:] = pick_s.T

    def gather(i):
        for u in range(NA):
            k = i * NA + u
            band = lax.div(k, NBLK)
            start = pl.multiple_of(band * BAND_NODES, BAND_NODES)
            table = jnp.concatenate(
                [
                    pr_t[pl.ds(start, BAND_NODES), :],
                    ps_t[pl.ds(start, 192), :],
                    col_t[pl.ds(pl.multiple_of(band * 16, 16), 16), :],
                    jnp.zeros((48, LAT), BF16),
                ],
                axis=0,
            )
            part_v[pl.ds(pl.multiple_of(k * BLK, BLK), BLK), :] = dot(oh_s[k], table)

    def one_hot_step(i, _):
        one_hot(i)
        return 0

    last = TRASH // NA
    lax.fori_loop(0, last, one_hot_step, 0)
    for c in halo_copies:
        c.wait_recv()
    p = dot(halo_v[...], w_snd)
    ps_t[0:COLS] = p[0:32].astype(BF16)
    ps_t[COLS + ROWS * COLS :] = p[32:64].astype(BF16)
    lr[0, 64:72] = jnp.zeros((8, LAT), F32)
    lr[1, 64:72] = jnp.zeros((8, LAT), F32)
    lr[0, 1:65] = p[64:128]
    lr[1, 1:65] = p[128:192]
    lr[0, 0:1] = p[207:208]
    lr[1, 0:1] = p[223:224]
    lr[0, 65:66] = p[224:225]
    lr[1, 65:66] = p[240:241]
    for b in range(BANDS):
        pair = jnp.concatenate([lr[0, 4 * b : 4 * b + 8], lr[1, 4 * b : 4 * b + 8]], axis=0)
        col_t[16 * b : 16 * b + 16] = pair.astype(BF16)

    def step(i, _):
        gather(i)
        return 0

    lax.fori_loop(0, SPLIT, step, 0)
    for c in copies:
        c.wait_recv()
    n, mean, m2 = combine([mine1[...]] + [got1[k] for k in range(1, n_col)])
    mine2[...] = jnp.concatenate([n, mean, m2, filler], axis=0)
    copies2 = []
    for k in range(1, n_row):
        c = pltpu.make_async_remote_copy(
            src_ref=mine2, dst_ref=got2.at[k], send_sem=s2_sem.at[k], recv_sem=r2_sem.at[k],
            device_id=(lax.rem(row + k, n_row), col), device_id_type=MESH,
        )
        c.start()
        copies2.append(c)
    wn_first[...] = wn_in[...]
    prepare(wn_hid, wn_out, n_bias, n_gain, n_shift, wn_hid2, wn_out2, wn_avg2, n_vecs)
    lax.fori_loop(SPLIT, last, step, 0)
    for c in copies2:
        c.wait_recv()
    n, mean, m2 = combine([mine2[...]] + [got2[k] for k in range(1, n_row)])
    inv = lax.rsqrt(m2 / n + EPS)
    stats_out[...] = jnp.concatenate([mean, inv, jnp.zeros((6, LAT), F32)], axis=0)
    for c in halo_copies + copies + copies2:
        c.wait_send()


def exchange(nodes, edges, counts, *small):
    n_row, n_col = lax.axis_size("row"), lax.axis_size("col")
    hbm, vmem = pl.BlockSpec(memory_space=pltpu.HBM), pl.BlockSpec(memory_space=pltpu.VMEM)
    pin = lambda a: pltpu.with_memory_space_constraint(a, pltpu.HBM)
    square = pltpu.VMEM((256, 256), BF16)
    outs = (
        pltpu.VMEM((8, LAT), F32),
        pltpu.VMEM(((TRASH + 1) * BLK, LAT), BF16),
        pltpu.VMEM(((TRASH + 1) * BLK, LAT), F32),
        pltpu.VMEM((ROWS, COLS, LAT), BF16),
        pltpu.VMEM((NBLK, 24, BLK), F32),
        square, square, square, square, pltpu.VMEM((8, 256), F32),
        pltpu.VMEM((2 * LAT, LAT), BF16), square, square, square, pltpu.VMEM((8, 256), F32),
    )
    return pl.pallas_call(
        exchange_kernel,
        out_shape=outs,
        in_specs=[hbm] * (3 + N_SMALL),
        out_specs=(vmem,) * len(outs),
        scratch_shapes=[pltpu.VMEM(a.shape, a.dtype) for a in small]
        + [
            pltpu.VMEM((2, ROWS, LAT), BF16),
            pltpu.VMEM((256, LAT), BF16),
            pltpu.VMEM((8, LAT), F32),
            pltpu.VMEM((8, LAT), F32),
            pltpu.VMEM((n_col, 8, LAT), F32),
            pltpu.VMEM((n_row, 8, LAT), F32),
            pltpu.VMEM((ROWS * COLS + 2 * COLS, LAT), BF16),
            pltpu.VMEM((ROWS * COLS, LAT), BF16),
            pltpu.VMEM((16 * BANDS, LAT), BF16),
            pltpu.VMEM((2, 72, LAT), F32),
            pltpu.VMEM((NBLK, 24, BLK), F32),
            pltpu.VMEM((TRASH, BLK, 384), BF16),
            pltpu.SMEM((1, BANDS), jnp.int32),
            pltpu.SemaphoreType.DMA,
            pltpu.SemaphoreType.DMA((BANDS,)),
            pltpu.SemaphoreType.DMA,
            pltpu.SemaphoreType.DMA((N_SMALL,)),
            pltpu.SemaphoreType.DMA((8,)),
            pltpu.SemaphoreType.DMA((8,)),
            pltpu.SemaphoreType.DMA((n_col,)),
            pltpu.SemaphoreType.DMA((n_col,)),
            pltpu.SemaphoreType.DMA((n_row,)),
            pltpu.SemaphoreType.DMA((n_row,)),
        ],
        compiler_params=pltpu.CompilerParams(
            collective_id=0, has_side_effects=True, vmem_limit_bytes=24 * 1024 * 1024
        ),
        name="exchange",
    )(pin(nodes), pin(edges), pin(counts), *[pin(a) for a in small])


def main_kernel(
    counts, stats, edges_v, part_v, nodes, ridx, w_x2, w_hid2, w_out2, w_avg2, vecs,
    wn_in, wn_hid2, wn_out2, wn_avg2, n_vecs,
    new_nodes, edges_out,
    out_v, zeros_v, acc, work, x_ring, h2_s, nodes_s, out_sem, node_sem,
):
    zeros_v[...] = jnp.zeros_like(zeros_v)

    place = jnp.int32(0)
    for b in range(BANDS):
        count = counts[0, b]
        for j in range(NBLK):
            work[place + NB * STAGES] = jnp.int32(b * NBLK + j)
            place = place + (count > j * BLK).astype(jnp.int32)
    for k in range(NB * STAGES):
        work[k] = jnp.int32(TRASH)
    for k in range(NB * (STAGES + 1)):
        work[place + NB * STAGES + k] = jnp.int32(TRASH)
    acc[...] = jnp.zeros_like(acc)
    for b in range(BANDS):
        for j in range(2, NBLK):

            @pl.when(counts[0, b] <= j * BLK)
            def _():
                pltpu.make_async_copy(
                    zeros_v, edges_out.at[pl.ds(b * SLOTS + j * BLK, BLK)], out_sem
                ).start()

    mean, inv = stats[0:1], stats[1:2]
    node_id = lax.broadcasted_iota(jnp.int32, (BAND_NODES, BLK), 0).astype(F32).astype(BF16)
    one, nought = jnp.ones((), BF16), jnp.zeros((), BF16)

    def item(i, stage, u):
        return work[(i + STAGES - stage) * NB + u]

    slot_id = lax.broadcasted_iota(jnp.int32, (HALF, LAT), 0).astype(F32).astype(BF16)
    bias2, shift = vecs[0:1].astype(BF16), vecs[2:3].astype(BF16)
    us = range(NB)

    def where_of(i, stage):
        ks = [item(i, stage, u) for u in us]
        return ks, [lax.shift_right_logical(k, 2) for k in ks], [lax.rem(k, NBLK) for k in ks]

    def half_rows(k, h):
        return pl.ds(pl.multiple_of(k * BLK + h * HALF, HALF), HALF)

    def step(i, _):
        k2, b2, j2 = where_of(i, 2)
        k1, b1, j1 = where_of(i, 1)
        k0, _, _ = where_of(i, 0)
        old, new = lax.rem(i + RING - 1, RING), lax.rem(i, RING)
        rows = [ridx[j2[u], pl.ds(b2[u], 1), :].astype(BF16) for u in us]
        for u in us:
            pick = jnp.where(node_id == rows[u], one, nought)
            acc[b2[u]] += dot(pick, out_v[pl.ds(pl.multiple_of(k2[u] * BLK, BLK), BLK), :])
        cgs = [dot(h2_s[u], w_out2[...]) + vecs[1:2] for u in us]
        h1s = []
        for u in us:
            halves = [((edges_v[half_rows(k0[u], h), :].astype(F32) - mean) * inv).astype(BF16) for h in range(2)]
            x = jnp.concatenate(halves, axis=1)
            x_ring[new, u] = x
            parts = [part_v[half_rows(k0[u], h), :] for h in range(2)]
            h1 = dot(x, w_x2[...]) + jnp.concatenate(parts, axis=1)
            h1s.append(jnp.maximum(h1.astype(BF16), nought))
        lows = [cgs[u].astype(BF16) for u in us]
        variances = [dot(lows[u] * lows[u], w_avg2[...]) for u in us]
        for u in us:
            scaled = (cgs[u] * lax.rsqrt(variances[u] + EPS)).astype(BF16) + (x_ring[old, u] + shift)
            left_count = counts[0, jnp.minimum(b1[u], BANDS - 1)] - j1[u] * BLK
            for h in range(2):
                bound = jnp.clip(left_count - h * HALF, 0, HALF).astype(F32)
                bound = jnp.full((HALF, LAT), bound).astype(BF16)
                v = jnp.where(slot_id < bound, scaled[:, h * LAT : (h + 1) * LAT], nought)
                out_v[half_rows(k1[u], h), :] = v
        for u in us:
            h2_s[u] = jnp.maximum(dot(h1s[u], w_hid2[...]).astype(BF16) + bias2, nought)

        @pl.when(i >= 1)
        def _():
            for u in range(NB):
                k = item(i, 1, u)

                @pl.when(k < TRASH)
                def _():
                    pltpu.make_async_copy(
                        out_v.at[pl.ds(pl.multiple_of(k * BLK, BLK), BLK)],
                        edges_out.at[pl.ds(pl.multiple_of(k * BLK, BLK), BLK)],
                        out_sem,
                    ).start()

        return 0

    lax.fori_loop(0, lax.div(place + (NB - 1), NB) + STAGES, step, 0)

    size = 2 * BLK
    chunks = range(ROWS * COLS // size)
    low_bias2, low_shift = n_vecs[0:1].astype(BF16), n_vecs[2:3].astype(BF16)
    owns = [nodes[k * 16 : (k + 1) * 16].reshape(size, LAT) for k in chunks]
    hs = []
    for k in chunks:
        gathered = jnp.concatenate([acc[k * 4 + t] for t in range(4)], axis=0).astype(BF16)
        h = dot(jnp.concatenate([owns[k], gathered], axis=1), wn_in[...]) + n_vecs[3:4, 0:LAT]
        h = jnp.maximum(h.astype(BF16), nought)
        hs.append(jnp.concatenate([h[:BLK], h[BLK:]], axis=1))
    hs = [jnp.maximum(dot(hs[k], wn_hid2[...]).astype(BF16) + low_bias2, nought) for k in chunks]
    cgs = [dot(hs[k], wn_out2[...]) + n_vecs[1:2] for k in chunks]
    lows = [cgs[k].astype(BF16) for k in chunks]
    variances = [dot(lows[k] * lows[k], wn_avg2[...]) for k in chunks]
    node_copies = []
    for k in chunks:
        v = (cgs[k] * lax.rsqrt(variances[k] + EPS)).astype(BF16) + low_shift
        nodes_s[k * size : k * size + BLK] = v[:, :LAT] + owns[k][:BLK]
        nodes_s[k * size + BLK : (k + 1) * size] = v[:, LAT:] + owns[k][BLK:]
        here = pl.ds(k * size, size)
        c = pltpu.make_async_copy(nodes_s.at[here], new_nodes.at[here], node_sem.at[k])
        c.start()
        node_copies.append(c)
    for c in node_copies:
        c.wait()
    pltpu.make_async_copy(out_v.at[pl.ds(0, BANDS * SLOTS)], edges_out, out_sem).wait()


def process(counts, *held):
    vmem, smem = pl.BlockSpec(memory_space=pltpu.VMEM), pl.BlockSpec(memory_space=pltpu.SMEM)
    pin = lambda a: pltpu.with_memory_space_constraint(a, pltpu.VMEM)
    return pl.pallas_call(
        main_kernel,
        out_shape=(
            jax.ShapeDtypeStruct((ROWS * COLS, LAT), BF16),
            jax.ShapeDtypeStruct((BANDS * SLOTS, LAT), BF16),
        ),
        in_specs=[smem] + [vmem] * len(held),
        out_specs=(pl.BlockSpec(memory_space=pl.ANY), pl.BlockSpec(memory_space=pl.ANY)),
        scratch_shapes=[
            pltpu.VMEM(((TRASH + 1) * BLK, LAT), BF16),
            pltpu.VMEM((BLK, LAT), BF16),
            pltpu.VMEM((BANDS + 1, BAND_NODES, LAT), F32),
            pltpu.SMEM((TRASH + NB * (2 * STAGES + 2),), jnp.int32),
            pltpu.VMEM((RING, NB, HALF, 256), BF16),
            pltpu.VMEM((NB, HALF, 256), BF16),
            pltpu.VMEM((ROWS * COLS, LAT), BF16),
            pltpu.SemaphoreType.DMA,
            pltpu.SemaphoreType.DMA((4,)),
        ],
        compiler_params=pltpu.CompilerParams(vmem_limit_bytes=32 * 1024 * 1024),
        name="process",
    )(counts, *[pin(a) for a in held])


def per_device(
    nodes, edges, senders, receivers, counts,
    w_edge_in, w_edge_hid, w_edge_out, edge_bias, edge_gain, edge_shift,
    w_node_in, w_node_hid, w_node_out, node_bias, node_gain, node_shift,
):
    flat_edges = edges.reshape(BANDS * SLOTS, LAT)
    count_row = counts.reshape(1, BANDS)
    held = exchange(
        nodes, flat_edges, count_row, senders.reshape(BANDS, SLOTS), receivers.reshape(BANDS, SLOTS),
        w_edge_in, w_edge_hid, w_edge_out, edge_bias, edge_gain.reshape(1, LAT), edge_shift.reshape(1, LAT),
        w_node_in, w_node_hid, w_node_out, node_bias, node_gain.reshape(1, LAT), node_shift.reshape(1, LAT),
    )
    new_nodes, new_edges = process(count_row, *held)
    return new_nodes.reshape(nodes.shape), new_edges.reshape(edges.shape)


def solution(mesh):
    in_specs = (
        P("row", "col", None),
        P("row", "col", None, None, None),
        P("row", "col", None, None),
        P("row", "col", None, None),
        P("row", "col", None),
    ) + (P(),) * 12
    out_specs = (P("row", "col", None), P("row", "col", None, None, None))
    return jax.shard_map(
        per_device, mesh=mesh, in_specs=in_specs, out_specs=out_specs, check_vma=False
    )
```

```python
import functools

import jax
import jax.numpy as jnp
from jax import lax
from jax.experimental import pallas as pl
from jax.experimental.pallas import tpu as pltpu
from jax.sharding import PartitionSpec as P

F32 = jnp.float32
BF16 = jnp.bfloat16
LAT = 128
ROWS = 64
COLS = 32
BANDS = 16
SLOTS = 1024
BAND_NODES = 128
BLK = 256
HALF = BLK // 2
NBLK = SLOTS // BLK
NA = 8
NP = 4
NB = 4
RING = 2
STAGES = 2
TRASH = BANDS * NBLK
EPS = 1e-5
MESH = pl.DeviceIdType.MESH


def combine(parts):
    n = functools.reduce(jnp.add, [p[0:1] for p in parts])
    weighted = functools.reduce(jnp.add, [p[0:1] * p[1:2] for p in parts])
    mean = weighted / n
    m2 = None
    for p in parts:
        d = p[1:2] - mean
        t = p[2:3] + p[0:1] * d * d
        m2 = t if m2 is None else m2 + t
    return n, mean, m2


def dot(a, b):
    return jnp.dot(a, b, preferred_element_type=F32)


def block_diagonal(w):
    z = jnp.zeros_like(w)
    return jnp.concatenate(
        [jnp.concatenate([w, z], axis=1), jnp.concatenate([z, w], axis=1)], axis=0
    )


def twice(v):
    return jnp.concatenate([v, v], axis=1)


def norm_weights(w_out, bias, gain):
    w = w_out.astype(F32)
    w = (w - jnp.mean(w, axis=1, keepdims=True)) * gain
    b = (bias - jnp.mean(bias, axis=1, keepdims=True)) * gain
    weights = jnp.transpose(jnp.broadcast_to(1.0 / (LAT * gain * gain), (LAT, LAT)))
    return w.astype(BF16), b, weights.astype(BF16)


def prepare(hid, out, bias, gain, shift, hid2, out2, avg2, vecs):
    hid2[...] = block_diagonal(hid[...])
    w, b3, avg = norm_weights(out[...], bias[2:3], gain[...])
    out2[...] = block_diagonal(w)
    avg2[...] = block_diagonal(avg)
    vecs[0:1] = twice(bias[1:2])
    vecs[1:2] = twice(b3)
    vecs[2:3] = twice(shift[...])
    vecs[3:4] = twice(bias[0:1])


N_SMALL = 14


def exchange_kernel(*refs):
    nodes_hbm, edges_hbm, counts_hbm = refs[:3]
    small_hbm = refs[3 : 3 + N_SMALL]
    (
        stats_out, edges_v, part_v, nodes_v, ridx, w_x2, w_hid2, w_out2, w_avg2, vecs,
        wn_first, wn_hid2, wn_out2, wn_avg2, n_vecs,
    ) = refs[3 + N_SMALL : 18 + N_SMALL]
    small = refs[18 + N_SMALL : 18 + 2 * N_SMALL]
    (
        cols_v, halo_v, mine1, mine2, got1, got2, ps_t, pr_t, col_t, lr, sidx, oh_s, counts,
        count_sem, edge_sem, node_sem, small_sem, hs_sem, hr_sem, s1_sem, r1_sem, s2_sem, r2_sem,
    ) = refs[18 + 2 * N_SMALL :]
    (
        senders, receivers, w_in, w_hid, w_out, e_bias, e_gain, e_shift,
        wn_in, wn_hid, wn_out, n_bias, n_gain, n_shift,
    ) = small
    n_row, n_col = lax.axis_size("row"), lax.axis_size("col")
    row, col = lax.axis_index("row"), lax.axis_index("col")
    up, down = lax.rem(row + n_row - 1, n_row), lax.rem(row + 1, n_row)
    left, right = lax.rem(col + n_col - 1, n_col), lax.rem(col + 1, n_col)

    barrier = pltpu.get_barrier_semaphore()
    peers = [(row, lax.rem(col + k, n_col)) for k in range(1, n_col)]
    peers += [(lax.rem(row + k, n_row), col) for k in range(1, n_row)]
    peers += [(up, left), (up, right), (down, left), (down, right)]
    for p in peers:
        pl.semaphore_signal(barrier, inc=1, device_id=p, device_id_type=MESH)

    def edge_copy(b):
        return pltpu.make_async_copy(
            edges_hbm.at[pl.ds(b * SLOTS, SLOTS)], edges_v.at[pl.ds(b * SLOTS, SLOTS)], edge_sem.at[b]
        )

    count_copy = pltpu.make_async_copy(counts_hbm, counts, count_sem)
    count_copy.start()
    node_copy = pltpu.make_async_copy(nodes_hbm, nodes_v, node_sem)
    for b in range(BANDS):
        edge_copy(b).start()
    node_copy.start()
    small_copies = [
        pltpu.make_async_copy(src, dst, small_sem.at[k])
        for k, (src, dst) in enumerate(zip(small_hbm, small))
    ]
    for c in small_copies:
        c.start()

    count_copy.wait()
    edge_copy(0).wait()
    pivot = edges_v[0:16, :].astype(F32)[0:1]
    slot_id = lax.broadcasted_iota(jnp.int32, (64, LAT), 0)

    def band_sums(b, s, q):
        count = counts[0, b]
        for j in range(SLOTS // 64):
            d = edges_v[pl.ds(pl.multiple_of(b * SLOTS + j * 64, 64), 64), :].astype(F32) - pivot
            if j >= SLOTS // 128:
                d = jnp.where(slot_id < count - j * 64, d, 0.0)
            e = d * d
            s = s + ((d[0:8] + d[8:16]) + (d[16:24] + d[24:32])) + ((d[32:40] + d[40:48]) + (d[48:56] + d[56:64]))
            q = q + ((e[0:8] + e[8:16]) + (e[16:24] + e[24:32])) + ((e[32:40] + e[40:48]) + (e[48:56] + e[56:64]))
        return s, q

    def band_stats(b, carry):
        edge_copy(b).wait()
        return band_sums(b, *carry)

    zero = jnp.zeros((8, LAT), F32)
    carry = band_sums(0, zero, zero)
    s, q = lax.fori_loop(1, BANDS, band_stats, carry)
    total = counts[0, 0]
    for b in range(1, BANDS):
        total = total + counts[0, b]
    n = jnp.full((1, LAT), total.astype(F32))
    s = jnp.sum(s, axis=0, keepdims=True)
    q = jnp.sum(q, axis=0, keepdims=True)
    local_mean = s / n
    filler = jnp.zeros((1, LAT), F32)
    mine1[...] = jnp.concatenate([n, pivot + local_mean, q - s * local_mean, filler], axis=0)

    node_copy.wait()
    cols_v[0] = nodes_v[:, 0, :]
    cols_v[1] = nodes_v[:, COLS - 1, :]
    pl.semaphore_wait(barrier, len(peers))
    copies = []
    for k in range(1, n_col):
        c = pltpu.make_async_remote_copy(
            src_ref=mine1, dst_ref=got1.at[k], send_sem=s1_sem.at[k], recv_sem=r1_sem.at[k],
            device_id=(row, lax.rem(col + k, n_col)), device_id_type=MESH,
        )
        c.start()
        copies.append(c)

    sends = [
        (nodes_v.at[ROWS - 1], (0, 32), (down, col)),
        (nodes_v.at[0], (32, 32), (up, col)),
        (cols_v.at[1], (64, 64), (row, right)),
        (cols_v.at[0], (128, 64), (row, left)),
        (cols_v.at[1, pl.ds(48, 16)], (192, 16), (down, right)),
        (cols_v.at[0, pl.ds(48, 16)], (208, 16), (down, left)),
        (cols_v.at[1, pl.ds(0, 16)], (224, 16), (up, right)),
        (cols_v.at[0, pl.ds(0, 16)], (240, 16), (up, left)),
    ]
    halo_copies = []
    for k, (src, (start, size), dev) in enumerate(sends):
        c = pltpu.make_async_remote_copy(
            src_ref=src, dst_ref=halo_v.at[pl.ds(start, size)],
            send_sem=hs_sem.at[k], recv_sem=hr_sem.at[k], device_id=dev, device_id_type=MESH,
        )
        c.start()
        halo_copies.append(c)

    for c in small_copies:
        c.wait()
    w_snd, w_rcv = w_in[LAT : 2 * LAT], w_in[2 * LAT :]
    w_both = jnp.concatenate([w_snd, w_rcv], axis=1)
    bias1 = e_bias[0:1]
    for k in range(ROWS * COLS // BLK):
        own = nodes_v[k * 8 : (k + 1) * 8].reshape(BLK, LAT)
        p = dot(own, w_both)
        ps_t[COLS + k * BLK : COLS + (k + 1) * BLK] = p[:, :LAT].astype(BF16)
        pr_t[k * BLK : (k + 1) * BLK] = (p[:, LAT:] + bias1).astype(BF16)

    s = senders[...]
    r = lax.shift_right_logical(s * 241, 13)
    c = s - r * 34
    place_s = jnp.where(c == 0, 192 + r, jnp.where(c == 33, 200 + r, r * 32 + c - 1)).astype(F32)
    place_r = receivers[...].astype(F32)
    for j in range(NBLK):
        sidx[j, 0:BANDS] = place_s[:, j * BLK : (j + 1) * BLK]
        ridx[j, 0:BANDS] = place_r[:, j * BLK : (j + 1) * BLK]

    w_x2[...] = block_diagonal(w_in[0:LAT])
    prepare(w_hid, w_out, e_bias, e_gain, e_shift, w_hid2, w_out2, w_avg2, vecs)

    node_id = lax.broadcasted_iota(jnp.int32, (256, BLK), 0).astype(F32).astype(BF16)
    one, nought = jnp.ones((), BF16), jnp.zeros((), BF16)

    ps_t[0:COLS] = jnp.zeros((COLS, LAT), BF16)
    ps_t[COLS + ROWS * COLS :] = jnp.zeros((COLS, LAT), BF16)

    def one_hot(k):
        band, j = lax.div(k, NBLK), lax.rem(k, NBLK)
        si = sidx[j, pl.ds(band, 1), :].astype(BF16)
        ri = ridx[j, pl.ds(band, 1), :].astype(BF16)
        pick_s = jnp.where(node_id == si, one, nought)
        pick_r = jnp.where(node_id[:BAND_NODES] == ri, one, nought)
        oh_s[k, :, 0:LAT] = pick_r.T
        oh_s[k, :, LAT:] = pick_s.T

    def gather(k):
        start = pl.multiple_of(lax.div(k, NBLK) * BAND_NODES, BAND_NODES)
        table = jnp.concatenate(
            [pr_t[pl.ds(start, BAND_NODES), :], ps_t[pl.ds(start, 192), :], jnp.zeros((64, LAT), BF16)],
            axis=0,
        )
        part_v[pl.ds(pl.multiple_of(k * BLK, BLK), BLK), :] = dot(oh_s[k], table)

    last = TRASH // NA - 1
    for u in range(NA):
        one_hot(jnp.int32(u))

    def step(i, _):
        for u in range(NA):
            gather(i * NA + u)
        for u in range(NA):
            one_hot(jnp.minimum(i + 1, last) * NA + u)
        return 0

    lax.fori_loop(0, last + 1, step, 0)

    for c in copies:
        c.wait_recv()
    n, mean, m2 = combine([mine1[...]] + [got1[k] for k in range(1, n_col)])
    mine2[...] = jnp.concatenate([n, mean, m2, filler], axis=0)
    copies2 = []
    for k in range(1, n_row):
        c = pltpu.make_async_remote_copy(
            src_ref=mine2, dst_ref=got2.at[k], send_sem=s2_sem.at[k], recv_sem=r2_sem.at[k],
            device_id=(lax.rem(row + k, n_row), col), device_id_type=MESH,
        )
        c.start()
        copies2.append(c)

    for c in halo_copies:
        c.wait_recv()
    p = dot(halo_v[...], w_snd)
    lr[0, 64:72] = jnp.zeros((8, LAT), F32)
    lr[1, 64:72] = jnp.zeros((8, LAT), F32)
    lr[0, 1:65] = p[64:128]
    lr[1, 1:65] = p[128:192]
    lr[0, 0:1] = p[207:208]
    lr[1, 0:1] = p[223:224]
    lr[0, 65:66] = p[224:225]
    lr[1, 65:66] = p[240:241]
    top = jnp.concatenate([p[0:32].astype(BF16), jnp.zeros((96, LAT), BF16)], axis=0)
    col_t[:, 0:64] = jnp.zeros((BANDS, 64, LAT), BF16)
    col_t[BANDS - 1, 32:64] = p[32:64].astype(BF16)
    col_t[:, 80:] = jnp.zeros((BANDS, 48, LAT), BF16)
    for b in range(BANDS):
        pair = jnp.concatenate([lr[0, 4 * b : 4 * b + 8], lr[1, 4 * b : 4 * b + 8]], axis=0)
        col_t[b, 64:80] = pair.astype(BF16)

    def halo_step(i, _):
        bands = [i * NP + u for u in range(NP)]
        tables = [block_diagonal(col_t[b]) for b in bands]
        lhs = [
            [jnp.concatenate([oh_s[b * NBLK + j, :HALF, 2 * LAT :], oh_s[b * NBLK + j, HALF:, 2 * LAT :]], axis=1) for j in range(NBLK)]
            for b in bands
        ]
        for u, b in enumerate(bands):
            more = dot(jnp.concatenate(lhs[u], axis=0), tables[u])
            for j in range(NBLK):
                for h in range(2):
                    here = pl.ds(pl.multiple_of((b * NBLK + j) * BLK + h * HALF, HALF), HALF)
                    part_v[here, :] += more[j * HALF : (j + 1) * HALF, h * LAT : (h + 1) * LAT]
        return 0

    lax.fori_loop(0, BANDS // NP, halo_step, 0)
    tops = block_diagonal(top)
    lhs = [jnp.concatenate([oh_s[j, :HALF, LAT : 2 * LAT], oh_s[j, HALF:, LAT : 2 * LAT]], axis=1) for j in range(NBLK)]
    more = dot(jnp.concatenate(lhs, axis=0), tops)
    for j in range(NBLK):
        for h in range(2):
            here = slice(j * BLK + h * HALF, j * BLK + (h + 1) * HALF)
            part_v[here] += more[j * HALF : (j + 1) * HALF, h * LAT : (h + 1) * LAT]
    wn_first[...] = wn_in[...]
    prepare(wn_hid, wn_out, n_bias, n_gain, n_shift, wn_hid2, wn_out2, wn_avg2, n_vecs)
    for c in copies2:
        c.wait_recv()
    n, mean, m2 = combine([mine2[...]] + [got2[k] for k in range(1, n_row)])
    inv = lax.rsqrt(m2 / n + EPS)
    stats_out[...] = jnp.concatenate([mean, inv, jnp.zeros((6, LAT), F32)], axis=0)
    for c in halo_copies + copies + copies2:
        c.wait_send()


def exchange(nodes, edges, counts, *small):
    n_row, n_col = lax.axis_size("row"), lax.axis_size("col")
    hbm, vmem = pl.BlockSpec(memory_space=pltpu.HBM), pl.BlockSpec(memory_space=pltpu.VMEM)
    pin = lambda a: pltpu.with_memory_space_constraint(a, pltpu.HBM)
    square = pltpu.VMEM((256, 256), BF16)
    outs = (
        pltpu.VMEM((8, LAT), F32),
        pltpu.VMEM(((TRASH + 1) * BLK, LAT), BF16),
        pltpu.VMEM(((TRASH + 1) * BLK, LAT), F32),
        pltpu.VMEM((ROWS, COLS, LAT), BF16),
        pltpu.VMEM((NBLK, 24, BLK), F32),
        square, square, square, square, pltpu.VMEM((8, 256), F32),
        pltpu.VMEM((2 * LAT, LAT), BF16), square, square, square, pltpu.VMEM((8, 256), F32),
    )
    return pl.pallas_call(
        exchange_kernel,
        out_shape=outs,
        in_specs=[hbm] * (3 + N_SMALL),
        out_specs=(vmem,) * len(outs),
        scratch_shapes=[pltpu.VMEM(a.shape, a.dtype) for a in small]
        + [
            pltpu.VMEM((2, ROWS, LAT), BF16),
            pltpu.VMEM((256, LAT), BF16),
            pltpu.VMEM((4, LAT), F32),
            pltpu.VMEM((4, LAT), F32),
            pltpu.VMEM((n_col, 4, LAT), F32),
            pltpu.VMEM((n_row, 4, LAT), F32),
            pltpu.VMEM((ROWS * COLS + 2 * COLS, LAT), BF16),
            pltpu.VMEM((ROWS * COLS, LAT), BF16),
            pltpu.VMEM((BANDS, BAND_NODES, LAT), BF16),
            pltpu.VMEM((2, 72, LAT), F32),
            pltpu.VMEM((NBLK, 24, BLK), F32),
            pltpu.VMEM((TRASH, BLK, 384), BF16),
            pltpu.SMEM((1, BANDS), jnp.int32),
            pltpu.SemaphoreType.DMA,
            pltpu.SemaphoreType.DMA((BANDS,)),
            pltpu.SemaphoreType.DMA,
            pltpu.SemaphoreType.DMA((N_SMALL,)),
            pltpu.SemaphoreType.DMA((8,)),
            pltpu.SemaphoreType.DMA((8,)),
            pltpu.SemaphoreType.DMA((n_col,)),
            pltpu.SemaphoreType.DMA((n_col,)),
            pltpu.SemaphoreType.DMA((n_row,)),
            pltpu.SemaphoreType.DMA((n_row,)),
        ],
        compiler_params=pltpu.CompilerParams(
            collective_id=0, has_side_effects=True, vmem_limit_bytes=24 * 1024 * 1024
        ),
        name="exchange",
    )(pin(nodes), pin(edges), pin(counts), *[pin(a) for a in small])


def main_kernel(
    counts, stats, edges_v, part_v, nodes, ridx, w_x2, w_hid2, w_out2, w_avg2, vecs,
    wn_in, wn_hid2, wn_out2, wn_avg2, n_vecs,
    new_nodes, edges_out,
    out_v, zeros_v, acc, work, x_ring, h2_s, nodes_s, out_sem, node_sem,
):
    zeros_v[...] = jnp.zeros_like(zeros_v)

    place = jnp.int32(0)
    for b in range(BANDS):
        count = counts[0, b]
        for j in range(NBLK):
            work[place + NB * STAGES] = jnp.int32(b * NBLK + j)
            place = place + (count > j * BLK).astype(jnp.int32)
    for k in range(NB * STAGES):
        work[k] = jnp.int32(TRASH)
    for k in range(NB * (STAGES + 1)):
        work[place + NB * STAGES + k] = jnp.int32(TRASH)
    acc[...] = jnp.zeros_like(acc)
    for b in range(BANDS):
        for j in range(2, NBLK):

            @pl.when(counts[0, b] <= j * BLK)
            def _():
                pltpu.make_async_copy(
                    zeros_v, edges_out.at[pl.ds(b * SLOTS + j * BLK, BLK)], out_sem
                ).start()

    mean, inv = stats[0:1], stats[1:2]
    node_id = lax.broadcasted_iota(jnp.int32, (BAND_NODES, BLK), 0).astype(F32).astype(BF16)
    one, nought = jnp.ones((), BF16), jnp.zeros((), BF16)

    def item(i, stage, u):
        return work[(i + STAGES - stage) * NB + u]

    slot_id = lax.broadcasted_iota(jnp.int32, (HALF, LAT), 0).astype(F32).astype(BF16)
    bias2, shift = vecs[0:1].astype(BF16), vecs[2:3].astype(BF16)
    us = range(NB)

    def where_of(i, stage):
        ks = [item(i, stage, u) for u in us]
        return ks, [lax.shift_right_logical(k, 2) for k in ks], [lax.rem(k, NBLK) for k in ks]

    def half_rows(k, h):
        return pl.ds(pl.multiple_of(k * BLK + h * HALF, HALF), HALF)

    def scatter(i):
        k2, b2, j2 = where_of(i, 2)
        rows = [ridx[j2[u], pl.ds(b2[u], 1), :].astype(BF16) for u in us]
        for u in us:
            pick = jnp.where(node_id == rows[u], one, nought)
            acc[b2[u]] += dot(pick, out_v[pl.ds(pl.multiple_of(k2[u] * BLK, BLK), BLK), :])

    def output():
        cgs = [dot(h2_s[u], w_out2[...]) + vecs[1:2] for u in us]
        return cgs

    def first(i):
        k0, _, _ = where_of(i, 0)
        new = lax.rem(i, RING)
        h1s = []
        for u in us:
            halves = [((edges_v[half_rows(k0[u], h), :].astype(F32) - mean) * inv).astype(BF16) for h in range(2)]
            x = jnp.concatenate(halves, axis=1)
            x_ring[new, u] = x
            parts = [part_v[half_rows(k0[u], h), :] for h in range(2)]
            h1 = dot(x, w_x2[...]) + jnp.concatenate(parts, axis=1)
            h1s.append(jnp.maximum(h1.astype(BF16), nought))
        return h1s

    def variance(cgs):
        lows = [cgs[u].astype(BF16) for u in us]
        variances = [dot(lows[u] * lows[u], w_avg2[...]) for u in us]
        return variances

    def finish(i, cgs, variances):
        k1, b1, j1 = where_of(i, 1)
        old = lax.rem(i + RING - 1, RING)
        for u in us:
            scaled = (cgs[u] * lax.rsqrt(variances[u] + EPS)).astype(BF16) + (x_ring[old, u] + shift)
            left_count = counts[0, jnp.minimum(b1[u], BANDS - 1)] - j1[u] * BLK
            for h in range(2):
                bound = jnp.clip(left_count - h * HALF, 0, HALF).astype(F32)
                bound = jnp.full((HALF, LAT), bound).astype(BF16)
                v = jnp.where(slot_id < bound, scaled[:, h * LAT : (h + 1) * LAT], nought)
                out_v[half_rows(k1[u], h), :] = v

    def hidden(h1s):
        for u in us:
            h2_s[u] = jnp.maximum(dot(h1s[u], w_hid2[...]).astype(BF16) + bias2, nought)

    def step(i, _):
        scatter(i)
        cgs = output()
        h1s = first(i)
        variances = variance(cgs)
        finish(i, cgs, variances)
        hidden(h1s)
        for u in range(NB):
            k = item(i, 1, u)

            @pl.when(k < TRASH)
            def _():
                pltpu.make_async_copy(
                    out_v.at[pl.ds(pl.multiple_of(k * BLK, BLK), BLK)],
                    edges_out.at[pl.ds(pl.multiple_of(k * BLK, BLK), BLK)],
                    out_sem,
                ).start()
        return 0

    steps = lax.div(place + (NB - 1), NB) + 1
    hidden(first(0))
    lax.fori_loop(1, steps, step, 0)
    scatter(steps)

    size = 2 * BLK
    chunks = range(ROWS * COLS // size)
    low_bias2, low_shift = n_vecs[0:1].astype(BF16), n_vecs[2:3].astype(BF16)
    owns = [nodes[k * 16 : (k + 1) * 16].reshape(size, LAT) for k in chunks]
    hs = []
    for k in chunks:
        gathered = jnp.concatenate([acc[k * 4 + t] for t in range(4)], axis=0).astype(BF16)
        h = dot(jnp.concatenate([owns[k], gathered], axis=1), wn_in[...]) + n_vecs[3:4, 0:LAT]
        h = jnp.maximum(h.astype(BF16), nought)
        hs.append(jnp.concatenate([h[:BLK], h[BLK:]], axis=1))
    hs = [jnp.maximum(dot(hs[k], wn_hid2[...]).astype(BF16) + low_bias2, nought) for k in chunks]
    cgs = [dot(hs[k], wn_out2[...]) + n_vecs[1:2] for k in chunks]
    lows = [cgs[k].astype(BF16) for k in chunks]
    variances = [dot(lows[k] * lows[k], wn_avg2[...]) for k in chunks]
    node_copies = []
    for k in chunks:
        v = (cgs[k] * lax.rsqrt(variances[k] + EPS)).astype(BF16) + low_shift
        nodes_s[k * size : k * size + BLK] = v[:, :LAT] + owns[k][:BLK]
        nodes_s[k * size + BLK : (k + 1) * size] = v[:, LAT:] + owns[k][BLK:]
        here = pl.ds(k * size, size)
        c = pltpu.make_async_copy(nodes_s.at[here], new_nodes.at[here], node_sem.at[k])
        c.start()
        node_copies.append(c)
    for c in node_copies:
        c.wait()
    pltpu.make_async_copy(out_v.at[pl.ds(0, BANDS * SLOTS)], edges_out, out_sem).wait()


def process(counts, *held):
    vmem, smem = pl.BlockSpec(memory_space=pltpu.VMEM), pl.BlockSpec(memory_space=pltpu.SMEM)
    pin = lambda a: pltpu.with_memory_space_constraint(a, pltpu.VMEM)
    return pl.pallas_call(
        main_kernel,
        out_shape=(
            jax.ShapeDtypeStruct((ROWS * COLS, LAT), BF16),
            jax.ShapeDtypeStruct((BANDS * SLOTS, LAT), BF16),
        ),
        in_specs=[smem] + [vmem] * len(held),
        out_specs=(pl.BlockSpec(memory_space=pl.ANY), pl.BlockSpec(memory_space=pl.ANY)),
        scratch_shapes=[
            pltpu.VMEM(((TRASH + 1) * BLK, LAT), BF16),
            pltpu.VMEM((BLK, LAT), BF16),
            pltpu.VMEM((BANDS + 1, BAND_NODES, LAT), F32),
            pltpu.SMEM((TRASH + NB * (2 * STAGES + 2),), jnp.int32),
            pltpu.VMEM((RING, NB, HALF, 256), BF16),
            pltpu.VMEM((NB, HALF, 256), BF16),
            pltpu.VMEM((ROWS * COLS, LAT), BF16),
            pltpu.SemaphoreType.DMA,
            pltpu.SemaphoreType.DMA((4,)),
        ],
        compiler_params=pltpu.CompilerParams(vmem_limit_bytes=32 * 1024 * 1024),
        name="process",
    )(counts, *[pin(a) for a in held])


def per_device(
    nodes, edges, senders, receivers, counts,
    w_edge_in, w_edge_hid, w_edge_out, edge_bias, edge_gain, edge_shift,
    w_node_in, w_node_hid, w_node_out, node_bias, node_gain, node_shift,
):
    flat_edges = edges.reshape(BANDS * SLOTS, LAT)
    count_row = counts.reshape(1, BANDS)
    held = exchange(
        nodes, flat_edges, count_row, senders.reshape(BANDS, SLOTS), receivers.reshape(BANDS, SLOTS),
        w_edge_in, w_edge_hid, w_edge_out, edge_bias, edge_gain.reshape(1, LAT), edge_shift.reshape(1, LAT),
        w_node_in, w_node_hid, w_node_out, node_bias, node_gain.reshape(1, LAT), node_shift.reshape(1, LAT),
    )
    new_nodes, new_edges = process(count_row, *held)
    return new_nodes.reshape(nodes.shape), new_edges.reshape(edges.shape)


def solution(mesh):
    in_specs = (
        P("row", "col", None),
        P("row", "col", None, None, None),
        P("row", "col", None, None),
        P("row", "col", None, None),
        P("row", "col", None),
    ) + (P(),) * 12
    out_specs = (P("row", "col", None), P("row", "col", None, None, None))
    return jax.shard_map(
        per_device, mesh=mesh, in_specs=in_specs, out_specs=out_specs, check_vma=False
    )
```

```python
import functools

import jax
import jax.numpy as jnp
from jax import lax
from jax.experimental import pallas as pl
from jax.experimental.pallas import tpu as pltpu
from jax.sharding import PartitionSpec as P

F32 = jnp.float32
BF16 = jnp.bfloat16
LAT = 128
ROWS = 64
COLS = 32
BANDS = 16
SLOTS = 1024
BAND_NODES = 128
BLK = 256
HALF = BLK // 2
NBLK = SLOTS // BLK
NA = 8
SPLIT = 4
NP = 4
NB = 4
GROUP = 2
RING = 2
STAGES = 2
TRASH = BANDS * NBLK
EPS = 1e-5
MESH = pl.DeviceIdType.MESH


def combine(parts):
    n = functools.reduce(jnp.add, [p[0:1] for p in parts])
    weighted = functools.reduce(jnp.add, [p[0:1] * p[1:2] for p in parts])
    mean = weighted / n
    m2 = None
    for p in parts:
        d = p[1:2] - mean
        t = p[2:3] + p[0:1] * d * d
        m2 = t if m2 is None else m2 + t
    return n, mean, m2


def dot(a, b):
    return jnp.dot(a, b, preferred_element_type=F32)


def block_diagonal(w):
    z = jnp.zeros_like(w)
    return jnp.concatenate(
        [jnp.concatenate([w, z], axis=1), jnp.concatenate([z, w], axis=1)], axis=0
    )


def twice(v):
    return jnp.concatenate([v, v], axis=1)


def norm_weights(w_out, bias, gain):
    w = w_out.astype(F32)
    w = (w - jnp.mean(w, axis=1, keepdims=True)) * gain
    b = (bias - jnp.mean(bias, axis=1, keepdims=True)) * gain
    weights = jnp.transpose(jnp.broadcast_to(1.0 / (LAT * gain * gain), (LAT, LAT)))
    return w.astype(BF16), b, weights.astype(BF16)


def prepare(hid, out, bias, gain, shift, hid2, out2, avg2, vecs):
    hid2[...] = block_diagonal(hid[...])
    w, b3, avg = norm_weights(out[...], bias[2:3], gain[...])
    out2[...] = block_diagonal(w)
    avg2[...] = block_diagonal(avg)
    vecs[0:1] = twice(bias[1:2])
    vecs[1:2] = twice(b3)
    vecs[2:3] = twice(shift[...])
    vecs[3:4] = twice(bias[0:1])
    vecs[4:5] = twice(1.0 / (LAT * gain[...] * gain[...]))


N_SMALL = 14


def exchange_kernel(*refs):
    nodes_hbm, edges_hbm, counts_hbm = refs[:3]
    small_hbm = refs[3 : 3 + N_SMALL]
    (
        stats_out, edges_v, part_v, nodes_v, ridx, w_x2, w_hid2, w_out2, w_avg2, vecs,
        wn_first, wn_hid2, wn_out2, wn_avg2, n_vecs,
    ) = refs[3 + N_SMALL : 18 + N_SMALL]
    small = refs[18 + N_SMALL : 18 + 2 * N_SMALL]
    (
        cols_v, halo_v, mine1, mine2, got1, got2, ps_t, pr_t, col_t, lr, sidx, oh_s, counts,
        count_sem, edge_sem, node_sem, small_sem, hs_sem, hr_sem, s1_sem, r1_sem, s2_sem, r2_sem,
    ) = refs[18 + 2 * N_SMALL :]
    (
        senders, receivers, w_in, w_hid, w_out, e_bias, e_gain, e_shift,
        wn_in, wn_hid, wn_out, n_bias, n_gain, n_shift,
    ) = small
    n_row, n_col = lax.axis_size("row"), lax.axis_size("col")
    row, col = lax.axis_index("row"), lax.axis_index("col")
    up, down = lax.rem(row + n_row - 1, n_row), lax.rem(row + 1, n_row)
    left, right = lax.rem(col + n_col - 1, n_col), lax.rem(col + 1, n_col)

    def edge_copy(b):
        return pltpu.make_async_copy(
            edges_hbm.at[pl.ds(b * SLOTS, SLOTS)], edges_v.at[pl.ds(b * SLOTS, SLOTS)], edge_sem.at[b]
        )

    node_copy = pltpu.make_async_copy(nodes_hbm, nodes_v, node_sem)
    for b in range(2):
        edge_copy(b).start()
    count_copy = pltpu.make_async_copy(counts_hbm, counts, count_sem)
    count_copy.start()
    barrier = pltpu.get_barrier_semaphore()
    peers = [(row, lax.rem(col + k, n_col)) for k in range(1, n_col)]
    peers += [(lax.rem(row + k, n_row), col) for k in range(1, n_row)]
    peers += [(up, left), (up, right), (down, left), (down, right)]
    for p in peers:
        pl.semaphore_signal(barrier, inc=1, device_id=p, device_id_type=MESH)
    for b in range(2, BANDS):
        edge_copy(b).start()
    node_copy.start()
    small_copies = [
        pltpu.make_async_copy(src, dst, small_sem.at[k])
        for k, (src, dst) in enumerate(zip(small_hbm, small))
    ]
    for c in small_copies:
        c.start()

    count_copy.wait()
    edge_copy(0).wait()
    low_pivot = edges_v[0:16, :][0:1]
    pivot = low_pivot.astype(F32)
    slot_id = lax.broadcasted_iota(jnp.int32, (64, LAT), 0).astype(F32).astype(BF16)

    def band_sums(b, s, q):
        count = counts[0, b]
        for j in range(SLOTS // 64):
            x = edges_v[pl.ds(pl.multiple_of(b * SLOTS + j * 64, 64), 64), :]
            if j >= SLOTS // 128:
                bound = jnp.clip(count - j * 64, 0, 64).astype(F32)
                x = jnp.where(slot_id < jnp.full((64, LAT), bound).astype(BF16), x, low_pivot)
            d = x.astype(F32) - pivot
            e = d * d
            s = s + ((d[0:8] + d[8:16]) + (d[16:24] + d[24:32])) + ((d[32:40] + d[40:48]) + (d[48:56] + d[56:64]))
            q = q + ((e[0:8] + e[8:16]) + (e[16:24] + e[24:32])) + ((e[32:40] + e[40:48]) + (e[48:56] + e[56:64]))
        return s, q

    def band_stats(b, carry):
        edge_copy(b).wait()
        return band_sums(b, *carry)

    zero = jnp.zeros((8, LAT), F32)
    carry = band_sums(0, zero, zero)
    s, q = lax.fori_loop(1, BANDS, band_stats, carry)
    total = counts[0, 0]
    for b in range(1, BANDS):
        total = total + counts[0, b]
    n = jnp.full((1, LAT), total.astype(F32))
    s = jnp.sum(s, axis=0, keepdims=True)
    q = jnp.sum(q, axis=0, keepdims=True)
    local_mean = s / n
    filler = jnp.zeros((1, LAT), F32)
    mine1[...] = jnp.concatenate([n, pivot + local_mean, q - s * local_mean, filler], axis=0)

    node_copy.wait()
    cols_v[0] = nodes_v[:, 0, :]
    cols_v[1] = nodes_v[:, COLS - 1, :]
    pl.semaphore_wait(barrier, len(peers))
    copies = []
    for k in range(1, n_row):
        c = pltpu.make_async_remote_copy(
            src_ref=mine1, dst_ref=got1.at[k], send_sem=s1_sem.at[k], recv_sem=r1_sem.at[k],
            device_id=(lax.rem(row + k, n_row), col), device_id_type=MESH,
        )
        c.start()
        copies.append(c)

    sends = [
        (nodes_v.at[ROWS - 1], (0, 32), (down, col)),
        (nodes_v.at[0], (32, 32), (up, col)),
        (cols_v.at[1], (64, 64), (row, right)),
        (cols_v.at[0], (128, 64), (row, left)),
        (cols_v.at[1, pl.ds(48, 16)], (192, 16), (down, right)),
        (cols_v.at[0, pl.ds(48, 16)], (208, 16), (down, left)),
        (cols_v.at[1, pl.ds(0, 16)], (224, 16), (up, right)),
        (cols_v.at[0, pl.ds(0, 16)], (240, 16), (up, left)),
    ]
    halo_copies = []
    for k, (src, (start, size), dev) in enumerate(sends):
        c = pltpu.make_async_remote_copy(
            src_ref=src, dst_ref=halo_v.at[pl.ds(start, size)],
            send_sem=hs_sem.at[k], recv_sem=hr_sem.at[k], device_id=dev, device_id_type=MESH,
        )
        c.start()
        halo_copies.append(c)

    for c in small_copies:
        c.wait()
    w_snd, w_rcv = w_in[LAT : 2 * LAT], w_in[2 * LAT :]
    w_both = jnp.concatenate([w_snd, w_rcv], axis=1)
    bias1 = e_bias[0:1]
    for k in range(ROWS * COLS // BLK):
        own = nodes_v[k * 8 : (k + 1) * 8].reshape(BLK, LAT)
        p = dot(own, w_both)
        ps_t[COLS + k * BLK : COLS + (k + 1) * BLK] = p[:, :LAT].astype(BF16)
        pr_t[k * BLK : (k + 1) * BLK] = (p[:, LAT:] + bias1).astype(BF16)

    s = senders[...]
    r = lax.shift_right_logical(s * 241, 13)
    c = s - r * 34
    place_s = jnp.where(c == 0, 192 + r, jnp.where(c == 33, 200 + r, r * 32 + c - 1)).astype(F32)
    place_r = receivers[...].astype(F32)
    for j in range(NBLK):
        sidx[j, 0:BANDS] = place_s[:, j * BLK : (j + 1) * BLK]
        ridx[j, 0:BANDS] = place_r[:, j * BLK : (j + 1) * BLK]

    w_x2[...] = block_diagonal(w_in[0:LAT])
    prepare(w_hid, w_out, e_bias, e_gain, e_shift, w_hid2, w_out2, w_avg2, vecs)

    node_id = lax.broadcasted_iota(jnp.int32, (256, BLK), 0).astype(F32).astype(BF16)
    one, nought = jnp.ones((), BF16), jnp.zeros((), BF16)

    ps_t[0:COLS] = jnp.zeros((COLS, LAT), BF16)
    ps_t[COLS + ROWS * COLS :] = jnp.zeros((COLS, LAT), BF16)

    def one_hot(k):
        band, j = lax.div(k, NBLK), lax.rem(k, NBLK)
        si = sidx[j, pl.ds(band, 1), :].astype(BF16)
        ri = ridx[j, pl.ds(band, 1), :].astype(BF16)
        pick_s = jnp.where(node_id == si, one, nought)
        pick_r = jnp.where(node_id[:BAND_NODES] == ri, one, nought)
        oh_s[k, :, 0:LAT] = pick_r.T
        oh_s[k, :, LAT:] = pick_s.T

    def gather(k):
        start = pl.multiple_of(lax.div(k, NBLK) * BAND_NODES, BAND_NODES)
        table = jnp.concatenate(
            [pr_t[pl.ds(start, BAND_NODES), :], ps_t[pl.ds(start, 192), :], jnp.zeros((64, LAT), BF16)],
            axis=0,
        )
        part_v[pl.ds(pl.multiple_of(k * BLK, BLK), BLK), :] = dot(oh_s[k], table)

    last = TRASH // NA - 1
    for u in range(NA):
        one_hot(jnp.int32(u))

    def step(i, _):
        for u in range(NA):
            gather(i * NA + u)
        for u in range(NA):
            one_hot(jnp.minimum(i + 1, last) * NA + u)
        return 0

    lax.fori_loop(0, SPLIT, step, 0)
    for c in copies:
        c.wait_recv()
    n, mean, m2 = combine([mine1[...]] + [got1[k] for k in range(1, n_row)])
    mine2[...] = jnp.concatenate([n, mean, m2, filler], axis=0)
    copies2 = []
    for k in range(1, n_col):
        c = pltpu.make_async_remote_copy(
            src_ref=mine2, dst_ref=got2.at[k], send_sem=s2_sem.at[k], recv_sem=r2_sem.at[k],
            device_id=(row, lax.rem(col + k, n_col)), device_id_type=MESH,
        )
        c.start()
        copies2.append(c)
    lax.fori_loop(SPLIT, last + 1, step, 0)

    for c in halo_copies:
        c.wait_recv()
    p = dot(halo_v[...], w_snd)
    lr[0, 64:72] = jnp.zeros((8, LAT), F32)
    lr[1, 64:72] = jnp.zeros((8, LAT), F32)
    lr[0, 1:65] = p[64:128]
    lr[1, 1:65] = p[128:192]
    lr[0, 0:1] = p[207:208]
    lr[1, 0:1] = p[223:224]
    lr[0, 65:66] = p[224:225]
    lr[1, 65:66] = p[240:241]
    top = jnp.concatenate([p[0:32].astype(BF16), jnp.zeros((96, LAT), BF16)], axis=0)
    col_t[:, 0:64] = jnp.zeros((BANDS, 64, LAT), BF16)
    col_t[BANDS - 1, 32:64] = p[32:64].astype(BF16)
    col_t[:, 80:] = jnp.zeros((BANDS, 48, LAT), BF16)
    for b in range(BANDS):
        pair = jnp.concatenate([lr[0, 4 * b : 4 * b + 8], lr[1, 4 * b : 4 * b + 8]], axis=0)
        col_t[b, 64:80] = pair.astype(BF16)

    def halo_step(i, _):
        bands = [i * NP + u for u in range(NP)]
        tables = [block_diagonal(col_t[b]) for b in bands]
        lhs = [
            [jnp.concatenate([oh_s[b * NBLK + j, :HALF, 2 * LAT :], oh_s[b * NBLK + j, HALF:, 2 * LAT :]], axis=1) for j in range(NBLK)]
            for b in bands
        ]
        for u, b in enumerate(bands):
            more = dot(jnp.concatenate(lhs[u], axis=0), tables[u])
            for j in range(NBLK):
                for h in range(2):
                    here = pl.ds(pl.multiple_of((b * NBLK + j) * BLK + h * HALF, HALF), HALF)
                    part_v[here, :] += more[j * HALF : (j + 1) * HALF, h * LAT : (h + 1) * LAT]
        return 0

    lax.fori_loop(0, BANDS // NP, halo_step, 0)
    tops = block_diagonal(top)
    lhs = [jnp.concatenate([oh_s[j, :HALF, LAT : 2 * LAT], oh_s[j, HALF:, LAT : 2 * LAT]], axis=1) for j in range(NBLK)]
    more = dot(jnp.concatenate(lhs, axis=0), tops)
    for j in range(NBLK):
        for h in range(2):
            here = slice(j * BLK + h * HALF, j * BLK + (h + 1) * HALF)
            part_v[here] += more[j * HALF : (j + 1) * HALF, h * LAT : (h + 1) * LAT]
    wn_first[...] = wn_in[...]
    prepare(wn_hid, wn_out, n_bias, n_gain, n_shift, wn_hid2, wn_out2, wn_avg2, n_vecs)
    for c in copies2:
        c.wait_recv()
    n, mean, m2 = combine([mine2[...]] + [got2[k] for k in range(1, n_col)])
    inv = lax.rsqrt(m2 / n + EPS)
    stats_out[...] = jnp.concatenate([mean, inv, jnp.zeros((6, LAT), F32)], axis=0)
    for c in halo_copies + copies + copies2:
        c.wait_send()


def exchange(nodes, edges, counts, *small):
    n_row, n_col = lax.axis_size("row"), lax.axis_size("col")
    hbm, vmem = pl.BlockSpec(memory_space=pltpu.HBM), pl.BlockSpec(memory_space=pltpu.VMEM)
    pin = lambda a: pltpu.with_memory_space_constraint(a, pltpu.HBM)
    square = pltpu.VMEM((256, 256), BF16)
    outs = (
        pltpu.VMEM((8, LAT), F32),
        pltpu.VMEM(((TRASH + 1) * BLK, LAT), BF16),
        pltpu.VMEM(((TRASH + 1) * BLK, LAT), F32),
        pltpu.VMEM((ROWS, COLS, LAT), BF16),
        pltpu.VMEM((NBLK, 24, BLK), F32),
        square, square, square, square, pltpu.VMEM((8, 256), F32),
        pltpu.VMEM((2 * LAT, LAT), BF16), square, square, square, pltpu.VMEM((8, 256), F32),
    )
    return pl.pallas_call(
        exchange_kernel,
        out_shape=outs,
        in_specs=[hbm] * (3 + N_SMALL),
        out_specs=(vmem,) * len(outs),
        scratch_shapes=[pltpu.VMEM(a.shape, a.dtype) for a in small]
        + [
            pltpu.VMEM((2, ROWS, LAT), BF16),
            pltpu.VMEM((256, LAT), BF16),
            pltpu.VMEM((4, LAT), F32),
            pltpu.VMEM((4, LAT), F32),
            pltpu.VMEM((n_row, 4, LAT), F32),
            pltpu.VMEM((n_col, 4, LAT), F32),
            pltpu.VMEM((ROWS * COLS + 2 * COLS, LAT), BF16),
            pltpu.VMEM((ROWS * COLS, LAT), BF16),
            pltpu.VMEM((BANDS, BAND_NODES, LAT), BF16),
            pltpu.VMEM((2, 72, LAT), F32),
            pltpu.VMEM((NBLK, 24, BLK), F32),
            pltpu.VMEM((TRASH, BLK, 384), BF16),
            pltpu.SMEM((1, BANDS), jnp.int32),
            pltpu.SemaphoreType.DMA,
            pltpu.SemaphoreType.DMA((BANDS,)),
            pltpu.SemaphoreType.DMA,
            pltpu.SemaphoreType.DMA((N_SMALL,)),
            pltpu.SemaphoreType.DMA((8,)),
            pltpu.SemaphoreType.DMA((8,)),
            pltpu.SemaphoreType.DMA((n_row,)),
            pltpu.SemaphoreType.DMA((n_row,)),
            pltpu.SemaphoreType.DMA((n_col,)),
            pltpu.SemaphoreType.DMA((n_col,)),
        ],
        compiler_params=pltpu.CompilerParams(
            collective_id=0, has_side_effects=True, vmem_limit_bytes=24 * 1024 * 1024
        ),
        name="exchange",
    )(pin(nodes), pin(edges), pin(counts), *[pin(a) for a in small])


def main_kernel(
    counts, stats, edges_v, part_v, nodes, ridx, w_x2, w_hid2, w_out2, w_avg2, vecs,
    wn_in, wn_hid2, wn_out2, wn_avg2, n_vecs,
    new_nodes, edges_out,
    out_v, zeros_v, acc, work, x_ring, h2_s, nodes_s, out_sem, node_sem,
):
    zeros_v[...] = jnp.zeros_like(zeros_v)

    place = jnp.int32(0)
    for b in range(BANDS):
        count = counts[0, b]
        for j in range(NBLK):
            work[place + NB * STAGES] = jnp.int32(b * NBLK + j)
            place = place + (count > j * BLK).astype(jnp.int32)
    for k in range(NB * STAGES):
        work[k] = jnp.int32(TRASH)
    for k in range(NB * (STAGES + 1)):
        work[place + NB * STAGES + k] = jnp.int32(TRASH)
    acc[...] = jnp.zeros_like(acc)
    for b in range(BANDS):
        for j in range(2, NBLK):

            @pl.when(counts[0, b] <= j * BLK)
            def _():
                pltpu.make_async_copy(
                    zeros_v, edges_out.at[pl.ds(b * SLOTS + j * BLK, BLK)], out_sem
                ).start()

    mean, inv = stats[0:1], stats[1:2]
    node_id = lax.broadcasted_iota(jnp.int32, (BAND_NODES, BLK), 0).astype(F32).astype(BF16)
    one, nought = jnp.ones((), BF16), jnp.zeros((), BF16)

    def item(i, stage, u):
        return work[(i + STAGES - stage) * NB + u]

    slot_id = lax.broadcasted_iota(jnp.int32, (HALF, LAT), 0).astype(F32).astype(BF16)
    bias2, shift = vecs[0:1].astype(BF16), vecs[2:3].astype(BF16)
    us = range(NB)

    def where_of(i, stage):
        ks = [item(i, stage, u) for u in us]
        return ks, [lax.shift_right_logical(k, 2) for k in ks], [lax.rem(k, NBLK) for k in ks]

    def half_rows(k, h):
        return pl.ds(pl.multiple_of(k * BLK + h * HALF, HALF), HALF)

    def scatter(i):
        k2, b2, j2 = where_of(i, 2)
        rows = [ridx[j2[u], pl.ds(b2[u], 1), :].astype(BF16) for u in us]
        for u in us:
            pick = jnp.where(node_id == rows[u], one, nought)
            acc[b2[u]] += dot(pick, out_v[pl.ds(pl.multiple_of(k2[u] * BLK, BLK), BLK), :])

    groups = range(NB // GROUP)

    def rows_of(g, t):
        return slice((g * GROUP + t) * HALF, (g * GROUP + t + 1) * HALF)

    def group(g):
        return slice(g * GROUP * HALF, (g + 1) * GROUP * HALF)

    def output():
        return [dot(h2_s[group(g)], w_out2[...]) + vecs[1:2] for g in groups]

    def first(i):
        k0, _, _ = where_of(i, 0)
        new = lax.rem(i, RING)
        h1s = []
        for g in groups:
            xs, parts = [], []
            for t in range(GROUP):
                k = k0[g * GROUP + t]
                halves = [((edges_v[half_rows(k, h), :].astype(F32) - mean) * inv).astype(BF16) for h in range(2)]
                xs.append(jnp.concatenate(halves, axis=1))
                parts.append(jnp.concatenate([part_v[half_rows(k, h), :] for h in range(2)], axis=1))
            x = jnp.concatenate(xs, axis=0)
            x_ring[new, group(g)] = x
            h1 = dot(x, w_x2[...]) + jnp.concatenate(parts, axis=0)
            h1s.append(jnp.maximum(h1.astype(BF16), nought))
        return h1s

    def variance(cgs):
        weight = vecs[4:5, 0:LAT]
        results = []
        for cg in cgs:
            halves = []
            for h in range(2):
                v = cg[:, h * LAT : (h + 1) * LAT]
                mean_sq = jnp.sum(v * v * weight, axis=1, keepdims=True)
                halves.append(jnp.broadcast_to(mean_sq, v.shape))
            results.append(jnp.concatenate(halves, axis=1))
        return results

    def finish(i, cgs, variances):
        k1, b1, j1 = where_of(i, 1)
        old = lax.rem(i + RING - 1, RING)
        for g in groups:
            scaled = (cgs[g] * lax.rsqrt(variances[g] + EPS)).astype(BF16) + (x_ring[old, group(g)] + shift)
            for t in range(GROUP):
                u = g * GROUP + t
                left_count = counts[0, jnp.minimum(b1[u], BANDS - 1)] - j1[u] * BLK
                for h in range(2):
                    bound = jnp.clip(left_count - h * HALF, 0, HALF).astype(F32)
                    bound = jnp.full((HALF, LAT), bound).astype(BF16)
                    v = scaled[t * HALF : (t + 1) * HALF, h * LAT : (h + 1) * LAT]
                    out_v[half_rows(k1[u], h), :] = jnp.where(slot_id < bound, v, nought)

    def hidden(h1s):
        for g in groups:
            h2_s[group(g)] = jnp.maximum(dot(h1s[g], w_hid2[...]).astype(BF16) + bias2, nought)

    def step(i, _):
        scatter(i)
        cgs = output()
        h1s = first(i)
        variances = variance(cgs)
        finish(i, cgs, variances)
        hidden(h1s)
        for u in range(NB):
            k = item(i, 1, u)

            @pl.when(k < TRASH)
            def _():
                pltpu.make_async_copy(
                    out_v.at[pl.ds(pl.multiple_of(k * BLK, BLK), BLK)],
                    edges_out.at[pl.ds(pl.multiple_of(k * BLK, BLK), BLK)],
                    out_sem,
                ).start()
        return 0

    steps = lax.div(place + (NB - 1), NB) + 1
    hidden(first(0))
    lax.fori_loop(1, steps, step, 0)
    scatter(steps)

    size = 2 * BLK
    chunks = range(ROWS * COLS // size)
    low_bias2, low_shift = n_vecs[0:1].astype(BF16), n_vecs[2:3].astype(BF16)
    owns = [nodes[k * 16 : (k + 1) * 16].reshape(size, LAT) for k in chunks]
    hs = []
    for k in chunks:
        gathered = jnp.concatenate([acc[k * 4 + t] for t in range(4)], axis=0).astype(BF16)
        h = dot(jnp.concatenate([owns[k], gathered], axis=1), wn_in[...]) + n_vecs[3:4, 0:LAT]
        h = jnp.maximum(h.astype(BF16), nought)
        hs.append(jnp.concatenate([h[:BLK], h[BLK:]], axis=1))
    hs = [jnp.maximum(dot(hs[k], wn_hid2[...]).astype(BF16) + low_bias2, nought) for k in chunks]
    cgs = [dot(hs[k], wn_out2[...]) + n_vecs[1:2] for k in chunks]
    lows = [cgs[k].astype(BF16) for k in chunks]
    variances = [dot(lows[k] * lows[k], wn_avg2[...]) for k in chunks]
    node_copies = []
    for k in chunks:
        v = (cgs[k] * lax.rsqrt(variances[k] + EPS)).astype(BF16) + low_shift
        nodes_s[k * size : k * size + BLK] = v[:, :LAT] + owns[k][:BLK]
        nodes_s[k * size + BLK : (k + 1) * size] = v[:, LAT:] + owns[k][BLK:]
        here = pl.ds(k * size, size)
        c = pltpu.make_async_copy(nodes_s.at[here], new_nodes.at[here], node_sem.at[k])
        c.start()
        node_copies.append(c)
    for c in node_copies:
        c.wait()
    pltpu.make_async_copy(out_v.at[pl.ds(0, BANDS * SLOTS)], edges_out, out_sem).wait()


def process(counts, *held):
    vmem, smem = pl.BlockSpec(memory_space=pltpu.VMEM), pl.BlockSpec(memory_space=pltpu.SMEM)
    pin = lambda a: pltpu.with_memory_space_constraint(a, pltpu.VMEM)
    return pl.pallas_call(
        main_kernel,
        out_shape=(
            jax.ShapeDtypeStruct((ROWS * COLS, LAT), BF16),
            jax.ShapeDtypeStruct((BANDS * SLOTS, LAT), BF16),
        ),
        in_specs=[smem] + [vmem] * len(held),
        out_specs=(pl.BlockSpec(memory_space=pl.ANY), pl.BlockSpec(memory_space=pl.ANY)),
        scratch_shapes=[
            pltpu.VMEM(((TRASH + 1) * BLK, LAT), BF16),
            pltpu.VMEM((BLK, LAT), BF16),
            pltpu.VMEM((BANDS + 1, BAND_NODES, LAT), F32),
            pltpu.SMEM((TRASH + NB * (2 * STAGES + 2),), jnp.int32),
            pltpu.VMEM((RING, NB * HALF, 256), BF16),
            pltpu.VMEM((NB * HALF, 256), BF16),
            pltpu.VMEM((ROWS * COLS, LAT), BF16),
            pltpu.SemaphoreType.DMA,
            pltpu.SemaphoreType.DMA((4,)),
        ],
        compiler_params=pltpu.CompilerParams(vmem_limit_bytes=32 * 1024 * 1024),
        name="process",
    )(counts, *[pin(a) for a in held])


def per_device(
    nodes, edges, senders, receivers, counts,
    w_edge_in, w_edge_hid, w_edge_out, edge_bias, edge_gain, edge_shift,
    w_node_in, w_node_hid, w_node_out, node_bias, node_gain, node_shift,
):
    flat_edges = edges.reshape(BANDS * SLOTS, LAT)
    count_row = counts.reshape(1, BANDS)
    held = exchange(
        nodes, flat_edges, count_row, senders.reshape(BANDS, SLOTS), receivers.reshape(BANDS, SLOTS),
        w_edge_in, w_edge_hid, w_edge_out, edge_bias, edge_gain.reshape(1, LAT), edge_shift.reshape(1, LAT),
        w_node_in, w_node_hid, w_node_out, node_bias, node_gain.reshape(1, LAT), node_shift.reshape(1, LAT),
    )
    new_nodes, new_edges = process(count_row, *held)
    return new_nodes.reshape(nodes.shape), new_edges.reshape(edges.shape)


def solution(mesh):
    in_specs = (
        P("row", "col", None),
        P("row", "col", None, None, None),
        P("row", "col", None, None),
        P("row", "col", None, None),
        P("row", "col", None),
    ) + (P(),) * 12
    out_specs = (P("row", "col", None), P("row", "col", None, None, None))
    return jax.shard_map(
        per_device, mesh=mesh, in_specs=in_specs, out_specs=out_specs, check_vma=False
    )
```

```python
import functools

import jax
import jax.numpy as jnp
from jax import lax
from jax.experimental import pallas as pl
from jax.experimental.pallas import tpu as pltpu
from jax.sharding import PartitionSpec as P

F32 = jnp.float32
BF16 = jnp.bfloat16
LAT = 128
ROWS = 64
COLS = 32
BANDS = 16
SLOTS = 1024
BAND_NODES = 128
BLK = 256
HALF = BLK // 2
NBLK = SLOTS // BLK
NA = 8
SPLIT = 5
NP = 16
NB = 4
GROUP = 2
RING = 2
STAGES = 2
TRASH = BANDS * NBLK
EPS = 1e-5
MESH = pl.DeviceIdType.MESH


def tree_sum(terms):
    while len(terms) > 1:
        terms = [functools.reduce(jnp.add, terms[k : k + 2]) for k in range(0, len(terms), 2)]
    return terms[0]


def combine(parts):
    n = tree_sum([p[0:1] for p in parts])
    mean = tree_sum([p[0:1] * p[1:2] for p in parts]) / n
    m2 = tree_sum([p[2:3] + p[0:1] * (p[1:2] - mean) * (p[1:2] - mean) for p in parts])
    return n, mean, m2


def dot(a, b):
    return jnp.dot(a, b, preferred_element_type=F32)


def block_diagonal(w):
    z = jnp.zeros_like(w)
    return jnp.concatenate(
        [jnp.concatenate([w, z], axis=1), jnp.concatenate([z, w], axis=1)], axis=0
    )


def twice(v):
    return jnp.concatenate([v, v], axis=1)


def norm_weights(w_out, bias, gain):
    w = w_out.astype(F32)
    w = (w - jnp.mean(w, axis=1, keepdims=True)) * gain
    b = (bias - jnp.mean(bias, axis=1, keepdims=True)) * gain
    weights = jnp.transpose(jnp.broadcast_to(1.0 / (LAT * gain * gain), (LAT, LAT)))
    return w.astype(BF16), b, weights.astype(BF16)


def prepare(hid, out, bias, gain, shift, hid2, out2, avg2, vecs):
    hid2[...] = block_diagonal(hid[...])
    w, b3, avg = norm_weights(out[...], bias[2:3], gain[...])
    out2[...] = block_diagonal(w)
    avg2[...] = block_diagonal(avg)
    vecs[0:1] = twice(bias[1:2])
    vecs[1:2] = twice(b3)
    vecs[2:3] = twice(shift[...])
    vecs[3:4] = twice(bias[0:1])
    vecs[4:5] = twice(1.0 / (LAT * gain[...] * gain[...]))


N_SMALL = 14


def exchange_kernel(*refs):
    nodes_hbm, edges_hbm, counts_hbm = refs[:3]
    small_hbm = refs[3 : 3 + N_SMALL]
    (
        stats_out, edges_v, part_v, nodes_v, ridx, w_x2, w_hid2, w_out2, w_avg2, vecs,
        wn_first, wn_hid2, wn_out2, wn_avg2, n_vecs,
    ) = refs[3 + N_SMALL : 18 + N_SMALL]
    small = refs[18 + N_SMALL : 18 + 2 * N_SMALL]
    (
        cols_v, halo_v, mine1, mine2, got1, got2, ps_t, pr_t, col_t, lr, sidx, oh_s, counts,
        count_sem, edge_sem, node_sem, small_sem, hs_sem, hr_sem, s1_sem, r1_sem, s2_sem, r2_sem,
    ) = refs[18 + 2 * N_SMALL :]
    (
        senders, receivers, w_in, w_hid, w_out, e_bias, e_gain, e_shift,
        wn_in, wn_hid, wn_out, n_bias, n_gain, n_shift,
    ) = small
    n_row, n_col = lax.axis_size("row"), lax.axis_size("col")
    row, col = lax.axis_index("row"), lax.axis_index("col")
    up, down = lax.rem(row + n_row - 1, n_row), lax.rem(row + 1, n_row)
    left, right = lax.rem(col + n_col - 1, n_col), lax.rem(col + 1, n_col)

    def edge_copy(b):
        return pltpu.make_async_copy(
            edges_hbm.at[pl.ds(b * SLOTS, SLOTS)], edges_v.at[pl.ds(b * SLOTS, SLOTS)], edge_sem.at[b]
        )

    node_copy = pltpu.make_async_copy(nodes_hbm, nodes_v, node_sem)
    for b in range(2):
        edge_copy(b).start()
    count_copy = pltpu.make_async_copy(counts_hbm, counts, count_sem)
    count_copy.start()
    barrier = pltpu.get_barrier_semaphore()
    peers = [(row, lax.rem(col + k, n_col)) for k in range(1, n_col)]
    peers += [(lax.rem(row + k, n_row), col) for k in range(1, n_row)]
    peers += [(up, left), (up, right), (down, left), (down, right)]
    for p in peers:
        pl.semaphore_signal(barrier, inc=1, device_id=p, device_id_type=MESH)
    for b in range(2, BANDS):
        edge_copy(b).start()
    node_copy.start()
    small_copies = [
        pltpu.make_async_copy(src, dst, small_sem.at[k])
        for k, (src, dst) in enumerate(zip(small_hbm, small))
    ]
    for c in small_copies:
        c.start()

    count_copy.wait()
    edge_copy(0).wait()
    low_pivot = edges_v[0:16, :][0:1]
    pivot = low_pivot.astype(F32)
    slot_id = lax.broadcasted_iota(jnp.int32, (64, LAT), 0).astype(F32).astype(BF16)

    def band_sums(b, s, q):
        count = counts[0, b]
        for j in range(SLOTS // 64):
            x = edges_v[pl.ds(pl.multiple_of(b * SLOTS + j * 64, 64), 64), :]
            if j >= SLOTS // 128:
                bound = jnp.clip(count - j * 64, 0, 64).astype(F32)
                x = jnp.where(slot_id < jnp.full((64, LAT), bound).astype(BF16), x, low_pivot)
            d = x.astype(F32) - pivot
            e = d * d
            s = s + ((d[0:8] + d[8:16]) + (d[16:24] + d[24:32])) + ((d[32:40] + d[40:48]) + (d[48:56] + d[56:64]))
            q = q + ((e[0:8] + e[8:16]) + (e[16:24] + e[24:32])) + ((e[32:40] + e[40:48]) + (e[48:56] + e[56:64]))
        return s, q

    def band_stats(b, carry):
        edge_copy(b).wait()
        return band_sums(b, *carry)

    zero = jnp.zeros((8, LAT), F32)
    carry = band_sums(0, zero, zero)
    s, q = lax.fori_loop(1, BANDS, band_stats, carry)
    total = counts[0, 0]
    for b in range(1, BANDS):
        total = total + counts[0, b]
    n = jnp.full((1, LAT), total.astype(F32))
    s = jnp.sum(s, axis=0, keepdims=True)
    q = jnp.sum(q, axis=0, keepdims=True)
    local_mean = s / n
    filler = jnp.zeros((1, LAT), F32)
    mine1[...] = jnp.concatenate([n, pivot + local_mean, q - s * local_mean, filler], axis=0)

    node_copy.wait()
    cols_v[0] = nodes_v[:, 0, :]
    cols_v[1] = nodes_v[:, COLS - 1, :]
    pl.semaphore_wait(barrier, len(peers))
    copies = []
    for k in range(1, n_row):
        c = pltpu.make_async_remote_copy(
            src_ref=mine1, dst_ref=got1.at[k], send_sem=s1_sem.at[k], recv_sem=r1_sem.at[k],
            device_id=(lax.rem(row + k, n_row), col), device_id_type=MESH,
        )
        c.start()
        copies.append(c)

    sends = [
        (nodes_v.at[ROWS - 1], (0, 32), (down, col)),
        (nodes_v.at[0], (32, 32), (up, col)),
        (cols_v.at[1], (64, 64), (row, right)),
        (cols_v.at[0], (128, 64), (row, left)),
        (cols_v.at[1, pl.ds(48, 16)], (192, 16), (down, right)),
        (cols_v.at[0, pl.ds(48, 16)], (208, 16), (down, left)),
        (cols_v.at[1, pl.ds(0, 16)], (224, 16), (up, right)),
        (cols_v.at[0, pl.ds(0, 16)], (240, 16), (up, left)),
    ]
    halo_copies = []
    for k, (src, (start, size), dev) in enumerate(sends):
        c = pltpu.make_async_remote_copy(
            src_ref=src, dst_ref=halo_v.at[pl.ds(start, size)],
            send_sem=hs_sem.at[k], recv_sem=hr_sem.at[k], device_id=dev, device_id_type=MESH,
        )
        c.start()
        halo_copies.append(c)

    for c in small_copies:
        c.wait()
    w_snd, w_rcv = w_in[LAT : 2 * LAT], w_in[2 * LAT :]
    w_both = jnp.concatenate([w_snd, w_rcv], axis=1)
    bias1 = e_bias[0:1]
    for k in range(ROWS * COLS // BLK):
        own = nodes_v[k * 8 : (k + 1) * 8].reshape(BLK, LAT)
        p = dot(own, w_both)
        ps_t[COLS + k * BLK : COLS + (k + 1) * BLK] = p[:, :LAT].astype(BF16)
        pr_t[k * BLK : (k + 1) * BLK] = (p[:, LAT:] + bias1).astype(BF16)

    s = senders[...]
    r = lax.shift_right_logical(s * 241, 13)
    c = s - r * 34
    place_s = jnp.where(c == 0, 192 + r, jnp.where(c == 33, 200 + r, r * 32 + c - 1)).astype(F32)
    place_r = receivers[...].astype(F32)
    for j in range(NBLK):
        sidx[j, 0:BANDS] = place_s[:, j * BLK : (j + 1) * BLK]
        ridx[j, 0:BANDS] = place_r[:, j * BLK : (j + 1) * BLK]

    w_x2[...] = block_diagonal(w_in[0:LAT])
    prepare(w_hid, w_out, e_bias, e_gain, e_shift, w_hid2, w_out2, w_avg2, vecs)

    node_id = lax.broadcasted_iota(jnp.int32, (256, BLK), 0).astype(F32).astype(BF16)
    one, nought = jnp.ones((), BF16), jnp.zeros((), BF16)

    ps_t[0:COLS] = jnp.zeros((COLS, LAT), BF16)
    ps_t[COLS + ROWS * COLS :] = jnp.zeros((COLS, LAT), BF16)

    def one_hot(k):
        band, j = lax.div(k, NBLK), lax.rem(k, NBLK)
        si = sidx[j, pl.ds(band, 1), :].astype(BF16)
        ri = ridx[j, pl.ds(band, 1), :].astype(BF16)
        pick_s = jnp.where(node_id == si, one, nought)
        pick_r = jnp.where(node_id[:BAND_NODES] == ri, one, nought)
        oh_s[k, :, 0:LAT] = pick_r.T
        oh_s[k, :, LAT:] = pick_s.T

    def gather(k):
        start = pl.multiple_of(lax.div(k, NBLK) * BAND_NODES, BAND_NODES)
        table = jnp.concatenate(
            [pr_t[pl.ds(start, BAND_NODES), :], ps_t[pl.ds(start, 192), :], jnp.zeros((64, LAT), BF16)],
            axis=0,
        )
        part_v[pl.ds(pl.multiple_of(k * BLK, BLK), BLK), :] = dot(oh_s[k], table)

    last = TRASH // NA - 1
    for u in range(NA):
        one_hot(jnp.int32(u))

    def step(i, _):
        for u in range(NA):
            gather(i * NA + u)
        for u in range(NA):
            one_hot(jnp.minimum(i + 1, last) * NA + u)
        return 0

    lax.fori_loop(0, SPLIT, step, 0)
    for c in copies:
        c.wait_recv()
    n, mean, m2 = combine([mine1[...]] + [got1[k] for k in range(1, n_row)])
    mine2[...] = jnp.concatenate([n, mean, m2, filler], axis=0)
    copies2 = []
    for k in range(1, n_col):
        c = pltpu.make_async_remote_copy(
            src_ref=mine2, dst_ref=got2.at[k], send_sem=s2_sem.at[k], recv_sem=r2_sem.at[k],
            device_id=(row, lax.rem(col + k, n_col)), device_id_type=MESH,
        )
        c.start()
        copies2.append(c)
    lax.fori_loop(SPLIT, last + 1, step, 0)

    for c in halo_copies:
        c.wait_recv()
    p = dot(halo_v[...], w_snd)
    lr[0, 64:72] = jnp.zeros((8, LAT), F32)
    lr[1, 64:72] = jnp.zeros((8, LAT), F32)
    lr[0, 1:65] = p[64:128]
    lr[1, 1:65] = p[128:192]
    lr[0, 0:1] = p[207:208]
    lr[1, 0:1] = p[223:224]
    lr[0, 65:66] = p[224:225]
    lr[1, 65:66] = p[240:241]
    top = jnp.concatenate([p[0:32].astype(BF16), jnp.zeros((96, LAT), BF16)], axis=0)
    col_t[:, 0:64] = jnp.zeros((BANDS, 64, LAT), BF16)
    col_t[BANDS - 1, 32:64] = p[32:64].astype(BF16)
    col_t[:, 80:] = jnp.zeros((BANDS, 48, LAT), BF16)
    for b in range(BANDS):
        pair = jnp.concatenate([lr[0, 4 * b : 4 * b + 8], lr[1, 4 * b : 4 * b + 8]], axis=0)
        col_t[b, 64:80] = pair.astype(BF16)

    def halo_step(i, _):
        bands = [i * NP + u for u in range(NP)]
        tables = [block_diagonal(col_t[b]) for b in bands]
        lhs = [
            [jnp.concatenate([oh_s[b * NBLK + j, :HALF, 2 * LAT :], oh_s[b * NBLK + j, HALF:, 2 * LAT :]], axis=1) for j in range(NBLK)]
            for b in bands
        ]
        for u, b in enumerate(bands):
            more = dot(jnp.concatenate(lhs[u], axis=0), tables[u])
            for j in range(NBLK):
                for h in range(2):
                    here = pl.ds(pl.multiple_of((b * NBLK + j) * BLK + h * HALF, HALF), HALF)
                    part_v[here, :] += more[j * HALF : (j + 1) * HALF, h * LAT : (h + 1) * LAT]
        return 0

    lax.fori_loop(0, BANDS // NP, halo_step, 0)
    tops = block_diagonal(top)
    lhs = [jnp.concatenate([oh_s[j, :HALF, LAT : 2 * LAT], oh_s[j, HALF:, LAT : 2 * LAT]], axis=1) for j in range(NBLK)]
    more = dot(jnp.concatenate(lhs, axis=0), tops)
    for j in range(NBLK):
        for h in range(2):
            here = slice(j * BLK + h * HALF, j * BLK + (h + 1) * HALF)
            part_v[here] += more[j * HALF : (j + 1) * HALF, h * LAT : (h + 1) * LAT]
    wn_first[...] = wn_in[...]
    prepare(wn_hid, wn_out, n_bias, n_gain, n_shift, wn_hid2, wn_out2, wn_avg2, n_vecs)
    for c in halo_copies + copies + copies2:
        c.wait_send()
    for c in copies2:
        c.wait_recv()
    n, mean, m2 = combine([mine2[...]] + [got2[k] for k in range(1, n_col)])
    inv = lax.rsqrt(m2 / n + EPS)
    stats_out[...] = jnp.concatenate([mean, inv, jnp.zeros((6, LAT), F32)], axis=0)


def exchange(nodes, edges, counts, *small):
    n_row, n_col = lax.axis_size("row"), lax.axis_size("col")
    hbm, vmem = pl.BlockSpec(memory_space=pltpu.HBM), pl.BlockSpec(memory_space=pltpu.VMEM)
    pin = lambda a: pltpu.with_memory_space_constraint(a, pltpu.HBM)
    square = pltpu.VMEM((256, 256), BF16)
    outs = (
        pltpu.VMEM((8, LAT), F32),
        pltpu.VMEM(((TRASH + 1) * BLK, LAT), BF16),
        pltpu.VMEM(((TRASH + 1) * BLK, LAT), F32),
        pltpu.VMEM((ROWS, COLS, LAT), BF16),
        pltpu.VMEM((NBLK, 24, BLK), F32),
        square, square, square, square, pltpu.VMEM((8, 256), F32),
        pltpu.VMEM((2 * LAT, LAT), BF16), square, square, square, pltpu.VMEM((8, 256), F32),
    )
    return pl.pallas_call(
        exchange_kernel,
        out_shape=outs,
        in_specs=[hbm] * (3 + N_SMALL),
        out_specs=(vmem,) * len(outs),
        scratch_shapes=[pltpu.VMEM(a.shape, a.dtype) for a in small]
        + [
            pltpu.VMEM((2, ROWS, LAT), BF16),
            pltpu.VMEM((256, LAT), BF16),
            pltpu.VMEM((4, LAT), F32),
            pltpu.VMEM((4, LAT), F32),
            pltpu.VMEM((n_row, 4, LAT), F32),
            pltpu.VMEM((n_col, 4, LAT), F32),
            pltpu.VMEM((ROWS * COLS + 2 * COLS, LAT), BF16),
            pltpu.VMEM((ROWS * COLS, LAT), BF16),
            pltpu.VMEM((BANDS, BAND_NODES, LAT), BF16),
            pltpu.VMEM((2, 72, LAT), F32),
            pltpu.VMEM((NBLK, 24, BLK), F32),
            pltpu.VMEM((TRASH, BLK, 384), BF16),
            pltpu.SMEM((1, BANDS), jnp.int32),
            pltpu.SemaphoreType.DMA,
            pltpu.SemaphoreType.DMA((BANDS,)),
            pltpu.SemaphoreType.DMA,
            pltpu.SemaphoreType.DMA((N_SMALL,)),
            pltpu.SemaphoreType.DMA((8,)),
            pltpu.SemaphoreType.DMA((8,)),
            pltpu.SemaphoreType.DMA((n_row,)),
            pltpu.SemaphoreType.DMA((n_row,)),
            pltpu.SemaphoreType.DMA((n_col,)),
            pltpu.SemaphoreType.DMA((n_col,)),
        ],
        compiler_params=pltpu.CompilerParams(
            collective_id=0, has_side_effects=True, vmem_limit_bytes=24 * 1024 * 1024
        ),
        name="exchange",
    )(pin(nodes), pin(edges), pin(counts), *[pin(a) for a in small])


def main_kernel(
    counts, stats, edges_v, part_v, nodes, ridx, w_x2, w_hid2, w_out2, w_avg2, vecs,
    wn_in, wn_hid2, wn_out2, wn_avg2, n_vecs,
    new_nodes, edges_out,
    out_v, zeros_v, acc, work, x_ring, h2_s, nodes_s, out_sem, node_sem,
):
    zeros_v[...] = jnp.zeros_like(zeros_v)

    place = jnp.int32(0)
    for b in range(BANDS):
        count = counts[0, b]
        for j in range(NBLK):
            work[place + NB * STAGES] = jnp.int32(b * NBLK + j)
            place = place + (count > j * BLK).astype(jnp.int32)
    for k in range(NB * STAGES):
        work[k] = jnp.int32(TRASH)
    for k in range(NB * (STAGES + 1)):
        work[place + NB * STAGES + k] = jnp.int32(TRASH)
    acc[...] = jnp.zeros_like(acc)
    for b in range(BANDS):
        for j in range(2, NBLK):

            @pl.when(counts[0, b] <= j * BLK)
            def _():
                pltpu.make_async_copy(
                    zeros_v, edges_out.at[pl.ds(b * SLOTS + j * BLK, BLK)], out_sem
                ).start()

    mean, inv = stats[0:1], stats[1:2]
    node_id = lax.broadcasted_iota(jnp.int32, (BAND_NODES, BLK), 0).astype(F32).astype(BF16)
    one, nought = jnp.ones((), BF16), jnp.zeros((), BF16)

    def item(i, stage, u):
        return work[(i + STAGES - stage) * NB + u]

    slot_id = lax.broadcasted_iota(jnp.int32, (HALF, LAT), 0).astype(F32).astype(BF16)
    bias2, shift = vecs[0:1].astype(BF16), vecs[2:3].astype(BF16)
    us = range(NB)

    def where_of(i, stage):
        ks = [item(i, stage, u) for u in us]
        return ks, [lax.shift_right_logical(k, 2) for k in ks], [lax.rem(k, NBLK) for k in ks]

    def half_rows(k, h):
        return pl.ds(pl.multiple_of(k * BLK + h * HALF, HALF), HALF)

    def scatter(i):
        k2, b2, j2 = where_of(i, 2)
        rows = [ridx[j2[u], pl.ds(b2[u], 1), :].astype(BF16) for u in us]
        for u in us:
            pick = jnp.where(node_id == rows[u], one, nought)
            acc[b2[u]] += dot(pick, out_v[pl.ds(pl.multiple_of(k2[u] * BLK, BLK), BLK), :])

    groups = range(NB // GROUP)

    def rows_of(g, t):
        return slice((g * GROUP + t) * HALF, (g * GROUP + t + 1) * HALF)

    def group(g):
        return slice(g * GROUP * HALF, (g + 1) * GROUP * HALF)

    def output():
        return [dot(h2_s[group(g)], w_out2[...]) + vecs[1:2] for g in groups]

    def first(i):
        k0, _, _ = where_of(i, 0)
        new = lax.rem(i, RING)
        h1s = []
        for g in groups:
            xs, parts = [], []
            for t in range(GROUP):
                k = k0[g * GROUP + t]
                halves = [((edges_v[half_rows(k, h), :].astype(F32) - mean) * inv).astype(BF16) for h in range(2)]
                xs.append(jnp.concatenate(halves, axis=1))
                parts.append(jnp.concatenate([part_v[half_rows(k, h), :] for h in range(2)], axis=1))
            x = jnp.concatenate(xs, axis=0)
            x_ring[new, group(g)] = x
            h1 = dot(x, w_x2[...]) + jnp.concatenate(parts, axis=0)
            h1s.append(jnp.maximum(h1.astype(BF16), nought))
        return h1s

    def variance(cgs):
        weight = vecs[4:5, 0:LAT]
        results = []
        for cg in cgs:
            halves = []
            for h in range(2):
                v = cg[:, h * LAT : (h + 1) * LAT]
                mean_sq = jnp.sum(v * v * weight, axis=1, keepdims=True)
                halves.append(jnp.broadcast_to(mean_sq, v.shape))
            results.append(jnp.concatenate(halves, axis=1))
        return results

    def finish(i, cgs, variances):
        k1, b1, j1 = where_of(i, 1)
        old = lax.rem(i + RING - 1, RING)
        for g in groups:
            scaled = (cgs[g] * lax.rsqrt(variances[g] + EPS)).astype(BF16) + (x_ring[old, group(g)] + shift)
            for t in range(GROUP):
                u = g * GROUP + t
                left_count = counts[0, jnp.minimum(b1[u], BANDS - 1)] - j1[u] * BLK
                for h in range(2):
                    bound = jnp.clip(left_count - h * HALF, 0, HALF).astype(F32)
                    bound = jnp.full((HALF, LAT), bound).astype(BF16)
                    v = scaled[t * HALF : (t + 1) * HALF, h * LAT : (h + 1) * LAT]
                    out_v[half_rows(k1[u], h), :] = jnp.where(slot_id < bound, v, nought)

    def hidden(h1s):
        for g in groups:
            h2_s[group(g)] = jnp.maximum(dot(h1s[g], w_hid2[...]).astype(BF16) + bias2, nought)

    def step(i, _):
        scatter(i)
        cgs = output()
        h1s = first(i)
        variances = variance(cgs)
        finish(i, cgs, variances)
        hidden(h1s)
        for u in range(NB):
            k = item(i, 1, u)

            @pl.when(k < TRASH)
            def _():
                pltpu.make_async_copy(
                    out_v.at[pl.ds(pl.multiple_of(k * BLK, BLK), BLK)],
                    edges_out.at[pl.ds(pl.multiple_of(k * BLK, BLK), BLK)],
                    out_sem,
                ).start()
        return 0

    steps = lax.div(place + (NB - 1), NB) + 1
    hidden(first(0))
    lax.fori_loop(1, steps, step, 0)
    scatter(steps)

    size = 2 * BLK
    chunks = range(ROWS * COLS // size)
    low_bias2, low_shift = n_vecs[0:1].astype(BF16), n_vecs[2:3].astype(BF16)
    owns = [nodes[k * 16 : (k + 1) * 16].reshape(size, LAT) for k in chunks]
    hs = []
    for k in chunks:
        gathered = jnp.concatenate([acc[k * 4 + t] for t in range(4)], axis=0).astype(BF16)
        h = dot(jnp.concatenate([owns[k], gathered], axis=1), wn_in[...]) + n_vecs[3:4, 0:LAT]
        h = jnp.maximum(h.astype(BF16), nought)
        hs.append(jnp.concatenate([h[:BLK], h[BLK:]], axis=1))
    hs = [jnp.maximum(dot(hs[k], wn_hid2[...]).astype(BF16) + low_bias2, nought) for k in chunks]
    cgs = [dot(hs[k], wn_out2[...]) + n_vecs[1:2] for k in chunks]
    lows = [cgs[k].astype(BF16) for k in chunks]
    variances = [dot(lows[k] * lows[k], wn_avg2[...]) for k in chunks]
    node_copies = []
    for k in chunks:
        v = (cgs[k] * lax.rsqrt(variances[k] + EPS)).astype(BF16) + low_shift
        nodes_s[k * size : k * size + BLK] = v[:, :LAT] + owns[k][:BLK]
        nodes_s[k * size + BLK : (k + 1) * size] = v[:, LAT:] + owns[k][BLK:]
        here = pl.ds(k * size, size)
        c = pltpu.make_async_copy(nodes_s.at[here], new_nodes.at[here], node_sem.at[k])
        c.start()
        node_copies.append(c)
    for c in node_copies:
        c.wait()
    pltpu.make_async_copy(out_v.at[pl.ds(0, BANDS * SLOTS)], edges_out, out_sem).wait()


def process(counts, *held):
    vmem, smem = pl.BlockSpec(memory_space=pltpu.VMEM), pl.BlockSpec(memory_space=pltpu.SMEM)
    pin = lambda a: pltpu.with_memory_space_constraint(a, pltpu.VMEM)
    return pl.pallas_call(
        main_kernel,
        out_shape=(
            jax.ShapeDtypeStruct((ROWS * COLS, LAT), BF16),
            jax.ShapeDtypeStruct((BANDS * SLOTS, LAT), BF16),
        ),
        in_specs=[smem] + [vmem] * len(held),
        out_specs=(pl.BlockSpec(memory_space=pl.ANY), pl.BlockSpec(memory_space=pl.ANY)),
        scratch_shapes=[
            pltpu.VMEM(((TRASH + 1) * BLK, LAT), BF16),
            pltpu.VMEM((BLK, LAT), BF16),
            pltpu.VMEM((BANDS + 1, BAND_NODES, LAT), F32),
            pltpu.SMEM((TRASH + NB * (2 * STAGES + 2),), jnp.int32),
            pltpu.VMEM((RING, NB * HALF, 256), BF16),
            pltpu.VMEM((NB * HALF, 256), BF16),
            pltpu.VMEM((ROWS * COLS, LAT), BF16),
            pltpu.SemaphoreType.DMA,
            pltpu.SemaphoreType.DMA((4,)),
        ],
        compiler_params=pltpu.CompilerParams(vmem_limit_bytes=32 * 1024 * 1024),
        name="process",
    )(counts, *[pin(a) for a in held])


def per_device(
    nodes, edges, senders, receivers, counts,
    w_edge_in, w_edge_hid, w_edge_out, edge_bias, edge_gain, edge_shift,
    w_node_in, w_node_hid, w_node_out, node_bias, node_gain, node_shift,
):
    flat_edges = edges.reshape(BANDS * SLOTS, LAT)
    count_row = counts.reshape(1, BANDS)
    held = exchange(
        nodes, flat_edges, count_row, senders.reshape(BANDS, SLOTS), receivers.reshape(BANDS, SLOTS),
        w_edge_in, w_edge_hid, w_edge_out, edge_bias, edge_gain.reshape(1, LAT), edge_shift.reshape(1, LAT),
        w_node_in, w_node_hid, w_node_out, node_bias, node_gain.reshape(1, LAT), node_shift.reshape(1, LAT),
    )
    new_nodes, new_edges = process(count_row, *held)
    return new_nodes.reshape(nodes.shape), new_edges.reshape(edges.shape)


def solution(mesh):
    in_specs = (
        P("row", "col", None),
        P("row", "col", None, None, None),
        P("row", "col", None, None),
        P("row", "col", None, None),
        P("row", "col", None),
    ) + (P(),) * 12
    out_specs = (P("row", "col", None), P("row", "col", None, None, None))
    return jax.shard_map(
        per_device, mesh=mesh, in_specs=in_specs, out_specs=out_specs, check_vma=False
    )
```

```python
import functools

import jax
import jax.numpy as jnp
from jax import lax
from jax.experimental import pallas as pl
from jax.experimental.pallas import tpu as pltpu
from jax.sharding import PartitionSpec as P

F32 = jnp.float32
BF16 = jnp.bfloat16
LAT = 128
ROWS = 64
COLS = 32
BANDS = 16
SLOTS = 1024
BAND_NODES = 128
BLK = 256
HALF = BLK // 2
NBLK = SLOTS // BLK
NA = 8
SPLIT = 5
NP = 16
NB = 4
GROUP = 2
RING = 2
STAGES = 2
TRASH = BANDS * NBLK
EPS = 1e-5
MESH = pl.DeviceIdType.MESH


def tree_sum(terms):
    while len(terms) > 1:
        terms = [functools.reduce(jnp.add, terms[k : k + 2]) for k in range(0, len(terms), 2)]
    return terms[0]


def combine(parts):
    n = tree_sum([p[0:1] for p in parts])
    mean = tree_sum([p[0:1] * p[1:2] for p in parts]) / n
    m2 = tree_sum([p[2:3] + p[0:1] * (p[1:2] - mean) * (p[1:2] - mean) for p in parts])
    return n, mean, m2


def dot(a, b):
    return jnp.dot(a, b, preferred_element_type=F32)


def block_diagonal(w):
    z = jnp.zeros_like(w)
    return jnp.concatenate(
        [jnp.concatenate([w, z], axis=1), jnp.concatenate([z, w], axis=1)], axis=0
    )


def twice(v):
    return jnp.concatenate([v, v], axis=1)


def norm_weights(w_out, bias, gain):
    w = w_out.astype(F32)
    w = (w - jnp.mean(w, axis=1, keepdims=True)) * gain
    b = (bias - jnp.mean(bias, axis=1, keepdims=True)) * gain
    weights = jnp.transpose(jnp.broadcast_to(1.0 / (LAT * gain * gain), (LAT, LAT)))
    return w.astype(BF16), b, weights.astype(BF16)


def prepare(hid, out, bias, gain, shift, hid2, out2, avg2, vecs):
    hid2[...] = block_diagonal(hid[...])
    w, b3, avg = norm_weights(out[...], bias[2:3], gain[...])
    out2[...] = block_diagonal(w)
    avg2[...] = block_diagonal(avg)
    vecs[0:1] = twice(bias[1:2])
    vecs[1:2] = twice(b3)
    vecs[2:3] = twice(shift[...])
    vecs[3:4] = twice(bias[0:1])
    vecs[4:5] = twice(1.0 / (LAT * gain[...] * gain[...]))


N_SMALL = 14


def exchange_kernel(*refs):
    nodes_hbm, edges_hbm, counts_hbm = refs[:3]
    small_hbm = refs[3 : 3 + N_SMALL]
    (
        stats_out, edges_v, part_v, nodes_v, ridx, w_x2, w_hid2, w_out2, w_avg2, vecs,
        wn_first, wn_hid2, wn_out2, wn_avg2, n_vecs,
    ) = refs[3 + N_SMALL : 18 + N_SMALL]
    small = refs[18 + N_SMALL : 18 + 2 * N_SMALL]
    (
        cols_v, halo_v, mine1, mine2, got1, got2, ps_t, pr_t, col_t, lr, sidx, oh_s, counts,
        count_sem, edge_sem, node_sem, small_sem, hs_sem, hr_sem, s1_sem, r1_sem, s2_sem, r2_sem,
    ) = refs[18 + 2 * N_SMALL :]
    (
        senders, receivers, w_in, w_hid, w_out, e_bias, e_gain, e_shift,
        wn_in, wn_hid, wn_out, n_bias, n_gain, n_shift,
    ) = small
    n_row, n_col = lax.axis_size("row"), lax.axis_size("col")
    row, col = lax.axis_index("row"), lax.axis_index("col")
    up, down = lax.rem(row + n_row - 1, n_row), lax.rem(row + 1, n_row)
    left, right = lax.rem(col + n_col - 1, n_col), lax.rem(col + 1, n_col)

    def edge_copy(b):
        return pltpu.make_async_copy(
            edges_hbm.at[pl.ds(b * SLOTS, SLOTS)], edges_v.at[pl.ds(b * SLOTS, SLOTS)], edge_sem.at[b]
        )

    node_copy = pltpu.make_async_copy(nodes_hbm, nodes_v, node_sem)
    for b in range(2):
        edge_copy(b).start()
    count_copy = pltpu.make_async_copy(counts_hbm, counts, count_sem)
    count_copy.start()
    barrier = pltpu.get_barrier_semaphore()
    peers = [(row, lax.rem(col + k, n_col)) for k in range(1, n_col)]
    peers += [(lax.rem(row + k, n_row), col) for k in range(1, n_row)]
    peers += [(up, left), (up, right), (down, left), (down, right)]
    for p in peers:
        pl.semaphore_signal(barrier, inc=1, device_id=p, device_id_type=MESH)
    for b in range(2, BANDS):
        edge_copy(b).start()
    node_copy.start()
    small_copies = [
        pltpu.make_async_copy(src, dst, small_sem.at[k])
        for k, (src, dst) in enumerate(zip(small_hbm, small))
    ]
    for c in small_copies:
        c.start()

    count_copy.wait()
    edge_copy(0).wait()
    low_pivot = edges_v[0:16, :][0:1]
    pivot = low_pivot.astype(F32)
    slot_id = lax.broadcasted_iota(jnp.int32, (64, LAT), 0).astype(F32).astype(BF16)

    def band_sums(b, s, q):
        count = counts[0, b]
        for j in range(SLOTS // 64):
            x = edges_v[pl.ds(pl.multiple_of(b * SLOTS + j * 64, 64), 64), :]
            if j >= SLOTS // 128:
                bound = jnp.clip(count - j * 64, 0, 64).astype(F32)
                x = jnp.where(slot_id < jnp.full((64, LAT), bound).astype(BF16), x, low_pivot)
            d = x.astype(F32) - pivot
            e = d * d
            s = s + ((d[0:8] + d[8:16]) + (d[16:24] + d[24:32])) + ((d[32:40] + d[40:48]) + (d[48:56] + d[56:64]))
            q = q + ((e[0:8] + e[8:16]) + (e[16:24] + e[24:32])) + ((e[32:40] + e[40:48]) + (e[48:56] + e[56:64]))
        return s, q

    def band_stats(b, carry):
        edge_copy(b).wait()
        return band_sums(b, *carry)

    zero = jnp.zeros((8, LAT), F32)
    carry = band_sums(0, zero, zero)
    s, q = lax.fori_loop(1, BANDS, band_stats, carry)
    total = counts[0, 0]
    for b in range(1, BANDS):
        total = total + counts[0, b]
    n = jnp.full((1, LAT), total.astype(F32))
    s = jnp.sum(s, axis=0, keepdims=True)
    q = jnp.sum(q, axis=0, keepdims=True)
    local_mean = s / n
    filler = jnp.zeros((1, LAT), F32)
    mine1[...] = jnp.concatenate([n, pivot + local_mean, q - s * local_mean, filler], axis=0)

    node_copy.wait()
    cols_v[0] = nodes_v[:, 0, :]
    cols_v[1] = nodes_v[:, COLS - 1, :]
    pl.semaphore_wait(barrier, len(peers))
    copies = []
    for k in range(1, n_row):
        c = pltpu.make_async_remote_copy(
            src_ref=mine1, dst_ref=got1.at[k], send_sem=s1_sem.at[k], recv_sem=r1_sem.at[k],
            device_id=(lax.rem(row + k, n_row), col), device_id_type=MESH,
        )
        c.start()
        copies.append(c)

    sends = [
        (nodes_v.at[ROWS - 1], (0, 32), (down, col)),
        (nodes_v.at[0], (32, 32), (up, col)),
        (cols_v.at[1], (64, 64), (row, right)),
        (cols_v.at[0], (128, 64), (row, left)),
        (cols_v.at[1, pl.ds(48, 16)], (192, 16), (down, right)),
        (cols_v.at[0, pl.ds(48, 16)], (208, 16), (down, left)),
        (cols_v.at[1, pl.ds(0, 16)], (224, 16), (up, right)),
        (cols_v.at[0, pl.ds(0, 16)], (240, 16), (up, left)),
    ]
    halo_copies = []
    for k, (src, (start, size), dev) in enumerate(sends):
        c = pltpu.make_async_remote_copy(
            src_ref=src, dst_ref=halo_v.at[pl.ds(start, size)],
            send_sem=hs_sem.at[k], recv_sem=hr_sem.at[k], device_id=dev, device_id_type=MESH,
        )
        c.start()
        halo_copies.append(c)

    for c in small_copies:
        c.wait()
    w_snd, w_rcv = w_in[LAT : 2 * LAT], w_in[2 * LAT :]
    w_both = jnp.concatenate([w_snd, w_rcv], axis=1)
    bias1 = e_bias[0:1]
    for k in range(ROWS * COLS // BLK):
        own = nodes_v[k * 8 : (k + 1) * 8].reshape(BLK, LAT)
        p = dot(own, w_both)
        ps_t[COLS + k * BLK : COLS + (k + 1) * BLK] = p[:, :LAT].astype(BF16)
        pr_t[k * BLK : (k + 1) * BLK] = (p[:, LAT:] + bias1).astype(BF16)

    s = senders[...]
    r = lax.shift_right_logical(s * 241, 13)
    c = s - r * 34
    place_s = jnp.where(c == 0, 192 + r, jnp.where(c == 33, 200 + r, r * 32 + c - 1)).astype(F32)
    place_r = receivers[...].astype(F32)
    for j in range(NBLK):
        sidx[j, 0:BANDS] = place_s[:, j * BLK : (j + 1) * BLK]
        ridx[j, 0:BANDS] = place_r[:, j * BLK : (j + 1) * BLK]

    w_x2[...] = block_diagonal(w_in[0:LAT])
    prepare(w_hid, w_out, e_bias, e_gain, e_shift, w_hid2, w_out2, w_avg2, vecs)

    node_id = lax.broadcasted_iota(jnp.int32, (256, BLK), 0).astype(F32).astype(BF16)
    one, nought = jnp.ones((), BF16), jnp.zeros((), BF16)

    ps_t[0:COLS] = jnp.zeros((COLS, LAT), BF16)
    ps_t[COLS + ROWS * COLS :] = jnp.zeros((COLS, LAT), BF16)

    def one_hot(k):
        band, j = lax.div(k, NBLK), lax.rem(k, NBLK)
        si = sidx[j, pl.ds(band, 1), :].astype(BF16)
        ri = ridx[j, pl.ds(band, 1), :].astype(BF16)
        pick_s = jnp.where(node_id == si, one, nought)
        pick_r = jnp.where(node_id[:BAND_NODES] == ri, one, nought)
        oh_s[k, :, 0:LAT] = pick_r.T
        oh_s[k, :, LAT:] = pick_s.T

    def gather(k):
        start = pl.multiple_of(lax.div(k, NBLK) * BAND_NODES, BAND_NODES)
        table = jnp.concatenate(
            [pr_t[pl.ds(start, BAND_NODES), :], ps_t[pl.ds(start, 192), :], jnp.zeros((64, LAT), BF16)],
            axis=0,
        )
        part_v[pl.ds(pl.multiple_of(k * BLK, BLK), BLK), :] = dot(oh_s[k], table)

    last = TRASH // NA - 1
    for u in range(NA):
        one_hot(jnp.int32(u))

    def step(i, _):
        for u in range(NA):
            gather(i * NA + u)
        for u in range(NA):
            one_hot(jnp.minimum(i + 1, last) * NA + u)
        return 0

    lax.fori_loop(0, SPLIT, step, 0)
    for c in copies:
        c.wait_recv()
    n, mean, m2 = combine([mine1[...]] + [got1[k] for k in range(1, n_row)])
    mine2[...] = jnp.concatenate([n, mean, m2, filler], axis=0)
    copies2 = []
    for k in range(1, n_col):
        c = pltpu.make_async_remote_copy(
            src_ref=mine2, dst_ref=got2.at[k], send_sem=s2_sem.at[k], recv_sem=r2_sem.at[k],
            device_id=(row, lax.rem(col + k, n_col)), device_id_type=MESH,
        )
        c.start()
        copies2.append(c)
    lax.fori_loop(SPLIT, last + 1, step, 0)

    for c in halo_copies:
        c.wait_recv()
    p = dot(halo_v[...], w_snd)
    lr[0, 64:72] = jnp.zeros((8, LAT), F32)
    lr[1, 64:72] = jnp.zeros((8, LAT), F32)
    lr[0, 1:65] = p[64:128]
    lr[1, 1:65] = p[128:192]
    lr[0, 0:1] = p[207:208]
    lr[1, 0:1] = p[223:224]
    lr[0, 65:66] = p[224:225]
    lr[1, 65:66] = p[240:241]
    top = jnp.concatenate([p[0:32].astype(BF16), jnp.zeros((96, LAT), BF16)], axis=0)
    col_t[:, 0:64] = jnp.zeros((BANDS, 64, LAT), BF16)
    col_t[BANDS - 1, 32:64] = p[32:64].astype(BF16)
    col_t[:, 80:] = jnp.zeros((BANDS, 48, LAT), BF16)
    for b in range(BANDS):
        pair = jnp.concatenate([lr[0, 4 * b : 4 * b + 8], lr[1, 4 * b : 4 * b + 8]], axis=0)
        col_t[b, 64:80] = pair.astype(BF16)

    def halo_step(i, _):
        bands = [i * NP + u for u in range(NP)]
        tables = [block_diagonal(col_t[b]) for b in bands]
        lhs = [
            [jnp.concatenate([oh_s[b * NBLK + j, :HALF, 2 * LAT :], oh_s[b * NBLK + j, HALF:, 2 * LAT :]], axis=1) for j in range(NBLK)]
            for b in bands
        ]
        for u, b in enumerate(bands):
            more = dot(jnp.concatenate(lhs[u], axis=0), tables[u])
            for j in range(NBLK):
                for h in range(2):
                    here = pl.ds(pl.multiple_of((b * NBLK + j) * BLK + h * HALF, HALF), HALF)
                    part_v[here, :] += more[j * HALF : (j + 1) * HALF, h * LAT : (h + 1) * LAT]
        return 0

    lax.fori_loop(0, BANDS // NP, halo_step, 0)
    tops = block_diagonal(top)
    lhs = [jnp.concatenate([oh_s[j, :HALF, LAT : 2 * LAT], oh_s[j, HALF:, LAT : 2 * LAT]], axis=1) for j in range(NBLK)]
    more = dot(jnp.concatenate(lhs, axis=0), tops)
    for j in range(NBLK):
        for h in range(2):
            here = slice(j * BLK + h * HALF, j * BLK + (h + 1) * HALF)
            part_v[here] += more[j * HALF : (j + 1) * HALF, h * LAT : (h + 1) * LAT]
    wn_first[...] = wn_in[...]
    prepare(wn_hid, wn_out, n_bias, n_gain, n_shift, wn_hid2, wn_out2, wn_avg2, n_vecs)
    for c in halo_copies + copies + copies2:
        c.wait_send()
    for c in copies2:
        c.wait_recv()
    n, mean, m2 = combine([mine2[...]] + [got2[k] for k in range(1, n_col)])
    inv = lax.rsqrt(m2 / n + EPS)
    stats_out[...] = jnp.concatenate([mean, inv, jnp.zeros((6, LAT), F32)], axis=0)


def exchange(nodes, edges, counts, *small):
    n_row, n_col = lax.axis_size("row"), lax.axis_size("col")
    hbm, vmem = pl.BlockSpec(memory_space=pltpu.HBM), pl.BlockSpec(memory_space=pltpu.VMEM)
    pin = lambda a: pltpu.with_memory_space_constraint(a, pltpu.HBM)
    square = pltpu.VMEM((256, 256), BF16)
    outs = (
        pltpu.VMEM((8, LAT), F32),
        pltpu.VMEM(((TRASH + 1) * BLK, LAT), BF16),
        pltpu.VMEM(((TRASH + 1) * BLK, LAT), F32),
        pltpu.VMEM((ROWS, COLS, LAT), BF16),
        pltpu.VMEM((NBLK, 24, BLK), F32),
        square, square, square, square, pltpu.VMEM((8, 256), F32),
        pltpu.VMEM((2 * LAT, LAT), BF16), square, square, square, pltpu.VMEM((8, 256), F32),
    )
    return pl.pallas_call(
        exchange_kernel,
        out_shape=outs,
        in_specs=[hbm] * (3 + N_SMALL),
        out_specs=(vmem,) * len(outs),
        scratch_shapes=[pltpu.VMEM(a.shape, a.dtype) for a in small]
        + [
            pltpu.VMEM((2, ROWS, LAT), BF16),
            pltpu.VMEM((256, LAT), BF16),
            pltpu.VMEM((4, LAT), F32),
            pltpu.VMEM((4, LAT), F32),
            pltpu.VMEM((n_row, 4, LAT), F32),
            pltpu.VMEM((n_col, 4, LAT), F32),
            pltpu.VMEM((ROWS * COLS + 2 * COLS, LAT), BF16),
            pltpu.VMEM((ROWS * COLS, LAT), BF16),
            pltpu.VMEM((BANDS, BAND_NODES, LAT), BF16),
            pltpu.VMEM((2, 72, LAT), F32),
            pltpu.VMEM((NBLK, 24, BLK), F32),
            pltpu.VMEM((TRASH, BLK, 384), BF16),
            pltpu.SMEM((1, BANDS), jnp.int32),
            pltpu.SemaphoreType.DMA,
            pltpu.SemaphoreType.DMA((BANDS,)),
            pltpu.SemaphoreType.DMA,
            pltpu.SemaphoreType.DMA((N_SMALL,)),
            pltpu.SemaphoreType.DMA((8,)),
            pltpu.SemaphoreType.DMA((8,)),
            pltpu.SemaphoreType.DMA((n_row,)),
            pltpu.SemaphoreType.DMA((n_row,)),
            pltpu.SemaphoreType.DMA((n_col,)),
            pltpu.SemaphoreType.DMA((n_col,)),
        ],
        compiler_params=pltpu.CompilerParams(
            collective_id=0, has_side_effects=True, vmem_limit_bytes=24 * 1024 * 1024
        ),
        name="exchange",
    )(pin(nodes), pin(edges), pin(counts), *[pin(a) for a in small])


def main_kernel(
    counts, stats, edges_v, part_v, nodes, ridx, w_x2, w_hid2, w_out2, w_avg2, vecs,
    wn_in, wn_hid2, wn_out2, wn_avg2, n_vecs,
    new_nodes, edges_out,
    out_v, zeros_v, acc, work, x_ring, h2_s, nodes_s, out_sem, node_sem,
):
    zeros_v[...] = jnp.zeros_like(zeros_v)

    place = jnp.int32(0)
    for b in range(BANDS):
        count = counts[0, b]
        for j in range(NBLK):
            work[place + NB * STAGES] = jnp.int32(b * NBLK + j)
            place = place + (count > j * BLK).astype(jnp.int32)
    for k in range(NB * STAGES):
        work[k] = jnp.int32(TRASH)
    for k in range(NB * (STAGES + 1)):
        work[place + NB * STAGES + k] = jnp.int32(TRASH)
    acc[...] = jnp.zeros_like(acc)
    def clear(b, j):
        pltpu.make_async_copy(zeros_v, edges_out.at[pl.ds(b * SLOTS + j * BLK, BLK)], out_sem).start()

    for b in range(BANDS):

        @pl.when(counts[0, b] <= 3 * BLK)
        def _():
            clear(b, 3)
            pl.when(counts[0, b] <= 2 * BLK)(functools.partial(clear, b, 2))

    mean, inv = stats[0:1], stats[1:2]
    node_id = lax.broadcasted_iota(jnp.int32, (BAND_NODES, BLK), 0).astype(F32).astype(BF16)
    one, nought = jnp.ones((), BF16), jnp.zeros((), BF16)

    def item(i, stage, u):
        return work[(i + STAGES - stage) * NB + u]

    slot_id = lax.broadcasted_iota(jnp.int32, (HALF, LAT), 0).astype(F32).astype(BF16)
    bias2, shift = vecs[0:1].astype(BF16), vecs[2:3].astype(BF16)
    us = range(NB)

    def where_of(i, stage):
        ks = [item(i, stage, u) for u in us]
        return ks, [lax.shift_right_logical(k, 2) for k in ks], [lax.rem(k, NBLK) for k in ks]

    def half_rows(k, h):
        return pl.ds(pl.multiple_of(k * BLK + h * HALF, HALF), HALF)

    def scatter(i):
        k2, b2, j2 = where_of(i, 2)
        rows = [ridx[j2[u], pl.ds(b2[u], 1), :].astype(BF16) for u in us]
        for u in us:
            pick = jnp.where(node_id == rows[u], one, nought)
            acc[b2[u]] += dot(pick, out_v[pl.ds(pl.multiple_of(k2[u] * BLK, BLK), BLK), :])

    groups = range(NB // GROUP)

    def rows_of(g, t):
        return slice((g * GROUP + t) * HALF, (g * GROUP + t + 1) * HALF)

    def group(g):
        return slice(g * GROUP * HALF, (g + 1) * GROUP * HALF)

    def output():
        return [dot(h2_s[group(g)], w_out2[...]) + vecs[1:2] for g in groups]

    def first(i):
        k0, _, _ = where_of(i, 0)
        new = lax.rem(i, RING)
        h1s = []
        for g in groups:
            xs, parts = [], []
            for t in range(GROUP):
                k = k0[g * GROUP + t]
                halves = [((edges_v[half_rows(k, h), :].astype(F32) - mean) * inv).astype(BF16) for h in range(2)]
                xs.append(jnp.concatenate(halves, axis=1))
                parts.append(jnp.concatenate([part_v[half_rows(k, h), :] for h in range(2)], axis=1))
            x = jnp.concatenate(xs, axis=0)
            x_ring[new, group(g)] = x
            h1 = dot(x, w_x2[...]) + jnp.concatenate(parts, axis=0)
            h1s.append(jnp.maximum(h1.astype(BF16), nought))
        return h1s

    def variance(cgs):
        weight = vecs[4:5, 0:LAT]
        results = []
        for cg in cgs:
            halves = []
            for h in range(2):
                v = cg[:, h * LAT : (h + 1) * LAT]
                mean_sq = jnp.sum(v * v * weight, axis=1, keepdims=True)
                halves.append(jnp.broadcast_to(mean_sq, v.shape))
            results.append(jnp.concatenate(halves, axis=1))
        return results

    def finish(i, cgs, variances):
        k1, b1, j1 = where_of(i, 1)
        old = lax.rem(i + RING - 1, RING)
        for g in groups:
            scaled = (cgs[g] * lax.rsqrt(variances[g] + EPS)).astype(BF16) + (x_ring[old, group(g)] + shift)
            for t in range(GROUP):
                u = g * GROUP + t
                left_count = counts[0, jnp.minimum(b1[u], BANDS - 1)] - j1[u] * BLK
                for h in range(2):
                    bound = jnp.clip(left_count - h * HALF, 0, HALF).astype(F32)
                    bound = jnp.full((HALF, LAT), bound).astype(BF16)
                    v = scaled[t * HALF : (t + 1) * HALF, h * LAT : (h + 1) * LAT]
                    out_v[half_rows(k1[u], h), :] = jnp.where(slot_id < bound, v, nought)

    def hidden(h1s):
        for g in groups:
            h2_s[group(g)] = jnp.maximum(dot(h1s[g], w_hid2[...]).astype(BF16) + bias2, nought)

    def step(i, _):
        cgs = output()
        h1s = first(i)
        scatter(i)
        variances = variance(cgs)
        finish(i, cgs, variances)
        hidden(h1s)
        for u in range(NB):
            k = item(i, 1, u)

            @pl.when(k < TRASH)
            def _():
                pltpu.make_async_copy(
                    out_v.at[pl.ds(pl.multiple_of(k * BLK, BLK), BLK)],
                    edges_out.at[pl.ds(pl.multiple_of(k * BLK, BLK), BLK)],
                    out_sem,
                ).start()
        return 0

    steps = lax.div(place + (NB - 1), NB) + 1
    hidden(first(0))
    lax.fori_loop(1, steps, step, 0)
    scatter(steps)

    size = 2 * BLK
    chunks = range(ROWS * COLS // size)
    low_bias2, low_shift = n_vecs[0:1].astype(BF16), n_vecs[2:3].astype(BF16)
    owns = [nodes[k * 16 : (k + 1) * 16].reshape(size, LAT) for k in chunks]
    hs = []
    for k in chunks:
        gathered = jnp.concatenate([acc[k * 4 + t] for t in range(4)], axis=0).astype(BF16)
        h = dot(jnp.concatenate([owns[k], gathered], axis=1), wn_in[...]) + n_vecs[3:4, 0:LAT]
        h = jnp.maximum(h.astype(BF16), nought)
        hs.append(jnp.concatenate([h[:BLK], h[BLK:]], axis=1))
    hs = [jnp.maximum(dot(hs[k], wn_hid2[...]).astype(BF16) + low_bias2, nought) for k in chunks]
    cgs = [dot(hs[k], wn_out2[...]) + n_vecs[1:2] for k in chunks]
    lows = [cgs[k].astype(BF16) for k in chunks]
    variances = [dot(lows[k] * lows[k], wn_avg2[...]) for k in chunks]
    node_copies = []
    for k in chunks:
        v = (cgs[k] * lax.rsqrt(variances[k] + EPS)).astype(BF16) + low_shift
        nodes_s[k * size : k * size + BLK] = v[:, :LAT] + owns[k][:BLK]
        nodes_s[k * size + BLK : (k + 1) * size] = v[:, LAT:] + owns[k][BLK:]
        here = pl.ds(k * size, size)
        c = pltpu.make_async_copy(nodes_s.at[here], new_nodes.at[here], node_sem.at[k])
        c.start()
        node_copies.append(c)
    for c in node_copies:
        c.wait()
    pltpu.make_async_copy(out_v.at[pl.ds(0, BANDS * SLOTS)], edges_out, out_sem).wait()


def process(counts, *held):
    vmem, smem = pl.BlockSpec(memory_space=pltpu.VMEM), pl.BlockSpec(memory_space=pltpu.SMEM)
    pin = lambda a: pltpu.with_memory_space_constraint(a, pltpu.VMEM)
    return pl.pallas_call(
        main_kernel,
        out_shape=(
            jax.ShapeDtypeStruct((ROWS * COLS, LAT), BF16),
            jax.ShapeDtypeStruct((BANDS * SLOTS, LAT), BF16),
        ),
        in_specs=[smem] + [vmem] * len(held),
        out_specs=(pl.BlockSpec(memory_space=pl.ANY), pl.BlockSpec(memory_space=pl.ANY)),
        scratch_shapes=[
            pltpu.VMEM(((TRASH + 1) * BLK, LAT), BF16),
            pltpu.VMEM((BLK, LAT), BF16),
            pltpu.VMEM((BANDS + 1, BAND_NODES, LAT), F32),
            pltpu.SMEM((TRASH + NB * (2 * STAGES + 2),), jnp.int32),
            pltpu.VMEM((RING, NB * HALF, 256), BF16),
            pltpu.VMEM((NB * HALF, 256), BF16),
            pltpu.VMEM((ROWS * COLS, LAT), BF16),
            pltpu.SemaphoreType.DMA,
            pltpu.SemaphoreType.DMA((4,)),
        ],
        compiler_params=pltpu.CompilerParams(vmem_limit_bytes=32 * 1024 * 1024),
        name="process",
    )(counts, *[pin(a) for a in held])


def per_device(
    nodes, edges, senders, receivers, counts,
    w_edge_in, w_edge_hid, w_edge_out, edge_bias, edge_gain, edge_shift,
    w_node_in, w_node_hid, w_node_out, node_bias, node_gain, node_shift,
):
    flat_edges = edges.reshape(BANDS * SLOTS, LAT)
    count_row = counts.reshape(1, BANDS)
    held = exchange(
        nodes, flat_edges, count_row, senders.reshape(BANDS, SLOTS), receivers.reshape(BANDS, SLOTS),
        w_edge_in, w_edge_hid, w_edge_out, edge_bias, edge_gain.reshape(1, LAT), edge_shift.reshape(1, LAT),
        w_node_in, w_node_hid, w_node_out, node_bias, node_gain.reshape(1, LAT), node_shift.reshape(1, LAT),
    )
    new_nodes, new_edges = process(count_row, *held)
    return new_nodes.reshape(nodes.shape), new_edges.reshape(edges.shape)


def solution(mesh):
    in_specs = (
        P("row", "col", None),
        P("row", "col", None, None, None),
        P("row", "col", None, None),
        P("row", "col", None, None),
        P("row", "col", None),
    ) + (P(),) * 12
    out_specs = (P("row", "col", None), P("row", "col", None, None, None))
    return jax.shard_map(
        per_device, mesh=mesh, in_specs=in_specs, out_specs=out_specs, check_vma=False
    )
```

```python
import functools

import jax
import jax.numpy as jnp
from jax import lax
from jax.experimental import pallas as pl
from jax.experimental.pallas import tpu as pltpu
from jax.sharding import PartitionSpec as P

F32 = jnp.float32
BF16 = jnp.bfloat16
LAT = 128
ROWS = 64
COLS = 32
BANDS = 16
SLOTS = 1024
BAND_NODES = 128
BLK = 256
HALF = BLK // 2
NBLK = SLOTS // BLK
NA = 8
SPLIT = 6
NP = 16
NB = 4
GROUP = 2
RING = 2
STAGES = 2
TRASH = BANDS * NBLK
EPS = 1e-5
MESH = pl.DeviceIdType.MESH


def tree_sum(terms):
    while len(terms) > 1:
        terms = [functools.reduce(jnp.add, terms[k : k + 2]) for k in range(0, len(terms), 2)]
    return terms[0]


def combine(parts):
    n = tree_sum([p[0:1] for p in parts])
    mean = tree_sum([p[0:1] * p[1:2] for p in parts]) / n
    m2 = tree_sum([p[2:3] + p[0:1] * (p[1:2] - mean) * (p[1:2] - mean) for p in parts])
    return n, mean, m2


def dot(a, b):
    return jnp.dot(a, b, preferred_element_type=F32)


def block_diagonal(w):
    z = jnp.zeros_like(w)
    return jnp.concatenate(
        [jnp.concatenate([w, z], axis=1), jnp.concatenate([z, w], axis=1)], axis=0
    )


def twice(v):
    return jnp.concatenate([v, v], axis=1)


def norm_weights(w_out, bias, gain):
    w = w_out.astype(F32)
    w = (w - jnp.mean(w, axis=1, keepdims=True)) * gain
    b = (bias - jnp.mean(bias, axis=1, keepdims=True)) * gain
    weights = jnp.transpose(jnp.broadcast_to(1.0 / (LAT * gain * gain), (LAT, LAT)))
    return w.astype(BF16), b, weights.astype(BF16)


def prepare(hid, out, bias, gain, shift, hid2, out2, avg2, vecs):
    hid2[...] = block_diagonal(hid[...])
    w, b3, avg = norm_weights(out[...], bias[2:3], gain[...])
    out2[...] = block_diagonal(w)
    avg2[...] = block_diagonal(avg)
    vecs[0:1] = twice(bias[1:2])
    vecs[1:2] = twice(b3)
    vecs[2:3] = twice(shift[...])
    vecs[3:4] = twice(bias[0:1])
    vecs[4:5] = twice(1.0 / (LAT * gain[...] * gain[...]))


N_SMALL = 14


def exchange_kernel(*refs):
    nodes_hbm, edges_hbm, counts_hbm = refs[:3]
    small_hbm = refs[3 : 3 + N_SMALL]
    (
        stats_out, edges_v, part_v, nodes_v, ridx, w_x2, w_hid2, w_out2, w_avg2, vecs,
        wn_first, wn_hid2, wn_out2, wn_avg2, n_vecs,
    ) = refs[3 + N_SMALL : 18 + N_SMALL]
    small = refs[18 + N_SMALL : 18 + 2 * N_SMALL]
    (
        cols_v, halo_v, mine1, mine2, got1, got2, ps_t, pr_t, col_t, lr, sidx, oh_s, counts,
        count_sem, edge_sem, node_sem, small_sem, hs_sem, hr_sem, s1_sem, r1_sem, s2_sem, r2_sem,
    ) = refs[18 + 2 * N_SMALL :]
    (
        senders, receivers, w_in, w_hid, w_out, e_bias, e_gain, e_shift,
        wn_in, wn_hid, wn_out, n_bias, n_gain, n_shift,
    ) = small
    n_row, n_col = lax.axis_size("row"), lax.axis_size("col")
    row, col = lax.axis_index("row"), lax.axis_index("col")
    up, down = lax.rem(row + n_row - 1, n_row), lax.rem(row + 1, n_row)
    left, right = lax.rem(col + n_col - 1, n_col), lax.rem(col + 1, n_col)

    def edge_copy(b):
        return pltpu.make_async_copy(
            edges_hbm.at[pl.ds(b * SLOTS, SLOTS)], edges_v.at[pl.ds(b * SLOTS, SLOTS)], edge_sem.at[b]
        )

    node_copy = pltpu.make_async_copy(nodes_hbm, nodes_v, node_sem)
    for b in range(2):
        edge_copy(b).start()
    count_copy = pltpu.make_async_copy(counts_hbm, counts, count_sem)
    count_copy.start()
    barrier = pltpu.get_barrier_semaphore()
    peers = [(row, lax.rem(col + k, n_col)) for k in range(1, n_col)]
    peers += [(lax.rem(row + k, n_row), col) for k in range(1, n_row)]
    peers += [(up, left), (up, right), (down, left), (down, right)]
    for p in peers:
        pl.semaphore_signal(barrier, inc=1, device_id=p, device_id_type=MESH)
    for b in range(2, BANDS):
        edge_copy(b).start()
    node_copy.start()
    small_copies = [
        pltpu.make_async_copy(src, dst, small_sem.at[k])
        for k, (src, dst) in enumerate(zip(small_hbm, small))
    ]
    for c in small_copies:
        c.start()

    count_copy.wait()
    edge_copy(0).wait()
    low_pivot = edges_v[0:16, :][0:1]
    pivot = low_pivot.astype(F32)
    slot_id = lax.broadcasted_iota(jnp.int32, (64, LAT), 0).astype(F32).astype(BF16)

    def band_sums(b, s, q):
        count = counts[0, b]
        for j in range(SLOTS // 64):
            x = edges_v[pl.ds(pl.multiple_of(b * SLOTS + j * 64, 64), 64), :]
            if j >= SLOTS // 128:
                bound = jnp.clip(count - j * 64, 0, 64).astype(F32)
                x = jnp.where(slot_id < jnp.full((64, LAT), bound).astype(BF16), x, low_pivot)
            d = x.astype(F32) - pivot
            e = d * d
            s = s + ((d[0:8] + d[8:16]) + (d[16:24] + d[24:32])) + ((d[32:40] + d[40:48]) + (d[48:56] + d[56:64]))
            q = q + ((e[0:8] + e[8:16]) + (e[16:24] + e[24:32])) + ((e[32:40] + e[40:48]) + (e[48:56] + e[56:64]))
        return s, q

    def band_stats(b, carry):
        edge_copy(b).wait()
        return band_sums(b, *carry)

    zero = jnp.zeros((8, LAT), F32)
    carry = band_sums(0, zero, zero)
    s, q = lax.fori_loop(1, BANDS, band_stats, carry)
    total = counts[0, 0]
    for b in range(1, BANDS):
        total = total + counts[0, b]
    n = jnp.full((1, LAT), total.astype(F32))
    s = jnp.sum(s, axis=0, keepdims=True)
    q = jnp.sum(q, axis=0, keepdims=True)
    local_mean = s / n
    filler = jnp.zeros((1, LAT), F32)
    mine1[...] = jnp.concatenate([n, pivot + local_mean, q - s * local_mean, filler], axis=0)

    node_copy.wait()
    cols_v[0] = nodes_v[:, 0, :]
    cols_v[1] = nodes_v[:, COLS - 1, :]
    for c in small_copies:
        c.wait()
    w_snd, w_rcv = w_in[LAT : 2 * LAT], w_in[2 * LAT :]
    w_both = jnp.concatenate([w_snd, w_rcv], axis=1)
    bias1 = e_bias[0:1]
    for k in range(ROWS * COLS // BLK):
        own = nodes_v[k * 8 : (k + 1) * 8].reshape(BLK, LAT)
        p = dot(own, w_both)
        ps_t[COLS + k * BLK : COLS + (k + 1) * BLK] = p[:, :LAT].astype(BF16)
        pr_t[k * BLK : (k + 1) * BLK] = (p[:, LAT:] + bias1).astype(BF16)

    s = senders[...]
    r = lax.shift_right_logical(s * 241, 13)
    c = s - r * 34
    place_s = jnp.where(c == 0, 192 + r, jnp.where(c == 33, 200 + r, r * 32 + c - 1)).astype(F32)
    place_r = receivers[...].astype(F32)
    for j in range(NBLK):
        sidx[j, 0:BANDS] = place_s[:, j * BLK : (j + 1) * BLK]
        ridx[j, 0:BANDS] = place_r[:, j * BLK : (j + 1) * BLK]

    w_x2[...] = block_diagonal(w_in[0:LAT])
    prepare(w_hid, w_out, e_bias, e_gain, e_shift, w_hid2, w_out2, w_avg2, vecs)

    node_id = lax.broadcasted_iota(jnp.int32, (256, BLK), 0).astype(F32).astype(BF16)
    one, nought = jnp.ones((), BF16), jnp.zeros((), BF16)

    ps_t[0:COLS] = jnp.zeros((COLS, LAT), BF16)
    ps_t[COLS + ROWS * COLS :] = jnp.zeros((COLS, LAT), BF16)

    def one_hot(k):
        band, j = lax.div(k, NBLK), lax.rem(k, NBLK)
        si = sidx[j, pl.ds(band, 1), :].astype(BF16)
        ri = ridx[j, pl.ds(band, 1), :].astype(BF16)
        pick_s = jnp.where(node_id == si, one, nought)
        pick_r = jnp.where(node_id[:BAND_NODES] == ri, one, nought)
        oh_s[k, :, 0:LAT] = pick_r.T
        oh_s[k, :, LAT:] = pick_s.T

    def gather(k):
        start = pl.multiple_of(lax.div(k, NBLK) * BAND_NODES, BAND_NODES)
        table = jnp.concatenate(
            [pr_t[pl.ds(start, BAND_NODES), :], ps_t[pl.ds(start, 192), :], jnp.zeros((64, LAT), BF16)],
            axis=0,
        )
        part_v[pl.ds(pl.multiple_of(k * BLK, BLK), BLK), :] = dot(oh_s[k], table)

    last = TRASH // NA - 1
    for u in range(NA):
        one_hot(jnp.int32(u))

    pl.semaphore_wait(barrier, len(peers))
    copies = []
    for k in range(1, n_row):
        c = pltpu.make_async_remote_copy(
            src_ref=mine1, dst_ref=got1.at[k], send_sem=s1_sem.at[k], recv_sem=r1_sem.at[k],
            device_id=(lax.rem(row + k, n_row), col), device_id_type=MESH,
        )
        c.start()
        copies.append(c)

    sends = [
        (nodes_v.at[ROWS - 1], (0, 32), (down, col)),
        (nodes_v.at[0], (32, 32), (up, col)),
        (cols_v.at[1], (64, 64), (row, right)),
        (cols_v.at[0], (128, 64), (row, left)),
        (cols_v.at[1, pl.ds(48, 16)], (192, 16), (down, right)),
        (cols_v.at[0, pl.ds(48, 16)], (208, 16), (down, left)),
        (cols_v.at[1, pl.ds(0, 16)], (224, 16), (up, right)),
        (cols_v.at[0, pl.ds(0, 16)], (240, 16), (up, left)),
    ]
    halo_copies = []
    for k, (src, (start, size), dev) in enumerate(sends):
        c = pltpu.make_async_remote_copy(
            src_ref=src, dst_ref=halo_v.at[pl.ds(start, size)],
            send_sem=hs_sem.at[k], recv_sem=hr_sem.at[k], device_id=dev, device_id_type=MESH,
        )
        c.start()
        halo_copies.append(c)

    def step(i, _):
        for u in range(NA):
            gather(i * NA + u)
        for u in range(NA):
            one_hot(jnp.minimum(i + 1, last) * NA + u)
        return 0

    lax.fori_loop(0, SPLIT, step, 0)
    for c in copies:
        c.wait_recv()
    n, mean, m2 = combine([mine1[...]] + [got1[k] for k in range(1, n_row)])
    mine2[...] = jnp.concatenate([n, mean, m2, filler], axis=0)
    copies2 = []
    for k in range(1, n_col):
        c = pltpu.make_async_remote_copy(
            src_ref=mine2, dst_ref=got2.at[k], send_sem=s2_sem.at[k], recv_sem=r2_sem.at[k],
            device_id=(row, lax.rem(col + k, n_col)), device_id_type=MESH,
        )
        c.start()
        copies2.append(c)
    lax.fori_loop(SPLIT, last + 1, step, 0)

    for c in halo_copies:
        c.wait_recv()
    p = dot(halo_v[...], w_snd)
    lr[0, 64:72] = jnp.zeros((8, LAT), F32)
    lr[1, 64:72] = jnp.zeros((8, LAT), F32)
    lr[0, 1:65] = p[64:128]
    lr[1, 1:65] = p[128:192]
    lr[0, 0:1] = p[207:208]
    lr[1, 0:1] = p[223:224]
    lr[0, 65:66] = p[224:225]
    lr[1, 65:66] = p[240:241]
    top = jnp.concatenate([p[0:32].astype(BF16), jnp.zeros((96, LAT), BF16)], axis=0)
    col_t[:, 0:64] = jnp.zeros((BANDS, 64, LAT), BF16)
    col_t[BANDS - 1, 32:64] = p[32:64].astype(BF16)
    col_t[:, 80:] = jnp.zeros((BANDS, 48, LAT), BF16)
    for b in range(BANDS):
        pair = jnp.concatenate([lr[0, 4 * b : 4 * b + 8], lr[1, 4 * b : 4 * b + 8]], axis=0)
        col_t[b, 64:80] = pair.astype(BF16)

    def halo_step(i, _):
        bands = [i * NP + u for u in range(NP)]
        tables = [block_diagonal(col_t[b]) for b in bands]
        lhs = [
            [jnp.concatenate([oh_s[b * NBLK + j, :HALF, 2 * LAT :], oh_s[b * NBLK + j, HALF:, 2 * LAT :]], axis=1) for j in range(NBLK)]
            for b in bands
        ]
        for u, b in enumerate(bands):
            more = dot(jnp.concatenate(lhs[u], axis=0), tables[u])
            for j in range(NBLK):
                for h in range(2):
                    here = pl.ds(pl.multiple_of((b * NBLK + j) * BLK + h * HALF, HALF), HALF)
                    part_v[here, :] += more[j * HALF : (j + 1) * HALF, h * LAT : (h + 1) * LAT]
        return 0

    lax.fori_loop(0, BANDS // NP, halo_step, 0)
    tops = block_diagonal(top)
    lhs = [jnp.concatenate([oh_s[j, :HALF, LAT : 2 * LAT], oh_s[j, HALF:, LAT : 2 * LAT]], axis=1) for j in range(NBLK)]
    more = dot(jnp.concatenate(lhs, axis=0), tops)
    for j in range(NBLK):
        for h in range(2):
            here = slice(j * BLK + h * HALF, j * BLK + (h + 1) * HALF)
            part_v[here] += more[j * HALF : (j + 1) * HALF, h * LAT : (h + 1) * LAT]
    wn_first[...] = wn_in[...]
    prepare(wn_hid, wn_out, n_bias, n_gain, n_shift, wn_hid2, wn_out2, wn_avg2, n_vecs)
    for c in halo_copies + copies + copies2:
        c.wait_send()
    for c in copies2:
        c.wait_recv()
    n, mean, m2 = combine([mine2[...]] + [got2[k] for k in range(1, n_col)])
    inv = lax.rsqrt(m2 / n + EPS)
    stats_out[...] = jnp.concatenate([mean, inv, jnp.zeros((6, LAT), F32)], axis=0)


def exchange(nodes, edges, counts, *small):
    n_row, n_col = lax.axis_size("row"), lax.axis_size("col")
    hbm, vmem = pl.BlockSpec(memory_space=pltpu.HBM), pl.BlockSpec(memory_space=pltpu.VMEM)
    pin = lambda a: pltpu.with_memory_space_constraint(a, pltpu.HBM)
    square = pltpu.VMEM((256, 256), BF16)
    outs = (
        pltpu.VMEM((8, LAT), F32),
        pltpu.VMEM(((TRASH + 1) * BLK, LAT), BF16),
        pltpu.VMEM(((TRASH + 1) * BLK, LAT), F32),
        pltpu.VMEM((ROWS, COLS, LAT), BF16),
        pltpu.VMEM((NBLK, 24, BLK), F32),
        square, square, square, square, pltpu.VMEM((8, 256), F32),
        pltpu.VMEM((2 * LAT, LAT), BF16), square, square, square, pltpu.VMEM((8, 256), F32),
    )
    return pl.pallas_call(
        exchange_kernel,
        out_shape=outs,
        in_specs=[hbm] * (3 + N_SMALL),
        out_specs=(vmem,) * len(outs),
        scratch_shapes=[pltpu.VMEM(a.shape, a.dtype) for a in small]
        + [
            pltpu.VMEM((2, ROWS, LAT), BF16),
            pltpu.VMEM((256, LAT), BF16),
            pltpu.VMEM((4, LAT), F32),
            pltpu.VMEM((4, LAT), F32),
            pltpu.VMEM((n_row, 4, LAT), F32),
            pltpu.VMEM((n_col, 4, LAT), F32),
            pltpu.VMEM((ROWS * COLS + 2 * COLS, LAT), BF16),
            pltpu.VMEM((ROWS * COLS, LAT), BF16),
            pltpu.VMEM((BANDS, BAND_NODES, LAT), BF16),
            pltpu.VMEM((2, 72, LAT), F32),
            pltpu.VMEM((NBLK, 24, BLK), F32),
            pltpu.VMEM((TRASH, BLK, 384), BF16),
            pltpu.SMEM((1, BANDS), jnp.int32),
            pltpu.SemaphoreType.DMA,
            pltpu.SemaphoreType.DMA((BANDS,)),
            pltpu.SemaphoreType.DMA,
            pltpu.SemaphoreType.DMA((N_SMALL,)),
            pltpu.SemaphoreType.DMA((8,)),
            pltpu.SemaphoreType.DMA((8,)),
            pltpu.SemaphoreType.DMA((n_row,)),
            pltpu.SemaphoreType.DMA((n_row,)),
            pltpu.SemaphoreType.DMA((n_col,)),
            pltpu.SemaphoreType.DMA((n_col,)),
        ],
        compiler_params=pltpu.CompilerParams(
            collective_id=0, has_side_effects=True, vmem_limit_bytes=24 * 1024 * 1024
        ),
        name="exchange",
    )(pin(nodes), pin(edges), pin(counts), *[pin(a) for a in small])


def main_kernel(
    counts, stats, edges_v, part_v, nodes, ridx, w_x2, w_hid2, w_out2, w_avg2, vecs,
    wn_in, wn_hid2, wn_out2, wn_avg2, n_vecs,
    new_nodes, edges_out,
    out_v, zeros_v, acc, work, x_ring, h2_s, nodes_s, out_sem, node_sem,
):
    zeros_v[...] = jnp.zeros_like(zeros_v)

    place = jnp.int32(0)
    for b in range(BANDS):
        count = counts[0, b]
        for j in range(NBLK):
            work[place + NB * STAGES] = jnp.int32(b * NBLK + j)
            place = place + (count > j * BLK).astype(jnp.int32)
    for k in range(NB * STAGES):
        work[k] = jnp.int32(TRASH)
    for k in range(NB * (STAGES + 1)):
        work[place + NB * STAGES + k] = jnp.int32(TRASH)
    acc[...] = jnp.zeros_like(acc)
    def clear(b, j):
        pltpu.make_async_copy(zeros_v, edges_out.at[pl.ds(b * SLOTS + j * BLK, BLK)], out_sem).start()

    for b in range(BANDS):

        @pl.when(counts[0, b] <= 3 * BLK)
        def _():
            clear(b, 3)
            pl.when(counts[0, b] <= 2 * BLK)(functools.partial(clear, b, 2))

    mean, inv = stats[0:1], stats[1:2]
    node_id = lax.broadcasted_iota(jnp.int32, (BAND_NODES, BLK), 0).astype(F32).astype(BF16)
    one, nought = jnp.ones((), BF16), jnp.zeros((), BF16)

    def item(i, stage, u):
        return work[(i + STAGES - stage) * NB + u]

    slot_id = lax.broadcasted_iota(jnp.int32, (HALF, LAT), 0).astype(F32).astype(BF16)
    bias2, shift = vecs[0:1].astype(BF16), vecs[2:3].astype(BF16)
    us = range(NB)

    def where_of(i, stage):
        ks = [item(i, stage, u) for u in us]
        return ks, [lax.shift_right_logical(k, 2) for k in ks], [lax.rem(k, NBLK) for k in ks]

    def half_rows(k, h):
        return pl.ds(pl.multiple_of(k * BLK + h * HALF, HALF), HALF)

    def scatter(i):
        k2, b2, j2 = where_of(i, 2)
        rows = [ridx[j2[u], pl.ds(b2[u], 1), :].astype(BF16) for u in us]
        for u in us:
            pick = jnp.where(node_id == rows[u], one, nought)
            acc[b2[u]] += dot(pick, out_v[pl.ds(pl.multiple_of(k2[u] * BLK, BLK), BLK), :])

    groups = range(NB // GROUP)

    def rows_of(g, t):
        return slice((g * GROUP + t) * HALF, (g * GROUP + t + 1) * HALF)

    def group(g):
        return slice(g * GROUP * HALF, (g + 1) * GROUP * HALF)

    def output():
        return [dot(h2_s[group(g)], w_out2[...]) + vecs[1:2] for g in groups]

    def first(i):
        k0, _, _ = where_of(i, 0)
        new = lax.rem(i, RING)
        h1s = []
        for g in groups:
            xs, parts = [], []
            for t in range(GROUP):
                k = k0[g * GROUP + t]
                halves = [((edges_v[half_rows(k, h), :].astype(F32) - mean) * inv).astype(BF16) for h in range(2)]
                xs.append(jnp.concatenate(halves, axis=1))
                parts.append(jnp.concatenate([part_v[half_rows(k, h), :] for h in range(2)], axis=1))
            x = jnp.concatenate(xs, axis=0)
            x_ring[new, group(g)] = x
            h1 = dot(x, w_x2[...]) + jnp.concatenate(parts, axis=0)
            h1s.append(jnp.maximum(h1.astype(BF16), nought))
        return h1s

    def variance(cgs):
        weight = vecs[4:5, 0:LAT]
        results = []
        for cg in cgs:
            halves = []
            for h in range(2):
                v = cg[:, h * LAT : (h + 1) * LAT]
                mean_sq = jnp.sum(v * v * weight, axis=1, keepdims=True)
                halves.append(jnp.broadcast_to(mean_sq, v.shape))
            results.append(jnp.concatenate(halves, axis=1))
        return results

    def finish(i, cgs, variances):
        k1, b1, j1 = where_of(i, 1)
        old = lax.rem(i + RING - 1, RING)
        for g in groups:
            scaled = (cgs[g] * lax.rsqrt(variances[g] + EPS)).astype(BF16) + (x_ring[old, group(g)] + shift)
            for t in range(GROUP):
                u = g * GROUP + t
                left_count = counts[0, jnp.minimum(b1[u], BANDS - 1)] - j1[u] * BLK
                for h in range(2):
                    bound = jnp.clip(left_count - h * HALF, 0, HALF).astype(F32)
                    bound = jnp.full((HALF, LAT), bound).astype(BF16)
                    v = scaled[t * HALF : (t + 1) * HALF, h * LAT : (h + 1) * LAT]
                    out_v[half_rows(k1[u], h), :] = jnp.where(slot_id < bound, v, nought)

    def hidden(h1s):
        for g in groups:
            h2_s[group(g)] = jnp.maximum(dot(h1s[g], w_hid2[...]).astype(BF16) + bias2, nought)

    def step(i, _):
        cgs = output()
        h1s = first(i)
        scatter(i)
        variances = variance(cgs)
        finish(i, cgs, variances)
        hidden(h1s)
        for u in range(NB):
            k = item(i, 1, u)

            @pl.when(k < TRASH)
            def _():
                pltpu.make_async_copy(
                    out_v.at[pl.ds(pl.multiple_of(k * BLK, BLK), BLK)],
                    edges_out.at[pl.ds(pl.multiple_of(k * BLK, BLK), BLK)],
                    out_sem,
                ).start()
        return 0

    steps = lax.div(place + (NB - 1), NB) + 1
    hidden(first(0))
    lax.fori_loop(1, steps, step, 0)
    scatter(steps)

    size = 2 * BLK
    chunks = range(ROWS * COLS // size)
    low_bias2, low_shift = n_vecs[0:1].astype(BF16), n_vecs[2:3].astype(BF16)
    owns = [nodes[k * 16 : (k + 1) * 16].reshape(size, LAT) for k in chunks]
    hs = []
    for k in chunks:
        gathered = jnp.concatenate([acc[k * 4 + t] for t in range(4)], axis=0).astype(BF16)
        h = dot(jnp.concatenate([owns[k], gathered], axis=1), wn_in[...]) + n_vecs[3:4, 0:LAT]
        h = jnp.maximum(h.astype(BF16), nought)
        hs.append(jnp.concatenate([h[:BLK], h[BLK:]], axis=1))
    hs = [jnp.maximum(dot(hs[k], wn_hid2[...]).astype(BF16) + low_bias2, nought) for k in chunks]
    cgs = [dot(hs[k], wn_out2[...]) + n_vecs[1:2] for k in chunks]
    lows = [cgs[k].astype(BF16) for k in chunks]
    variances = [dot(lows[k] * lows[k], wn_avg2[...]) for k in chunks]
    node_copies = []
    for k in chunks:
        v = (cgs[k] * lax.rsqrt(variances[k] + EPS)).astype(BF16) + low_shift
        nodes_s[k * size : k * size + BLK] = v[:, :LAT] + owns[k][:BLK]
        nodes_s[k * size + BLK : (k + 1) * size] = v[:, LAT:] + owns[k][BLK:]
        here = pl.ds(k * size, size)
        c = pltpu.make_async_copy(nodes_s.at[here], new_nodes.at[here], node_sem.at[k])
        c.start()
        node_copies.append(c)
    for c in node_copies:
        c.wait()
    pltpu.make_async_copy(out_v.at[pl.ds(0, BANDS * SLOTS)], edges_out, out_sem).wait()


def process(counts, *held):
    vmem, smem = pl.BlockSpec(memory_space=pltpu.VMEM), pl.BlockSpec(memory_space=pltpu.SMEM)
    pin = lambda a: pltpu.with_memory_space_constraint(a, pltpu.VMEM)
    return pl.pallas_call(
        main_kernel,
        out_shape=(
            jax.ShapeDtypeStruct((ROWS * COLS, LAT), BF16),
            jax.ShapeDtypeStruct((BANDS * SLOTS, LAT), BF16),
        ),
        in_specs=[smem] + [vmem] * len(held),
        out_specs=(pl.BlockSpec(memory_space=pl.ANY), pl.BlockSpec(memory_space=pl.ANY)),
        scratch_shapes=[
            pltpu.VMEM(((TRASH + 1) * BLK, LAT), BF16),
            pltpu.VMEM((BLK, LAT), BF16),
            pltpu.VMEM((BANDS + 1, BAND_NODES, LAT), F32),
            pltpu.SMEM((TRASH + NB * (2 * STAGES + 2),), jnp.int32),
            pltpu.VMEM((RING, NB * HALF, 256), BF16),
            pltpu.VMEM((NB * HALF, 256), BF16),
            pltpu.VMEM((ROWS * COLS, LAT), BF16),
            pltpu.SemaphoreType.DMA,
            pltpu.SemaphoreType.DMA((4,)),
        ],
        compiler_params=pltpu.CompilerParams(vmem_limit_bytes=32 * 1024 * 1024),
        name="process",
    )(counts, *[pin(a) for a in held])


def per_device(
    nodes, edges, senders, receivers, counts,
    w_edge_in, w_edge_hid, w_edge_out, edge_bias, edge_gain, edge_shift,
    w_node_in, w_node_hid, w_node_out, node_bias, node_gain, node_shift,
):
    flat_edges = edges.reshape(BANDS * SLOTS, LAT)
    count_row = counts.reshape(1, BANDS)
    held = exchange(
        nodes, flat_edges, count_row, senders.reshape(BANDS, SLOTS), receivers.reshape(BANDS, SLOTS),
        w_edge_in, w_edge_hid, w_edge_out, edge_bias, edge_gain.reshape(1, LAT), edge_shift.reshape(1, LAT),
        w_node_in, w_node_hid, w_node_out, node_bias, node_gain.reshape(1, LAT), node_shift.reshape(1, LAT),
    )
    new_nodes, new_edges = process(count_row, *held)
    return new_nodes.reshape(nodes.shape), new_edges.reshape(edges.shape)


def solution(mesh):
    in_specs = (
        P("row", "col", None),
        P("row", "col", None, None, None),
        P("row", "col", None, None),
        P("row", "col", None, None),
        P("row", "col", None),
    ) + (P(),) * 12
    out_specs = (P("row", "col", None), P("row", "col", None, None, None))
    return jax.shard_map(
        per_device, mesh=mesh, in_specs=in_specs, out_specs=out_specs, check_vma=False
    )
```
